32 devices in a mesh: ta: 4 (over y, core), xyz: 8 (over z, x).
Axes of the slice: x: 2, y: 2, z: 4, core: 2. Of those that a mesh axis runs over, the one named last changes fastest.
Arguments:
- prop_one: bfloat16 [4, 2, 12, 12, 32768], P('ta', None, None, None, 'xyz'), may hold values from -1.796875 to 1.796875
- prop_two: bfloat16 [4, 2, 12, 12, 32768], P('ta', None, None, None, 'xyz'), may hold values from -1.796875 to 1.796875
Outputs:
- momentum_fields: float32 [4, 16, 2, 32768], P(None, 'ta', None, 'xyz')
The draws below stay inside these ranges and needn't reach their ends.
All inputs are finite; a program needn't handle non-finite values.
Results may differ from the reference program's by a relative error of at most 0.0003.
Values sent between devices are 32-bit elements; how exact they have to be, the bound alone decides.
A program may use at most 128 MiB of HBM per device.

```python
import jax
import jax.numpy as jnp
import numpy as np
from jax import lax

L = 32
TIMES = 4
SITES = 32768


def level_of(key, extent, split, low, top_value):
    loudness, own = 1.0, jax.random.fold_in(key, 6)
    for axis_at, parts in split:
        heights = jnp.exp(jax.random.uniform(jax.random.fold_in(own, axis_at), (parts,), jnp.float32, low / len(split), top_value / len(split)))
        loudness = loudness * jnp.repeat(heights, extent[axis_at] // parts).reshape([-1 if axis == axis_at else 1 for axis in range(len(extent))])
    return loudness


def centred(own_key, shape, spread, limit, cuts=(), dtype=jnp.bfloat16):
    factor_of = level_of(own_key, shape, cuts, -0.22, 0.18) if cuts else 1.0
    values = jax.random.normal(own_key, shape, jnp.float32) * spread * factor_of
    return jnp.minimum(jnp.maximum(values, -limit), limit).astype(dtype)


def setup_inputs(seed: int = 0) -> dict:
    seeds = jax.random.split(jax.random.key(seed), 3)
    return {
        "prop_one": centred(seeds[0], (TIMES, 2, 12, 12, SITES), 0.2887, 1.796875, ((0, 4), (4, 8))),
        "prop_two": centred(seeds[1], (TIMES, 2, 12, 12, SITES), 0.2887, 1.796875, ((0, 4), (4, 8))),
    }


spin_columns = [[3, 2, 1, 0], [3, 2, 1, 0], [2, 3, 0, 1], [2, 3, 0, 1]]
spin_phases = [[1j, 1j, -1j, -1j], [-1.0, 1.0, 1.0, -1.0], [1j, -1j, -1j, 1j], [1.0, 1.0, 1.0, 1.0]]
chiral_signs = [1.0, 1.0, -1.0, -1.0]


def vertex_parts():
    result = []
    for gamma_index in range(4):
        columns = spin_columns[gamma_index]
        phases = spin_phases[gamma_index]
        rows_list = [columns[a // 3] * 3 + a % 3 for a in range(12)]
        phase_list = [complex(phases[a // 3]) for a in range(12)]
        result.append((rows_list, phase_list))
    return result, [chiral_signs[a // 3] for a in range(12)]


def build_operands(prop_a, prop_b):
    gammas, chirality = vertex_parts()
    left_real, left_imag, right_real, right_imag = [], [], [], []
    for rows_list, phase_list in gammas:
        pick_real = jnp.stack([prop_a[0, q] for q in rows_list])
        pick_imag = jnp.stack([prop_a[1, q] for q in rows_list])
        phase_real = jnp.asarray(np.array([p.real for p in phase_list]), jnp.bfloat16)[:, None, None]
        phase_imag = jnp.asarray(np.array([p.imag for p in phase_list]), jnp.bfloat16)[:, None, None]
        left_real.append(phase_real * pick_real - phase_imag * pick_imag)
        left_imag.append(phase_real * pick_imag + phase_imag * pick_real)
        col_real = jnp.stack([prop_b[0][:, q] for q in rows_list], axis=1)
        col_imag = jnp.stack([prop_b[1][:, q] for q in rows_list], axis=1)
        factor = np.array([[phase_list[c] * chirality[rows_list[c]] * chirality[a] for c in range(12)] for a in range(12)])
        factor_real = jnp.asarray(factor.real, jnp.bfloat16)[:, :, None]
        factor_imag = jnp.asarray(factor.imag, jnp.bfloat16)[:, :, None]
        right_real.append(factor_real * col_real + factor_imag * col_imag)
        right_imag.append(factor_imag * col_real - factor_real * col_imag)
    left_rows = jnp.stack(left_real + left_imag).reshape(8, 144, -1)
    right_rows = jnp.stack(right_real + right_imag).reshape(8, 144, -1)
    return left_rows, right_rows


def combine_products(products):
    real_sum = products[:4, :4] - products[4:, 4:]
    imag_sum = products[:4, 4:] + products[4:, :4]
    return jnp.stack([real_sum.reshape(16, -1), imag_sum.reshape(16, -1)], axis=1)


def contract(prop_a, prop_b):
    left_rows, right_rows = build_operands(prop_a, prop_b)
    products = jnp.einsum("mks,nks->mns", left_rows.astype(jnp.float32), right_rows.astype(jnp.float32))
    return combine_products(products)


def reference(prop_one, prop_two):
    def per_slice(slice_pair):
        first_planes = jnp.moveaxis(slice_pair[0].reshape(2, 12, 12, L, L * L), 3, 0)
        second_planes = jnp.moveaxis(slice_pair[1].reshape(2, 12, 12, L, L * L), 3, 0)
        fields = lax.map(lambda plane_pair: contract(plane_pair[0], plane_pair[1]), (first_planes, second_planes))
        fields = jnp.moveaxis(fields, 0, 2).reshape(16, 2, L * L * L)
        complex_field = lax.complex(fields[:, 0], fields[:, 1]).reshape(16, L, L, L)
        spectrum = jnp.fft.fftn(complex_field, axes=(1, 2, 3), norm="ortho")
        spectrum = jnp.transpose(spectrum, (0, 2, 3, 1)).reshape(16, L * L * L)
        return jnp.stack([jnp.real(spectrum), jnp.imag(spectrum)], axis=1).astype(jnp.float32)

    return lax.map(per_slice, (prop_one, prop_two))
```

```python
import functools
import math

import jax
import jax.numpy as jnp
import numpy as np
from jax import lax
from jax.experimental import pallas as pl
from jax.experimental.pallas import tpu as pltpu
from jax.sharding import PartitionSpec as P

L = 32


spin_columns = [[3, 2, 1, 0], [3, 2, 1, 0], [2, 3, 0, 1], [2, 3, 0, 1]]
spin_phases = [[1j, 1j, -1j, -1j], [-1.0, 1.0, 1.0, -1.0], [1j, -1j, -1j, 1j], [1.0, 1.0, 1.0, 1.0]]
chiral_signs = [1.0, 1.0, -1.0, -1.0]


def vertex_parts():
    result = []
    for gamma_index in range(4):
        columns = spin_columns[gamma_index]
        phases = spin_phases[gamma_index]
        rows_list = [columns[a // 3] * 3 + a % 3 for a in range(12)]
        phase_list = [complex(phases[a // 3]) for a in range(12)]
        result.append((rows_list, phase_list))
    return (result, [chiral_signs[a // 3] for a in range(12)])


def contract(prop_a, prop_b):
    gammas, chirality = vertex_parts()
    left_real, left_imag, right_real, right_imag = ([], [], [], [])
    for rows_list, phase_list in gammas:
        pick_real = jnp.stack([prop_a[0, q] for q in rows_list])
        pick_imag = jnp.stack([prop_a[1, q] for q in rows_list])
        phase_real = jnp.asarray(np.array([p.real for p in phase_list]), jnp.bfloat16)[
            :, None, None
        ]
        phase_imag = jnp.asarray(np.array([p.imag for p in phase_list]), jnp.bfloat16)[
            :, None, None
        ]
        left_real.append(phase_real * pick_real - phase_imag * pick_imag)
        left_imag.append(phase_real * pick_imag + phase_imag * pick_real)
        col_real = jnp.stack([prop_b[0][:, q] for q in rows_list], axis=1)
        col_imag = jnp.stack([prop_b[1][:, q] for q in rows_list], axis=1)
        factor = np.array(
            [
                [phase_list[c] * chirality[rows_list[c]] * chirality[a] for c in range(12)]
                for a in range(12)
            ]
        )
        factor_real = jnp.asarray(factor.real, jnp.bfloat16)[:, :, None]
        factor_imag = jnp.asarray(factor.imag, jnp.bfloat16)[:, :, None]
        right_real.append(factor_real * col_real + factor_imag * col_imag)
        right_imag.append(factor_imag * col_real - factor_real * col_imag)
    left_rows = jnp.stack(left_real + left_imag).reshape(8, 144, -1)
    right_rows = jnp.stack(right_real + right_imag).reshape(8, 144, -1)
    products = jnp.einsum("mks,nks->mns", left_rows, right_rows, preferred_element_type=jnp.float32)
    real_sum = products[:4, :4] - products[4:, 4:]
    imag_sum = products[:4, 4:] + products[4:, :4]
    return jnp.stack([real_sum.reshape(16, -1), imag_sum.reshape(16, -1)], axis=1)


def dft_tables(length):
    positions = np.arange(length)
    turn_count = positions[:, None] * positions[None, :] % length
    angles = turn_count * (2.0 * math.pi / length)
    cosines = jnp.asarray(np.cos(angles) / math.sqrt(length), jnp.float32)
    sines = jnp.asarray(np.sin(angles) / math.sqrt(length), jnp.float32)
    return (cosines, sines)


def plane_dft(fields):
    cosines, sines = dft_tables(L)
    highest = lax.Precision.HIGHEST
    shape = fields.shape
    grid = fields.reshape(shape[:4] + (L, L))
    real_part = grid[:, :, 0]
    imag_part = grid[:, :, 1]

    def along_z(values, table):
        return jnp.einsum(
            "tfpyz,zk->tfpyk", values, table, precision=highest, preferred_element_type=jnp.float32
        )

    def along_y(values, table):
        return jnp.einsum(
            "tfpyz,yk->tfpkz", values, table, precision=highest, preferred_element_type=jnp.float32
        )

    mid_real = along_z(real_part, cosines) + along_z(imag_part, sines)
    mid_imag = along_z(imag_part, cosines) - along_z(real_part, sines)
    out_real = along_y(mid_real, cosines) + along_y(mid_imag, sines)
    out_imag = along_y(mid_imag, cosines) - along_y(mid_real, sines)
    return jnp.stack([out_real, out_imag], axis=2).reshape(shape)


def line_dft(data):
    length = data.shape[-2]
    cosines, sines = dft_tables(length)
    real_part = data[..., 0, :, :]
    imag_part = data[..., 1, :, :]

    def transform_rows(values, table):
        return jnp.einsum(
            "...xq,xk->...qk",
            values,
            table,
            precision=lax.Precision.HIGHEST,
            preferred_element_type=jnp.float32,
        )

    out_real = transform_rows(real_part, cosines) + transform_rows(imag_part, sines)
    out_imag = transform_rows(imag_part, cosines) - transform_rows(real_part, sines)
    stacked = jnp.stack([out_real, out_imag], axis=-3)
    return stacked.reshape(stacked.shape[:-2] + (stacked.shape[-2] * stacked.shape[-1],))


def on_device(prop_one, prop_two):
    fields = lax.map(
        lambda slice_pair: contract(slice_pair[0], slice_pair[1]), (prop_one, prop_two)
    )
    local_times, field_count, parts, slab = fields.shape
    planes = slab // (L * L)
    fields = plane_dft(fields.reshape(local_times, field_count, parts, planes, L * L))
    turned_fields = line_dft(lax.all_to_all(fields, "xyz", split_axis=4, concat_axis=3, tiled=True))
    result = lax.all_to_all(turned_fields, "ta", split_axis=1, concat_axis=0, tiled=True)
    return result

LANES = 128
GROUP_PERMS = (0, 2)


def spin_tables():
    chi = np.array(chiral_signs)
    alpha = np.array(spin_phases) * chi[None, :]
    beta = np.array([[spin_phases[n][c] * chi[spin_columns[n][c]] for c in range(4)] for n in range(4)])
    tables = []
    for phases in (alpha, beta):
        pairs = []
        for first in GROUP_PERMS:
            found = []
            for a in range(4):
                for members in found:
                    ratio = phases[first : first + 2, a] / phases[first : first + 2, members[0][0]]
                    if ratio[0] == ratio[1] and ratio[0] in (1, -1):
                        members.append((a, int(ratio[0].real)))
                        break
                else:
                    found.append([(a, 1)])
            assert len(found) == 2
            pairs.append(found)
        lead = np.array([[phases[m, pairs[m // 2][half][0][0]] for half in range(2)] for m in range(4)])
        signs = np.array([[int((lead[m, half] / lead[m, 0]).real) for half in range(2)] for m in range(4)])
        tables.append((pairs, lead[:, 0], signs))
    left, right = tables
    phase = np.outer(left[1], right[1]).reshape(16)
    return left[0], left[2], right[0], right[2], phase


def complex_block(table):
    return np.block([[table.real, table.imag], [-table.imag, table.real]])


def high_low(table):
    high = np.asarray(table).astype(jnp.bfloat16)
    low = (table - high.astype(np.float64)).astype(jnp.bfloat16)
    return jnp.asarray(np.stack([high, low]))


def plane_tables(length):
    quarter = LANES // length
    outer = length // quarter
    lane = np.arange(LANES)
    y, z = lane // length, lane % length
    twiddle = np.exp(-2j * np.pi * np.outer(np.arange(outer), y) / length)
    ky, slot = lane // length, lane % length
    kz = (slot % outer) * quarter + slot // outer
    table = np.exp(-2j * np.pi * (np.outer(y, ky) / quarter + np.outer(z, kz) / length)) / length
    return (
        jnp.asarray(np.stack([twiddle.real, twiddle.imag]), jnp.float32),
        high_low(complex_block(table)),
    )


def line_table(length, own, sources):
    x = np.arange(length)
    turn = np.exp(-2j * np.pi * np.outer(x, x) / length) / math.sqrt(length)
    parts = complex_block(turn).reshape(2, sources, length // sources, 2, length)
    full = np.einsum("asxbk,fg->sxafbgk", parts, np.eye(own))
    rows = length * 2 * own
    return high_low(full.reshape(rows, rows))


def split_dot(values, table):
    high = values.astype(jnp.bfloat16)
    low = (values - high.astype(jnp.float32)).astype(jnp.bfloat16)

    def dot(a, b):
        return jnp.dot(a, b, preferred_element_type=jnp.float32)

    return dot(high, table[0]) + (dot(low, table[0]) + dot(high, table[1]))


def small_fft(values):
    count = len(values)
    if count == 1:
        return values
    even, odd = small_fft(values[0::2]), small_fft(values[1::2])
    low, high = [], []
    for k in range(count // 2):
        re, im = odd[k]
        if k == 0:
            pass
        elif 4 * k == count:
            re, im = im, -re
        else:
            c, s = math.cos(2 * math.pi * k / count), math.sin(2 * math.pi * k / count)
            re, im = c * re + s * im, c * im - s * re
        low.append((even[k][0] + re, even[k][1] + im))
        high.append((even[k][0] - re, even[k][1] - im))
    return low + high


def swap_blocks(values):
    width = LANES // 4
    shape = values[0].shape
    block = lax.broadcasted_iota(jnp.int32, shape, len(shape) - 1) // width
    axis = len(shape) - 1
    values = list(values)
    for step in (2, 1):
        keep = (block // step) % 2 == 0
        result = [None] * 4
        for i in range(4):
            if (i // step) % 2 == 0:
                a, b = values[i], values[i + step]
                result[i] = jnp.where(keep, a, pltpu.roll(b, step * width, axis))
                result[i + step] = jnp.where(keep, pltpu.roll(a, LANES - step * width, axis), b)
        values = result
    return values


def add_signed(total, term, sign):
    if total is None:
        return term if sign > 0 else -term
    return total + term if sign > 0 else total - term


def site_sums(tables, one_ref, two_ref, wide, turned, mixed, row):
    left_groups, left_signs, right_groups, right_signs, _ = tables
    rows = wide.shape[2]
    even = lax.broadcasted_iota(jnp.int32, (8, LANES), 0) % 2 == 0
    span = pl.ds(row, rows)

    @pl.loop(0, 12)
    def _(a):
        for c in range(12):
            value = two_ref[a, c, span, :].astype(jnp.float32)
            wide[a, c, :, :] = value
            for at in range(0, rows, 8):
                piece = value[at : at + 8]
                turned[a, c, at : at + 8, :] = jnp.where(even, pltpu.roll(piece, 7, 0), pltpu.roll(piece, 1, 0))

    for pair in range(2):
        left_columns = spin_columns[GROUP_PERMS[pair]]
        sums = {}
        for half in range(2):
            for turn in range(2):
                right_columns = spin_columns[GROUP_PERMS[turn]]
                for side in range(2):
                    straight, crossed = None, None
                    for a, left_sign in left_groups[pair][half]:
                        for c, right_sign in right_groups[turn][side]:
                            for i in range(3):
                                for j in range(3):
                                    sink, source = left_columns[a] * 3 + i, c * 3 + j
                                    first = one_ref[sink, source, span, :].astype(jnp.float32)
                                    at = (a * 3 + i, right_columns[c] * 3 + j)
                                    sign = left_sign * right_sign
                                    straight = add_signed(straight, first * wide[at[0], at[1], :, :], sign)
                                    crossed = add_signed(crossed, first * turned[at[0], at[1], :, :], sign)
                    sums[half, turn, side] = (straight, crossed)
        for mu in (2 * pair, 2 * pair + 1):
            for nu in range(4):
                for kind in range(2):
                    total = None
                    for half in range(2):
                        for side in range(2):
                            sign = int(left_signs[mu][half] * right_signs[nu][side])
                            total = add_signed(total, sums[half, nu // 2, side][kind], sign)
                    start = (4 * mu + nu) * rows
                    mixed[kind, start : start + rows, :] = total


def plane_blocks(phase_ref, twiddle_ref, plane_ref, mixed, tiles, store):
    blocks = []
    for t in range(tiles):
        straight = [mixed[0, pl.ds(2 * t + part, 16, stride=2 * tiles), :] for part in range(2)]
        crossed = [mixed[1, pl.ds(2 * t + part, 16, stride=2 * tiles), :] for part in range(2)]
        re, im = straight[0] + straight[1], crossed[1] - crossed[0]
        c, s = phase_ref[0], phase_ref[1]
        blocks.append((c * re - s * im, c * im + s * re))
    spectrum = small_fft(blocks)
    turned = []
    for k, (re, im) in enumerate(spectrum):
        c = twiddle_ref[0, k : k + 1, :]
        s = twiddle_ref[1, k : k + 1, :]
        turned.append(jnp.concatenate([re * c - im * s, re * s + im * c], axis=1) if k else jnp.concatenate([re, im], axis=1))
    out = split_dot(jnp.concatenate(turned, axis=0), plane_ref)
    upper = lax.broadcasted_iota(jnp.int32, (8, LANES), 0) < 4
    for half in range(tiles // 4):
        parts = []
        for part in range(2):
            rows = [
                out[(4 * half + p) * 16 : (4 * half + p + 1) * 16, part * LANES : (part + 1) * LANES]
                for p in range(4)
            ]
            parts.append(swap_blocks(rows))
        for k in range(4):
            owner = k * (tiles // 4) + half
            for pair in range(2):
                re = parts[0][k][pair * 8 : pair * 8 + 8]
                im = parts[1][k][pair * 8 : pair * 8 + 8]
                store(owner, 2 * pair, jnp.where(upper, re, pltpu.roll(im, 4, 0)))
                store(owner, 2 * pair + 1, jnp.where(upper, pltpu.roll(re, 4, 0), im))


def finish_time(rows, line_ref, out_ref, at, own):
    out = split_dot(rows.T, line_ref)
    for part in range(2):
        grid = out[:, part * LANES : (part + 1) * LANES].reshape(4, 4, 8, LANES)
        done = swap_blocks([grid[:, q].reshape(32, LANES) for q in range(4)])
        for f in range(own):
            out_ref[at, f, pl.ds(part, 32, stride=2), :] = done[f]


def peers_of(t, s, times, sources):
    y, core, z, x = t // 2, t % 2, s // 2, s % 2
    own_half, other_half = z // 2 * 2, (1 - z // 2) * 2
    near, far = (z + 1) % 2, z % 2
    levels = [other_half, other_half + 1, own_half + near, own_half + far]
    result = []
    for level in range(4):
        for plane in range(8):
            dy, dx, dc = plane // 4, plane // 2 % 2, plane % 2
            if level == 3 and plane == 0:
                continue
            result.append(((y + dy) % 2 * 2 + (core + dc) % 2, levels[level] * 2 + (x + dx) % 2))
    return result


def exchange_kernel(
    tables, tiles, planes, times, sources, names,
    one_hbm, two_hbm, phase_hbm, twiddle_hbm, plane_hbm, line_hbm, got, line_out,
    one_ref, two_ref, phase_ref, twiddle_ref, plane_ref, wide, turned, mixed, send,
    in_sem, table_sem, send_sem, recv_sem,
):
    t, s = lax.axis_index(names[0]), lax.axis_index(names[1])
    barrier = pltpu.get_barrier_semaphore()
    peers = peers_of(t, s, times, sources)
    count = len(peers)

    def device(k):
        return {names[0]: peers[k][0], names[1]: peers[k][1]}

    def load(p, which):
        source, target = ((one_hbm, one_ref), (two_hbm, two_ref))[which]
        rows = pl.ds(pl.multiple_of(p * 2 * tiles, 2 * tiles), 2 * tiles)
        return pltpu.make_async_copy(source.at[:, :, rows, :], target.at[:, :, rows, :], in_sem.at[which, p])

    table_copies = [
        pltpu.make_async_copy(source, target, table_sem.at[k])
        for k, (source, target) in enumerate(
            ((phase_hbm, phase_ref), (twiddle_hbm, twiddle_ref), (plane_hbm, plane_ref), (line_hbm, line_out))
        )
    ]
    for which in (1, 0):
        load(0, which).start()
    for k in range(count):
        pl.semaphore_signal(barrier, inc=1, device_id=device(k), device_id_type=pl.DeviceIdType.MESH)
    for copy in table_copies[:3]:
        copy.start()
    for p in range(1, planes):
        for which in (1, 0):
            load(p, which).start()
    table_copies[3].start()

    @pl.loop(0, planes)
    def _(p):
        load(p, 1).wait()
        load(p, 0).wait()
        row = pl.multiple_of(p * 2 * tiles, 2 * tiles)
        site_sums(tables, one_ref, two_ref, wide, turned, mixed, row)

        @pl.when(p == 0)
        def _():
            for copy in table_copies[:3]:
                copy.wait()

        def store(owner, group, value):
            send[group * sources + owner, p, :, :] = value

        plane_blocks(phase_ref, twiddle_ref, plane_ref, mixed, tiles, store)

        @pl.when(p == 0)
        def _():
            pl.semaphore_wait(barrier, count)

        for k in range(count):
            to_t, to_s = peers[k]
            pltpu.make_async_remote_copy(
                src_ref=send.at[to_t * sources + to_s, p],
                dst_ref=got.at[t * sources + s, p],
                send_sem=send_sem,
                recv_sem=recv_sem,
                device_id=device(k),
                device_id_type=pl.DeviceIdType.MESH,
            ).start()
        own = t * sources + s
        got[own, p, :, :] = send[own, p, :, :]

    table_copies[3].wait()
    everything = pltpu.make_async_remote_copy(
        src_ref=send.at[pl.ds(0, count)],
        dst_ref=got.at[pl.ds(0, count)],
        send_sem=send_sem,
        recv_sem=recv_sem,
        device_id=device(0),
        device_id_type=pl.DeviceIdType.MESH,
    )
    everything.wait_recv()
    everything.wait_send()


def finish_kernel(times, own, got, line_ref, out_hbm, out_ref, out_sem):
    copies = []
    for at in range(times):
        span = got.shape[0] // times
        rows = got[at * span : (at + 1) * span].reshape(-1, LANES)
        finish_time(rows, line_ref, out_ref, at, own)
        copy = pltpu.make_async_copy(out_ref.at[at], out_hbm.at[at], out_sem.at[at])
        copy.start()
        copies.append(copy)
    for copy in copies:
        copy.wait()


def fast_device(prop_one, prop_two, times, sources):
    slab = prop_one.shape[-1]
    plane = L * L
    planes, tiles = slab // plane, plane // LANES
    own = 16 // times
    tables = spin_tables()
    twiddle, plane_table = plane_tables(L)
    line = line_table(L, own, sources)
    phase = np.broadcast_to(tables[4][:, None], (16, LANES))
    phase = jnp.asarray(np.stack([phase.real, phase.imag]), jnp.float32)

    def paired(prop):
        split = prop.reshape(2, 12, 12, slab // LANES, LANES).transpose(1, 2, 3, 0, 4)
        return split.reshape(12, 12, slab // LANES * 2, LANES)

    anywhere = pl.BlockSpec(memory_space=pltpu.HBM)
    vmem = pl.BlockSpec(memory_space=pltpu.VMEM)
    everyone = times * sources
    inputs = (paired(prop_one), paired(prop_two), phase, twiddle, plane_table, line)
    got, line_near = pl.pallas_call(
        functools.partial(exchange_kernel, tables, tiles, planes, times, sources, ("ta", "xyz")),
        out_shape=(
            pltpu.VMEM((everyone, planes, 8, LANES), jnp.float32),
            pltpu.VMEM(line.shape, line.dtype),
        ),
        in_specs=[anywhere] * len(inputs),
        out_specs=(vmem, vmem),
        scratch_shapes=[
            pltpu.VMEM((12, 12, slab // LANES * 2, LANES), jnp.bfloat16),
            pltpu.VMEM((12, 12, slab // LANES * 2, LANES), jnp.bfloat16),
            pltpu.VMEM(phase.shape, phase.dtype),
            pltpu.VMEM(twiddle.shape, twiddle.dtype),
            pltpu.VMEM(plane_table.shape, plane_table.dtype),
            pltpu.VMEM((12, 12, 2 * tiles, LANES), jnp.float32),
            pltpu.VMEM((12, 12, 2 * tiles, LANES), jnp.float32),
            pltpu.VMEM((2, 16 * 2 * tiles, LANES), jnp.float32),
            pltpu.VMEM((everyone, planes, 8, LANES), jnp.float32),
            pltpu.SemaphoreType.DMA((2, planes)),
            pltpu.SemaphoreType.DMA((4,)),
            pltpu.SemaphoreType.DMA,
            pltpu.SemaphoreType.DMA,
        ],
        compiler_params=pltpu.CompilerParams(
            collective_id=0, has_side_effects=True, vmem_limit_bytes=40 * 2**20
        ),
    )(*inputs)
    shape = (times, own, slab * 2 // LANES, LANES)
    out = pl.pallas_call(
        functools.partial(finish_kernel, times, own),
        out_shape=jax.ShapeDtypeStruct(shape, jnp.float32),
        in_specs=[vmem, vmem],
        out_specs=anywhere,
        scratch_shapes=[pltpu.VMEM(shape, jnp.float32), pltpu.SemaphoreType.DMA((times,))],
        compiler_params=pltpu.CompilerParams(vmem_limit_bytes=40 * 2**20),
    )(got, line_near)
    return out.reshape(times, own, slab // LANES, 2, LANES).transpose(0, 1, 3, 2, 4).reshape(times, own, 2, slab)


def solution(mesh):
    placed = (P("ta", None, None, None, "xyz"), P("ta", None, None, None, "xyz"))
    times, sources = mesh.shape["ta"], mesh.shape["xyz"]

    def device(prop_one, prop_two):
        planes = prop_one.shape[-1] // (L * L)
        fits = 4 * L == LANES and planes * sources == L and L // sources == 4 and times == 4
        if fits and prop_one.shape[0] == 1:
            return fast_device(prop_one, prop_two, times, sources)
        return on_device(prop_one, prop_two)

    return jax.shard_map(
        device, mesh=mesh, in_specs=placed, out_specs=P(None, "ta", None, "xyz"), check_vma=False
    )
```

```python
import functools
import math

import jax
import jax.numpy as jnp
import numpy as np
from jax import lax
from jax.experimental import pallas as pl
from jax.experimental.pallas import tpu as pltpu
from jax.sharding import PartitionSpec as P

L = 32


spin_columns = [[3, 2, 1, 0], [3, 2, 1, 0], [2, 3, 0, 1], [2, 3, 0, 1]]
spin_phases = [[1j, 1j, -1j, -1j], [-1.0, 1.0, 1.0, -1.0], [1j, -1j, -1j, 1j], [1.0, 1.0, 1.0, 1.0]]
chiral_signs = [1.0, 1.0, -1.0, -1.0]


def vertex_parts():
    result = []
    for gamma_index in range(4):
        columns = spin_columns[gamma_index]
        phases = spin_phases[gamma_index]
        rows_list = [columns[a // 3] * 3 + a % 3 for a in range(12)]
        phase_list = [complex(phases[a // 3]) for a in range(12)]
        result.append((rows_list, phase_list))
    return (result, [chiral_signs[a // 3] for a in range(12)])


def contract(prop_a, prop_b):
    gammas, chirality = vertex_parts()
    left_real, left_imag, right_real, right_imag = ([], [], [], [])
    for rows_list, phase_list in gammas:
        pick_real = jnp.stack([prop_a[0, q] for q in rows_list])
        pick_imag = jnp.stack([prop_a[1, q] for q in rows_list])
        phase_real = jnp.asarray(np.array([p.real for p in phase_list]), jnp.bfloat16)[
            :, None, None
        ]
        phase_imag = jnp.asarray(np.array([p.imag for p in phase_list]), jnp.bfloat16)[
            :, None, None
        ]
        left_real.append(phase_real * pick_real - phase_imag * pick_imag)
        left_imag.append(phase_real * pick_imag + phase_imag * pick_real)
        col_real = jnp.stack([prop_b[0][:, q] for q in rows_list], axis=1)
        col_imag = jnp.stack([prop_b[1][:, q] for q in rows_list], axis=1)
        factor = np.array(
            [
                [phase_list[c] * chirality[rows_list[c]] * chirality[a] for c in range(12)]
                for a in range(12)
            ]
        )
        factor_real = jnp.asarray(factor.real, jnp.bfloat16)[:, :, None]
        factor_imag = jnp.asarray(factor.imag, jnp.bfloat16)[:, :, None]
        right_real.append(factor_real * col_real + factor_imag * col_imag)
        right_imag.append(factor_imag * col_real - factor_real * col_imag)
    left_rows = jnp.stack(left_real + left_imag).reshape(8, 144, -1)
    right_rows = jnp.stack(right_real + right_imag).reshape(8, 144, -1)
    products = jnp.einsum("mks,nks->mns", left_rows, right_rows, preferred_element_type=jnp.float32)
    real_sum = products[:4, :4] - products[4:, 4:]
    imag_sum = products[:4, 4:] + products[4:, :4]
    return jnp.stack([real_sum.reshape(16, -1), imag_sum.reshape(16, -1)], axis=1)


def dft_tables(length):
    positions = np.arange(length)
    turn_count = positions[:, None] * positions[None, :] % length
    angles = turn_count * (2.0 * math.pi / length)
    cosines = jnp.asarray(np.cos(angles) / math.sqrt(length), jnp.float32)
    sines = jnp.asarray(np.sin(angles) / math.sqrt(length), jnp.float32)
    return (cosines, sines)


def plane_dft(fields):
    cosines, sines = dft_tables(L)
    highest = lax.Precision.HIGHEST
    shape = fields.shape
    grid = fields.reshape(shape[:4] + (L, L))
    real_part = grid[:, :, 0]
    imag_part = grid[:, :, 1]

    def along_z(values, table):
        return jnp.einsum(
            "tfpyz,zk->tfpyk", values, table, precision=highest, preferred_element_type=jnp.float32
        )

    def along_y(values, table):
        return jnp.einsum(
            "tfpyz,yk->tfpkz", values, table, precision=highest, preferred_element_type=jnp.float32
        )

    mid_real = along_z(real_part, cosines) + along_z(imag_part, sines)
    mid_imag = along_z(imag_part, cosines) - along_z(real_part, sines)
    out_real = along_y(mid_real, cosines) + along_y(mid_imag, sines)
    out_imag = along_y(mid_imag, cosines) - along_y(mid_real, sines)
    return jnp.stack([out_real, out_imag], axis=2).reshape(shape)


def line_dft(data):
    length = data.shape[-2]
    cosines, sines = dft_tables(length)
    real_part = data[..., 0, :, :]
    imag_part = data[..., 1, :, :]

    def transform_rows(values, table):
        return jnp.einsum(
            "...xq,xk->...qk",
            values,
            table,
            precision=lax.Precision.HIGHEST,
            preferred_element_type=jnp.float32,
        )

    out_real = transform_rows(real_part, cosines) + transform_rows(imag_part, sines)
    out_imag = transform_rows(imag_part, cosines) - transform_rows(real_part, sines)
    stacked = jnp.stack([out_real, out_imag], axis=-3)
    return stacked.reshape(stacked.shape[:-2] + (stacked.shape[-2] * stacked.shape[-1],))


def on_device(prop_one, prop_two):
    fields = lax.map(
        lambda slice_pair: contract(slice_pair[0], slice_pair[1]), (prop_one, prop_two)
    )
    local_times, field_count, parts, slab = fields.shape
    planes = slab // (L * L)
    fields = plane_dft(fields.reshape(local_times, field_count, parts, planes, L * L))
    turned_fields = line_dft(lax.all_to_all(fields, "xyz", split_axis=4, concat_axis=3, tiled=True))
    result = lax.all_to_all(turned_fields, "ta", split_axis=1, concat_axis=0, tiled=True)
    return result

LANES = 128
GROUP_PERMS = (0, 2)


def spin_tables():
    chi = np.array(chiral_signs)
    alpha = np.array(spin_phases) * chi[None, :]
    beta = np.array([[spin_phases[n][c] * chi[spin_columns[n][c]] for c in range(4)] for n in range(4)])
    tables = []
    for phases in (alpha, beta):
        pairs = []
        for first in GROUP_PERMS:
            found = []
            for a in range(4):
                for members in found:
                    ratio = phases[first : first + 2, a] / phases[first : first + 2, members[0][0]]
                    if ratio[0] == ratio[1] and ratio[0] in (1, -1):
                        members.append((a, int(ratio[0].real)))
                        break
                else:
                    found.append([(a, 1)])
            assert len(found) == 2
            pairs.append(found)
        lead = np.array([[phases[m, pairs[m // 2][half][0][0]] for half in range(2)] for m in range(4)])
        signs = np.array([[int((lead[m, half] / lead[m, 0]).real) for half in range(2)] for m in range(4)])
        tables.append((pairs, lead[:, 0], signs))
    left, right = tables
    phase = np.outer(left[1], right[1]).reshape(16)
    return left[0], left[2], right[0], right[2], phase


def complex_block(table):
    return np.block([[table.real, table.imag], [-table.imag, table.real]])


def high_low(table):
    high = np.asarray(table).astype(jnp.bfloat16)
    low = (table - high.astype(np.float64)).astype(jnp.bfloat16)
    return jnp.asarray(np.stack([high, low]))


def plane_tables(length):
    quarter = LANES // length
    outer = length // quarter
    lane = np.arange(LANES)
    y, z = lane // length, lane % length
    twiddle = np.exp(-2j * np.pi * np.outer(np.arange(outer), y) / length)
    ky, slot = lane // length, lane % length
    kz = (slot % outer) * quarter + slot // outer
    table = np.exp(-2j * np.pi * (np.outer(y, ky) / quarter + np.outer(z, kz) / length)) / length
    return (
        jnp.asarray(np.stack([twiddle.real, twiddle.imag]), jnp.float32),
        high_low(complex_block(table)),
    )


def line_table(length, own, sources):
    x = np.arange(length)
    turn = np.exp(-2j * np.pi * np.outer(x, x) / length) / math.sqrt(length)
    parts = complex_block(turn).reshape(2, sources, length // sources, 2, length)
    full = np.einsum("asxbk,fg->sxafbgk", parts, np.eye(own))
    rows = length * 2 * own
    return high_low(full.reshape(rows, rows))


def split_dot(values, table):
    high = values.astype(jnp.bfloat16)
    low = (values - high.astype(jnp.float32)).astype(jnp.bfloat16)

    def dot(a, b):
        return jnp.dot(a, b, preferred_element_type=jnp.float32)

    return dot(high, table[0]) + (dot(low, table[0]) + dot(high, table[1]))


def small_fft(values):
    count = len(values)
    if count == 1:
        return values
    even, odd = small_fft(values[0::2]), small_fft(values[1::2])
    low, high = [], []
    for k in range(count // 2):
        re, im = odd[k]
        if k == 0:
            pass
        elif 4 * k == count:
            re, im = im, -re
        else:
            c, s = math.cos(2 * math.pi * k / count), math.sin(2 * math.pi * k / count)
            re, im = c * re + s * im, c * im - s * re
        low.append((even[k][0] + re, even[k][1] + im))
        high.append((even[k][0] - re, even[k][1] - im))
    return low + high


def swap_blocks(values):
    width = LANES // 4
    shape = values[0].shape
    block = lax.broadcasted_iota(jnp.int32, shape, len(shape) - 1) // width
    axis = len(shape) - 1
    values = list(values)
    for step in (2, 1):
        keep = (block // step) % 2 == 0
        result = [None] * 4
        for i in range(4):
            if (i // step) % 2 == 0:
                a, b = values[i], values[i + step]
                result[i] = jnp.where(keep, a, pltpu.roll(b, step * width, axis))
                result[i + step] = jnp.where(keep, pltpu.roll(a, LANES - step * width, axis), b)
        values = result
    return values


def add_signed(total, term, sign):
    if total is None:
        return term if sign > 0 else -term
    return total + term if sign > 0 else total - term


def site_sums(tables, one_ref, two_ref, wide, turned, mixed, row):
    left_groups, left_signs, right_groups, right_signs, _ = tables
    rows = wide.shape[2]
    even = lax.broadcasted_iota(jnp.int32, (8, LANES), 0) % 2 == 0
    span = pl.ds(row, rows)

    @pl.loop(0, 12)
    def _(a):
        for c in range(12):
            value = two_ref[a, c, span, :].astype(jnp.float32)
            wide[a, c, :, :] = value
            for at in range(0, rows, 8):
                piece = value[at : at + 8]
                turned[a, c, at : at + 8, :] = jnp.where(even, pltpu.roll(piece, 7, 0), pltpu.roll(piece, 1, 0))

    for pair in range(2):
        left_columns = spin_columns[GROUP_PERMS[pair]]
        sums = {}
        for half in range(2):
            for turn in range(2):
                right_columns = spin_columns[GROUP_PERMS[turn]]
                for side in range(2):
                    straight, crossed = None, None
                    for a, left_sign in left_groups[pair][half]:
                        for c, right_sign in right_groups[turn][side]:
                            for i in range(3):
                                for j in range(3):
                                    sink, source = left_columns[a] * 3 + i, c * 3 + j
                                    first = one_ref[sink, source, span, :].astype(jnp.float32)
                                    at = (a * 3 + i, right_columns[c] * 3 + j)
                                    sign = left_sign * right_sign
                                    straight = add_signed(straight, first * wide[at[0], at[1], :, :], sign)
                                    crossed = add_signed(crossed, first * turned[at[0], at[1], :, :], sign)
                    sums[half, turn, side] = (straight, crossed)
        for mu in (2 * pair, 2 * pair + 1):
            for nu in range(4):
                for kind in range(2):
                    total = None
                    for half in range(2):
                        for side in range(2):
                            sign = int(left_signs[mu][half] * right_signs[nu][side])
                            total = add_signed(total, sums[half, nu // 2, side][kind], sign)
                    start = (4 * mu + nu) * rows
                    mixed[kind, start : start + rows, :] = total


def plane_blocks(phase_ref, twiddle_ref, plane_ref, mixed, tiles, store):
    blocks = []
    for t in range(tiles):
        straight = [mixed[0, pl.ds(2 * t + part, 16, stride=2 * tiles), :] for part in range(2)]
        crossed = [mixed[1, pl.ds(2 * t + part, 16, stride=2 * tiles), :] for part in range(2)]
        re, im = straight[0] + straight[1], crossed[1] - crossed[0]
        c, s = phase_ref[0], phase_ref[1]
        blocks.append((c * re - s * im, c * im + s * re))
    spectrum = small_fft(blocks)
    turned = []
    for k, (re, im) in enumerate(spectrum):
        c = twiddle_ref[0, k : k + 1, :]
        s = twiddle_ref[1, k : k + 1, :]
        turned.append(jnp.concatenate([re * c - im * s, re * s + im * c], axis=1) if k else jnp.concatenate([re, im], axis=1))
    out = split_dot(jnp.concatenate(turned, axis=0), plane_ref)
    upper = lax.broadcasted_iota(jnp.int32, (8, LANES), 0) < 4
    for half in range(tiles // 4):
        parts = []
        for part in range(2):
            rows = [
                out[(4 * half + p) * 16 : (4 * half + p + 1) * 16, part * LANES : (part + 1) * LANES]
                for p in range(4)
            ]
            parts.append(swap_blocks(rows))
        for k in range(4):
            owner = k * (tiles // 4) + half
            for pair in range(2):
                re = parts[0][k][pair * 8 : pair * 8 + 8]
                im = parts[1][k][pair * 8 : pair * 8 + 8]
                store(owner, 2 * pair, jnp.where(upper, re, pltpu.roll(im, 4, 0)))
                store(owner, 2 * pair + 1, jnp.where(upper, pltpu.roll(re, 4, 0), im))


def finish_time(rows, line_ref, out_ref, at, own):
    out = split_dot(rows.T, line_ref)
    for part in range(2):
        grid = out[:, part * LANES : (part + 1) * LANES].reshape(4, 4, 8, LANES)
        done = swap_blocks([grid[:, q].reshape(32, LANES) for q in range(4)])
        for f in range(own):
            out_ref[at, f, pl.ds(part, 32, stride=2), :] = done[f]


def peers_of(t, s, times, sources):
    y, core, z, x = t // 2, t % 2, s // 2, s % 2
    own_half, other_half = z // 2 * 2, (1 - z // 2) * 2
    near, far = (z + 1) % 2, z % 2
    levels = [other_half, other_half + 1, own_half + near, own_half + far]
    result = []
    for level in range(4):
        for plane in range(8):
            dy, dx, dc = plane // 4, plane // 2 % 2, plane % 2
            if level == 3 and plane == 0:
                continue
            result.append(((y + dy) % 2 * 2 + (core + dc) % 2, levels[level] * 2 + (x + dx) % 2))
    return result


def exchange_kernel(
    tables, tiles, planes, times, sources, names,
    one_hbm, two_hbm, phase_hbm, twiddle_hbm, plane_hbm, line_hbm, got, line_out,
    one_ref, two_ref, phase_ref, twiddle_ref, plane_ref, wide, turned, mixed, send,
    in_sem, table_sem, send_sem, recv_sem,
):
    t, s = lax.axis_index(names[0]), lax.axis_index(names[1])
    barrier = pltpu.get_barrier_semaphore()
    peers = peers_of(t, s, times, sources)
    count = len(peers)

    def device(k):
        return {names[0]: peers[k][0], names[1]: peers[k][1]}

    def load(p, which):
        source, target = ((one_hbm, one_ref), (two_hbm, two_ref))[which]
        rows = pl.ds(pl.multiple_of(p * 2 * tiles, 2 * tiles), 2 * tiles)
        return pltpu.make_async_copy(source.at[:, :, rows, :], target.at[:, :, rows, :], in_sem.at[which, p])

    table_copies = [
        pltpu.make_async_copy(source, target, table_sem.at[k])
        for k, (source, target) in enumerate(
            ((phase_hbm, phase_ref), (twiddle_hbm, twiddle_ref), (plane_hbm, plane_ref), (line_hbm, line_out))
        )
    ]
    for which in (1, 0):
        load(0, which).start()
    for k in range(count):
        pl.semaphore_signal(barrier, inc=1, device_id=device(k), device_id_type=pl.DeviceIdType.MESH)
    for copy in table_copies[:3]:
        copy.start()
    for p in range(1, planes):
        for which in (1, 0):
            load(p, which).start()
    table_copies[3].start()

    @pl.loop(0, planes)
    def _(p):
        load(p, 1).wait()
        load(p, 0).wait()
        row = pl.multiple_of(p * 2 * tiles, 2 * tiles)
        site_sums(tables, one_ref, two_ref, wide, turned, mixed, row)

        @pl.when(p == 0)
        def _():
            for copy in table_copies[:3]:
                copy.wait()

        def store(owner, group, value):
            send[group * sources + owner, p, :, :] = value

        plane_blocks(phase_ref, twiddle_ref, plane_ref, mixed, tiles, store)

        @pl.when(p == 0)
        def _():
            pl.semaphore_wait(barrier, count)

        for k in range(count):
            to_t, to_s = peers[k]
            pltpu.make_async_remote_copy(
                src_ref=send.at[to_t * sources + to_s, p],
                dst_ref=got.at[t * sources + s, p],
                send_sem=send_sem,
                recv_sem=recv_sem,
                device_id=device(k),
                device_id_type=pl.DeviceIdType.MESH,
            ).start()
        own = t * sources + s
        got[own, p, :, :] = send[own, p, :, :]

    table_copies[3].wait()
    everything = pltpu.make_async_remote_copy(
        src_ref=send.at[pl.ds(0, count)],
        dst_ref=got.at[pl.ds(0, count)],
        send_sem=send_sem,
        recv_sem=recv_sem,
        device_id=device(0),
        device_id_type=pl.DeviceIdType.MESH,
    )
    everything.wait_recv()
    everything.wait_send()


def finish_kernel(times, own, got, line_ref, out_hbm, out_ref, out_sem):
    copies = []
    for at in range(times):
        span = got.shape[0] // times
        rows = got[at * span : (at + 1) * span].reshape(-1, LANES)
        finish_time(rows, line_ref, out_ref, at, own)
        copy = pltpu.make_async_copy(out_ref.at[at], out_hbm.at[at], out_sem.at[at])
        copy.start()
        copies.append(copy)
    for copy in copies:
        copy.wait()


def fast_device(prop_one, prop_two, times, sources):
    slab = prop_one.shape[-1]
    plane = L * L
    planes, tiles = slab // plane, plane // LANES
    own = 16 // times
    tables = spin_tables()
    twiddle, plane_table = plane_tables(L)
    line = line_table(L, own, sources)
    phase = np.broadcast_to(tables[4][:, None], (16, LANES))
    phase = jnp.asarray(np.stack([phase.real, phase.imag]), jnp.float32)

    def paired(prop):
        split = prop.reshape(2, 12, 12, slab // LANES, LANES).transpose(1, 2, 3, 0, 4)
        return split.reshape(12, 12, slab // LANES * 2, LANES)

    anywhere = pl.BlockSpec(memory_space=pltpu.HBM)
    vmem = pl.BlockSpec(memory_space=pltpu.VMEM)
    everyone = times * sources
    inputs = (paired(prop_one), paired(prop_two), phase, twiddle, plane_table, line)
    got, line_near = pl.pallas_call(
        functools.partial(exchange_kernel, tables, tiles, planes, times, sources, ("ta", "xyz")),
        out_shape=(
            pltpu.VMEM((everyone, planes, 8, LANES), jnp.float32),
            pltpu.VMEM(line.shape, line.dtype),
        ),
        in_specs=[anywhere] * len(inputs),
        out_specs=(vmem, vmem),
        scratch_shapes=[
            pltpu.VMEM((12, 12, slab // LANES * 2, LANES), jnp.bfloat16),
            pltpu.VMEM((12, 12, slab // LANES * 2, LANES), jnp.bfloat16),
            pltpu.VMEM(phase.shape, phase.dtype),
            pltpu.VMEM(twiddle.shape, twiddle.dtype),
            pltpu.VMEM(plane_table.shape, plane_table.dtype),
            pltpu.VMEM((12, 12, 2 * tiles, LANES), jnp.float32),
            pltpu.VMEM((12, 12, 2 * tiles, LANES), jnp.float32),
            pltpu.VMEM((2, 16 * 2 * tiles, LANES), jnp.float32),
            pltpu.VMEM((everyone, planes, 8, LANES), jnp.float32),
            pltpu.SemaphoreType.DMA((2, planes)),
            pltpu.SemaphoreType.DMA((4,)),
            pltpu.SemaphoreType.DMA,
            pltpu.SemaphoreType.DMA,
        ],
        compiler_params=pltpu.CompilerParams(
            collective_id=0, has_side_effects=True, vmem_limit_bytes=40 * 2**20
        ),
    )(*[pltpu.with_memory_space_constraint(v, pltpu.HBM) for v in inputs])
    shape = (times, own, slab * 2 // LANES, LANES)
    out = pl.pallas_call(
        functools.partial(finish_kernel, times, own),
        out_shape=jax.ShapeDtypeStruct(shape, jnp.float32),
        in_specs=[vmem, vmem],
        out_specs=anywhere,
        scratch_shapes=[pltpu.VMEM(shape, jnp.float32), pltpu.SemaphoreType.DMA((times,))],
        compiler_params=pltpu.CompilerParams(vmem_limit_bytes=40 * 2**20),
    )(got, line_near)
    return out.reshape(times, own, slab // LANES, 2, LANES).transpose(0, 1, 3, 2, 4).reshape(times, own, 2, slab)


def solution(mesh):
    placed = (P("ta", None, None, None, "xyz"), P("ta", None, None, None, "xyz"))
    times, sources = mesh.shape["ta"], mesh.shape["xyz"]

    def device(prop_one, prop_two):
        planes = prop_one.shape[-1] // (L * L)
        fits = 4 * L == LANES and planes * sources == L and L // sources == 4 and times == 4
        if fits and prop_one.shape[0] == 1:
            return fast_device(prop_one, prop_two, times, sources)
        return on_device(prop_one, prop_two)

    return jax.shard_map(
        device, mesh=mesh, in_specs=placed, out_specs=P(None, "ta", None, "xyz"), check_vma=False
    )
```

```python
import functools
import math

import jax
import jax.numpy as jnp
import numpy as np
from jax import lax
from jax.experimental import pallas as pl
from jax.experimental.pallas import tpu as pltpu
from jax.sharding import PartitionSpec as P

L = 32


spin_columns = [[3, 2, 1, 0], [3, 2, 1, 0], [2, 3, 0, 1], [2, 3, 0, 1]]
spin_phases = [[1j, 1j, -1j, -1j], [-1.0, 1.0, 1.0, -1.0], [1j, -1j, -1j, 1j], [1.0, 1.0, 1.0, 1.0]]
chiral_signs = [1.0, 1.0, -1.0, -1.0]


def vertex_parts():
    result = []
    for gamma_index in range(4):
        columns = spin_columns[gamma_index]
        phases = spin_phases[gamma_index]
        rows_list = [columns[a // 3] * 3 + a % 3 for a in range(12)]
        phase_list = [complex(phases[a // 3]) for a in range(12)]
        result.append((rows_list, phase_list))
    return (result, [chiral_signs[a // 3] for a in range(12)])


def contract(prop_a, prop_b):
    gammas, chirality = vertex_parts()
    left_real, left_imag, right_real, right_imag = ([], [], [], [])
    for rows_list, phase_list in gammas:
        pick_real = jnp.stack([prop_a[0, q] for q in rows_list])
        pick_imag = jnp.stack([prop_a[1, q] for q in rows_list])
        phase_real = jnp.asarray(np.array([p.real for p in phase_list]), jnp.bfloat16)[
            :, None, None
        ]
        phase_imag = jnp.asarray(np.array([p.imag for p in phase_list]), jnp.bfloat16)[
            :, None, None
        ]
        left_real.append(phase_real * pick_real - phase_imag * pick_imag)
        left_imag.append(phase_real * pick_imag + phase_imag * pick_real)
        col_real = jnp.stack([prop_b[0][:, q] for q in rows_list], axis=1)
        col_imag = jnp.stack([prop_b[1][:, q] for q in rows_list], axis=1)
        factor = np.array(
            [
                [phase_list[c] * chirality[rows_list[c]] * chirality[a] for c in range(12)]
                for a in range(12)
            ]
        )
        factor_real = jnp.asarray(factor.real, jnp.bfloat16)[:, :, None]
        factor_imag = jnp.asarray(factor.imag, jnp.bfloat16)[:, :, None]
        right_real.append(factor_real * col_real + factor_imag * col_imag)
        right_imag.append(factor_imag * col_real - factor_real * col_imag)
    left_rows = jnp.stack(left_real + left_imag).reshape(8, 144, -1)
    right_rows = jnp.stack(right_real + right_imag).reshape(8, 144, -1)
    products = jnp.einsum("mks,nks->mns", left_rows, right_rows, preferred_element_type=jnp.float32)
    real_sum = products[:4, :4] - products[4:, 4:]
    imag_sum = products[:4, 4:] + products[4:, :4]
    return jnp.stack([real_sum.reshape(16, -1), imag_sum.reshape(16, -1)], axis=1)


def dft_tables(length):
    positions = np.arange(length)
    turn_count = positions[:, None] * positions[None, :] % length
    angles = turn_count * (2.0 * math.pi / length)
    cosines = jnp.asarray(np.cos(angles) / math.sqrt(length), jnp.float32)
    sines = jnp.asarray(np.sin(angles) / math.sqrt(length), jnp.float32)
    return (cosines, sines)


def plane_dft(fields):
    cosines, sines = dft_tables(L)
    highest = lax.Precision.HIGHEST
    shape = fields.shape
    grid = fields.reshape(shape[:4] + (L, L))
    real_part = grid[:, :, 0]
    imag_part = grid[:, :, 1]

    def along_z(values, table):
        return jnp.einsum(
            "tfpyz,zk->tfpyk", values, table, precision=highest, preferred_element_type=jnp.float32
        )

    def along_y(values, table):
        return jnp.einsum(
            "tfpyz,yk->tfpkz", values, table, precision=highest, preferred_element_type=jnp.float32
        )

    mid_real = along_z(real_part, cosines) + along_z(imag_part, sines)
    mid_imag = along_z(imag_part, cosines) - along_z(real_part, sines)
    out_real = along_y(mid_real, cosines) + along_y(mid_imag, sines)
    out_imag = along_y(mid_imag, cosines) - along_y(mid_real, sines)
    return jnp.stack([out_real, out_imag], axis=2).reshape(shape)


def line_dft(data):
    length = data.shape[-2]
    cosines, sines = dft_tables(length)
    real_part = data[..., 0, :, :]
    imag_part = data[..., 1, :, :]

    def transform_rows(values, table):
        return jnp.einsum(
            "...xq,xk->...qk",
            values,
            table,
            precision=lax.Precision.HIGHEST,
            preferred_element_type=jnp.float32,
        )

    out_real = transform_rows(real_part, cosines) + transform_rows(imag_part, sines)
    out_imag = transform_rows(imag_part, cosines) - transform_rows(real_part, sines)
    stacked = jnp.stack([out_real, out_imag], axis=-3)
    return stacked.reshape(stacked.shape[:-2] + (stacked.shape[-2] * stacked.shape[-1],))


def on_device(prop_one, prop_two):
    fields = lax.map(
        lambda slice_pair: contract(slice_pair[0], slice_pair[1]), (prop_one, prop_two)
    )
    local_times, field_count, parts, slab = fields.shape
    planes = slab // (L * L)
    fields = plane_dft(fields.reshape(local_times, field_count, parts, planes, L * L))
    turned_fields = line_dft(lax.all_to_all(fields, "xyz", split_axis=4, concat_axis=3, tiled=True))
    result = lax.all_to_all(turned_fields, "ta", split_axis=1, concat_axis=0, tiled=True)
    return result

LANES = 128
GROUP_PERMS = (0, 2)


def spin_tables():
    chi = np.array(chiral_signs)
    alpha = np.array(spin_phases) * chi[None, :]
    beta = np.array([[spin_phases[n][c] * chi[spin_columns[n][c]] for c in range(4)] for n in range(4)])
    tables = []
    for phases in (alpha, beta):
        pairs = []
        for first in GROUP_PERMS:
            found = []
            for a in range(4):
                for members in found:
                    ratio = phases[first : first + 2, a] / phases[first : first + 2, members[0][0]]
                    if ratio[0] == ratio[1] and ratio[0] in (1, -1):
                        members.append((a, int(ratio[0].real)))
                        break
                else:
                    found.append([(a, 1)])
            assert len(found) == 2
            pairs.append(found)
        lead = np.array([[phases[m, pairs[m // 2][half][0][0]] for half in range(2)] for m in range(4)])
        signs = np.array([[int((lead[m, half] / lead[m, 0]).real) for half in range(2)] for m in range(4)])
        tables.append((pairs, lead[:, 0], signs))
    left, right = tables
    phase = np.outer(left[1], right[1]).reshape(16)
    return left[0], left[2], right[0], right[2], phase


def complex_block(table):
    return np.block([[table.real, table.imag], [-table.imag, table.real]])


def high_low(table):
    high = np.asarray(table).astype(jnp.bfloat16)
    low = (table - high.astype(np.float64)).astype(jnp.bfloat16)
    return jnp.asarray(np.stack([high, low]))


def plane_tables(length):
    quarter = LANES // length
    outer = length // quarter
    lane = np.arange(LANES)
    y, z = lane // length, lane % length
    twiddle = np.exp(-2j * np.pi * np.outer(np.arange(outer), y) / length)
    ky, slot = lane // length, lane % length
    kz = (slot % outer) * quarter + slot // outer
    table = np.exp(-2j * np.pi * (np.outer(y, ky) / quarter + np.outer(z, kz) / length)) / length
    return (
        jnp.asarray(np.stack([twiddle.real, twiddle.imag]), jnp.float32),
        high_low(complex_block(table)),
    )


def line_table(length, own, sources):
    x = np.arange(length)
    turn = np.exp(-2j * np.pi * np.outer(x, x) / length) / math.sqrt(length)
    parts = complex_block(turn).reshape(2, sources, length // sources, 2, length)
    full = np.einsum("asxbk,fg->sxafbgk", parts, np.eye(own))
    rows = length * 2 * own
    return high_low(full.reshape(rows, rows))


def split_dot(values, table):
    high = values.astype(jnp.bfloat16)
    low = (values - high.astype(jnp.float32)).astype(jnp.bfloat16)

    def dot(a, b):
        return jnp.dot(a, b, preferred_element_type=jnp.float32)

    return dot(high, table[0]) + (dot(low, table[0]) + dot(high, table[1]))


def small_fft(values):
    count = len(values)
    if count == 1:
        return values
    even, odd = small_fft(values[0::2]), small_fft(values[1::2])
    low, high = [], []
    for k in range(count // 2):
        re, im = odd[k]
        if k == 0:
            pass
        elif 4 * k == count:
            re, im = im, -re
        else:
            c, s = math.cos(2 * math.pi * k / count), math.sin(2 * math.pi * k / count)
            re, im = c * re + s * im, c * im - s * re
        low.append((even[k][0] + re, even[k][1] + im))
        high.append((even[k][0] - re, even[k][1] - im))
    return low + high


def swap_blocks(values):
    width = LANES // 4
    shape = values[0].shape
    block = lax.broadcasted_iota(jnp.int32, shape, len(shape) - 1) // width
    axis = len(shape) - 1
    values = list(values)
    for step in (2, 1):
        keep = (block // step) % 2 == 0
        result = [None] * 4
        for i in range(4):
            if (i // step) % 2 == 0:
                a, b = values[i], values[i + step]
                result[i] = jnp.where(keep, a, pltpu.roll(b, step * width, axis))
                result[i + step] = jnp.where(keep, pltpu.roll(a, LANES - step * width, axis), b)
        values = result
    return values


def add_signed(total, term, sign):
    if total is None:
        return term if sign > 0 else -term
    return total + term if sign > 0 else total - term


def site_sums(tables, one_ref, two_ref, wide, turned, mixed, row):
    left_groups, left_signs, right_groups, right_signs, _ = tables
    rows = wide.shape[2]
    even = lax.broadcasted_iota(jnp.int32, (8, LANES), 0) % 2 == 0
    span = pl.ds(row, rows)

    @pl.loop(0, 12)
    def _(a):
        for c in range(12):
            value = two_ref[a, c, span, :].astype(jnp.float32)
            wide[a, c, :, :] = value
            for at in range(0, rows, 8):
                piece = value[at : at + 8]
                turned[a, c, at : at + 8, :] = jnp.where(even, pltpu.roll(piece, 7, 0), pltpu.roll(piece, 1, 0))

    for pair in range(2):
        left_columns = spin_columns[GROUP_PERMS[pair]]
        sums = {}
        for half in range(2):
            for turn in range(2):
                right_columns = spin_columns[GROUP_PERMS[turn]]
                for side in range(2):
                    straight, crossed = None, None
                    for a, left_sign in left_groups[pair][half]:
                        for c, right_sign in right_groups[turn][side]:
                            for i in range(3):
                                for j in range(3):
                                    sink, source = left_columns[a] * 3 + i, c * 3 + j
                                    first = one_ref[sink, source, span, :].astype(jnp.float32)
                                    at = (a * 3 + i, right_columns[c] * 3 + j)
                                    sign = left_sign * right_sign
                                    straight = add_signed(straight, first * wide[at[0], at[1], :, :], sign)
                                    crossed = add_signed(crossed, first * turned[at[0], at[1], :, :], sign)
                    sums[half, turn, side] = (straight, crossed)
        for mu in (2 * pair, 2 * pair + 1):
            for nu in range(4):
                for kind in range(2):
                    total = None
                    for half in range(2):
                        for side in range(2):
                            sign = int(left_signs[mu][half] * right_signs[nu][side])
                            total = add_signed(total, sums[half, nu // 2, side][kind], sign)
                    start = (4 * mu + nu) * rows
                    mixed[kind, start : start + rows, :] = total


def plane_blocks(phase_ref, twiddle_ref, plane_ref, mixed, tiles, store):
    blocks = []
    for t in range(tiles):
        straight = [mixed[0, pl.ds(2 * t + part, 16, stride=2 * tiles), :] for part in range(2)]
        crossed = [mixed[1, pl.ds(2 * t + part, 16, stride=2 * tiles), :] for part in range(2)]
        re, im = straight[0] + straight[1], crossed[1] - crossed[0]
        c, s = phase_ref[0], phase_ref[1]
        blocks.append((c * re - s * im, c * im + s * re))
    spectrum = small_fft(blocks)
    turned = []
    for k, (re, im) in enumerate(spectrum):
        c = twiddle_ref[0, k : k + 1, :]
        s = twiddle_ref[1, k : k + 1, :]
        turned.append(jnp.concatenate([re * c - im * s, re * s + im * c], axis=1) if k else jnp.concatenate([re, im], axis=1))
    out = split_dot(jnp.concatenate(turned, axis=0), plane_ref)
    upper = lax.broadcasted_iota(jnp.int32, (8, LANES), 0) < 4
    for half in range(tiles // 4):
        parts = []
        for part in range(2):
            rows = [
                out[(4 * half + p) * 16 : (4 * half + p + 1) * 16, part * LANES : (part + 1) * LANES]
                for p in range(4)
            ]
            parts.append(swap_blocks(rows))
        for k in range(4):
            owner = k * (tiles // 4) + half
            for pair in range(2):
                re = parts[0][k][pair * 8 : pair * 8 + 8]
                im = parts[1][k][pair * 8 : pair * 8 + 8]
                store(owner, 2 * pair, jnp.where(upper, re, pltpu.roll(im, 4, 0)))
                store(owner, 2 * pair + 1, jnp.where(upper, pltpu.roll(re, 4, 0), im))


def finish_time(rows, line_ref, out_ref, at, own):
    out = split_dot(rows.T, line_ref)
    for part in range(2):
        grid = out[:, part * LANES : (part + 1) * LANES].reshape(4, 4, 8, LANES)
        done = swap_blocks([grid[:, q].reshape(32, LANES) for q in range(4)])
        for f in range(own):
            out_ref[at, f, pl.ds(part, 32, stride=2), :] = done[f]


def peers_of(t, s, late):
    y, core, z, x = t // 2, t % 2, s // 2, s % 2
    own_half, other_half = z // 2 * 2, (1 - z // 2) * 2
    edge = 3 * (1 - z // 2)
    inner = edge + 2 * (z // 2) - 1
    near, far = own_half + (z + 1) % 2, z
    relative = []
    for level in (edge, inner, near, far):
        for plane in reversed(range(8)):
            dy, dx, dc = plane // 4, plane // 2 % 2, plane % 2
            if level is far and plane == 0:
                continue
            relative.append(((y + dy) % 2 * 2 + (core + dc) % 2, level * 2 + (x + dx) % 2))
    if not late:
        return relative
    first, second = (edge, inner)
    result = []
    for level in (edge, inner, near):
        for plane in range(8):
            dy, dx, dc = plane // 4, plane // 2 % 2, plane % 2
            result.append((dy * 2 + (core + dc) % 2, level * 2 + dx))
    for plane in reversed(range(1, 8)):
        dy, dx, dc = plane // 4, plane // 2 % 2, plane % 2
        result.append(((y + dy) % 2 * 2 + (core + dc) % 2, far * 2 + (x + dx) % 2))
    return result


def exchange_kernel(
    tables, tiles, planes, times, sources, names,
    one_hbm, two_hbm, phase_hbm, twiddle_hbm, plane_hbm, line_hbm, got, line_out,
    one_ref, two_ref, phase_ref, twiddle_ref, plane_ref, wide, turned, mixed, send,
    in_sem, table_sem, send_sem, recv_sem,
):
    t, s = lax.axis_index(names[0]), lax.axis_index(names[1])
    barrier = pltpu.get_barrier_semaphore()
    peers, late_peers = peers_of(t, s, False), peers_of(t, s, True)
    count = len(peers)
    early = planes // 2

    def device(peer):
        return {names[0]: peer[0], names[1]: peer[1]}

    def send_to(peer, at):
        pltpu.make_async_remote_copy(
            src_ref=send.at[peer[0] * sources + peer[1], at],
            dst_ref=got.at[t * sources + s, at],
            send_sem=send_sem,
            recv_sem=recv_sem,
            device_id=device(peer),
            device_id_type=pl.DeviceIdType.MESH,
        ).start()

    def load(p, which):
        source, target = ((one_hbm, one_ref), (two_hbm, two_ref))[which]
        rows = pl.ds(pl.multiple_of(p * 2 * tiles, 2 * tiles), 2 * tiles)
        return pltpu.make_async_copy(source.at[:, :, rows, :], target.at[:, :, rows, :], in_sem.at[which, p])

    table_copies = [
        pltpu.make_async_copy(source, target, table_sem.at[k])
        for k, (source, target) in enumerate(
            ((phase_hbm, phase_ref), (twiddle_hbm, twiddle_ref), (plane_hbm, plane_ref), (line_hbm, line_out))
        )
    ]
    for which in (1, 0):
        load(0, which).start()
    for peer in peers:
        pl.semaphore_signal(barrier, inc=1, device_id=device(peer), device_id_type=pl.DeviceIdType.MESH)
    for copy in table_copies[:3]:
        copy.start()
    for p in range(1, planes):
        for which in (1, 0):
            load(p, which).start()
    table_copies[3].start()

    @pl.loop(0, planes)
    def _(p):
        load(p, 1).wait()
        load(p, 0).wait()
        row = pl.multiple_of(p * 2 * tiles, 2 * tiles)
        site_sums(tables, one_ref, two_ref, wide, turned, mixed, row)

        @pl.when(p == 0)
        def _():
            for copy in table_copies[:3]:
                copy.wait()

        def store(owner, group, value):
            send[group * sources + owner, p, :, :] = value

        plane_blocks(phase_ref, twiddle_ref, plane_ref, mixed, tiles, store)

        @pl.when(p == 0)
        def _():
            pl.semaphore_wait(barrier, count)

        @pl.when(p < early)
        def _():
            for peer in peers:
                send_to(peer, p)

        own = t * sources + s
        got[own, p, :, :] = send[own, p, :, :]

    for peer in late_peers:
        send_to(peer, pl.ds(early, planes - early))
    table_copies[3].wait()
    everything = pltpu.make_async_remote_copy(
        src_ref=send.at[pl.ds(0, count)],
        dst_ref=got.at[pl.ds(0, count)],
        send_sem=send_sem,
        recv_sem=recv_sem,
        device_id=device(peers[0]),
        device_id_type=pl.DeviceIdType.MESH,
    )
    everything.wait_recv()
    everything.wait_send()


def finish_kernel(times, own, got, line_ref, out_hbm, out_ref, out_sem):
    copies = []
    for at in range(times):
        span = got.shape[0] // times
        rows = got[at * span : (at + 1) * span].reshape(-1, LANES)
        finish_time(rows, line_ref, out_ref, at, own)
        copy = pltpu.make_async_copy(out_ref.at[at], out_hbm.at[at], out_sem.at[at])
        copy.start()
        copies.append(copy)
    for copy in copies:
        copy.wait()


def fast_device(prop_one, prop_two, times, sources):
    slab = prop_one.shape[-1]
    plane = L * L
    planes, tiles = slab // plane, plane // LANES
    own = 16 // times
    tables = spin_tables()
    twiddle, plane_table = plane_tables(L)
    line = line_table(L, own, sources)
    phase = np.broadcast_to(tables[4][:, None], (16, LANES))
    phase = jnp.asarray(np.stack([phase.real, phase.imag]), jnp.float32)

    def paired(prop):
        split = prop.reshape(2, 12, 12, slab // LANES, LANES).transpose(1, 2, 3, 0, 4)
        return split.reshape(12, 12, slab // LANES * 2, LANES)

    anywhere = pl.BlockSpec(memory_space=pltpu.HBM)
    vmem = pl.BlockSpec(memory_space=pltpu.VMEM)
    everyone = times * sources
    inputs = (paired(prop_one), paired(prop_two), phase, twiddle, plane_table, line)
    got, line_near = pl.pallas_call(
        functools.partial(exchange_kernel, tables, tiles, planes, times, sources, ("ta", "xyz")),
        out_shape=(
            pltpu.VMEM((everyone, planes, 8, LANES), jnp.float32),
            pltpu.VMEM(line.shape, line.dtype),
        ),
        in_specs=[anywhere] * len(inputs),
        out_specs=(vmem, vmem),
        scratch_shapes=[
            pltpu.VMEM((12, 12, slab // LANES * 2, LANES), jnp.bfloat16),
            pltpu.VMEM((12, 12, slab // LANES * 2, LANES), jnp.bfloat16),
            pltpu.VMEM(phase.shape, phase.dtype),
            pltpu.VMEM(twiddle.shape, twiddle.dtype),
            pltpu.VMEM(plane_table.shape, plane_table.dtype),
            pltpu.VMEM((12, 12, 2 * tiles, LANES), jnp.float32),
            pltpu.VMEM((12, 12, 2 * tiles, LANES), jnp.float32),
            pltpu.VMEM((2, 16 * 2 * tiles, LANES), jnp.float32),
            pltpu.VMEM((everyone, planes, 8, LANES), jnp.float32),
            pltpu.SemaphoreType.DMA((2, planes)),
            pltpu.SemaphoreType.DMA((4,)),
            pltpu.SemaphoreType.DMA,
            pltpu.SemaphoreType.DMA,
        ],
        compiler_params=pltpu.CompilerParams(
            collective_id=0, has_side_effects=True, vmem_limit_bytes=40 * 2**20
        ),
    )(*[pltpu.with_memory_space_constraint(v, pltpu.HBM) for v in inputs])
    shape = (times, own, slab * 2 // LANES, LANES)
    out = pl.pallas_call(
        functools.partial(finish_kernel, times, own),
        out_shape=jax.ShapeDtypeStruct(shape, jnp.float32),
        in_specs=[vmem, vmem],
        out_specs=anywhere,
        scratch_shapes=[pltpu.VMEM(shape, jnp.float32), pltpu.SemaphoreType.DMA((times,))],
        compiler_params=pltpu.CompilerParams(vmem_limit_bytes=40 * 2**20),
    )(got, line_near)
    return out.reshape(times, own, slab // LANES, 2, LANES).transpose(0, 1, 3, 2, 4).reshape(times, own, 2, slab)


def solution(mesh):
    placed = (P("ta", None, None, None, "xyz"), P("ta", None, None, None, "xyz"))
    times, sources = mesh.shape["ta"], mesh.shape["xyz"]

    def device(prop_one, prop_two):
        planes = prop_one.shape[-1] // (L * L)
        fits = 4 * L == LANES and planes * sources == L and L // sources == 4 and times == 4
        if fits and prop_one.shape[0] == 1:
            return fast_device(prop_one, prop_two, times, sources)
        return on_device(prop_one, prop_two)

    return jax.shard_map(
        device, mesh=mesh, in_specs=placed, out_specs=P(None, "ta", None, "xyz"), check_vma=False
    )
```

```python
import functools
import itertools
import math

import jax
import jax.numpy as jnp
import numpy as np
from jax import lax
from jax.experimental import pallas as pl
from jax.experimental.pallas import tpu as pltpu
from jax.sharding import PartitionSpec as P

L = 32


spin_columns = [[3, 2, 1, 0], [3, 2, 1, 0], [2, 3, 0, 1], [2, 3, 0, 1]]
spin_phases = [[1j, 1j, -1j, -1j], [-1.0, 1.0, 1.0, -1.0], [1j, -1j, -1j, 1j], [1.0, 1.0, 1.0, 1.0]]
chiral_signs = [1.0, 1.0, -1.0, -1.0]


def vertex_parts():
    result = []
    for gamma_index in range(4):
        columns = spin_columns[gamma_index]
        phases = spin_phases[gamma_index]
        rows_list = [columns[a // 3] * 3 + a % 3 for a in range(12)]
        phase_list = [complex(phases[a // 3]) for a in range(12)]
        result.append((rows_list, phase_list))
    return (result, [chiral_signs[a // 3] for a in range(12)])


def contract(prop_a, prop_b):
    gammas, chirality = vertex_parts()
    left_real, left_imag, right_real, right_imag = ([], [], [], [])
    for rows_list, phase_list in gammas:
        pick_real = jnp.stack([prop_a[0, q] for q in rows_list])
        pick_imag = jnp.stack([prop_a[1, q] for q in rows_list])
        phase_real = jnp.asarray(np.array([p.real for p in phase_list]), jnp.bfloat16)[
            :, None, None
        ]
        phase_imag = jnp.asarray(np.array([p.imag for p in phase_list]), jnp.bfloat16)[
            :, None, None
        ]
        left_real.append(phase_real * pick_real - phase_imag * pick_imag)
        left_imag.append(phase_real * pick_imag + phase_imag * pick_real)
        col_real = jnp.stack([prop_b[0][:, q] for q in rows_list], axis=1)
        col_imag = jnp.stack([prop_b[1][:, q] for q in rows_list], axis=1)
        factor = np.array(
            [
                [phase_list[c] * chirality[rows_list[c]] * chirality[a] for c in range(12)]
                for a in range(12)
            ]
        )
        factor_real = jnp.asarray(factor.real, jnp.bfloat16)[:, :, None]
        factor_imag = jnp.asarray(factor.imag, jnp.bfloat16)[:, :, None]
        right_real.append(factor_real * col_real + factor_imag * col_imag)
        right_imag.append(factor_imag * col_real - factor_real * col_imag)
    left_rows = jnp.stack(left_real + left_imag).reshape(8, 144, -1)
    right_rows = jnp.stack(right_real + right_imag).reshape(8, 144, -1)
    products = jnp.einsum("mks,nks->mns", left_rows, right_rows, preferred_element_type=jnp.float32)
    real_sum = products[:4, :4] - products[4:, 4:]
    imag_sum = products[:4, 4:] + products[4:, :4]
    return jnp.stack([real_sum.reshape(16, -1), imag_sum.reshape(16, -1)], axis=1)


def dft_tables(length):
    positions = np.arange(length)
    turn_count = positions[:, None] * positions[None, :] % length
    angles = turn_count * (2.0 * math.pi / length)
    cosines = jnp.asarray(np.cos(angles) / math.sqrt(length), jnp.float32)
    sines = jnp.asarray(np.sin(angles) / math.sqrt(length), jnp.float32)
    return (cosines, sines)


def plane_dft(fields):
    cosines, sines = dft_tables(L)
    highest = lax.Precision.HIGHEST
    shape = fields.shape
    grid = fields.reshape(shape[:4] + (L, L))
    real_part = grid[:, :, 0]
    imag_part = grid[:, :, 1]

    def along_z(values, table):
        return jnp.einsum(
            "tfpyz,zk->tfpyk", values, table, precision=highest, preferred_element_type=jnp.float32
        )

    def along_y(values, table):
        return jnp.einsum(
            "tfpyz,yk->tfpkz", values, table, precision=highest, preferred_element_type=jnp.float32
        )

    mid_real = along_z(real_part, cosines) + along_z(imag_part, sines)
    mid_imag = along_z(imag_part, cosines) - along_z(real_part, sines)
    out_real = along_y(mid_real, cosines) + along_y(mid_imag, sines)
    out_imag = along_y(mid_imag, cosines) - along_y(mid_real, sines)
    return jnp.stack([out_real, out_imag], axis=2).reshape(shape)


def line_dft(data):
    length = data.shape[-2]
    cosines, sines = dft_tables(length)
    real_part = data[..., 0, :, :]
    imag_part = data[..., 1, :, :]

    def transform_rows(values, table):
        return jnp.einsum(
            "...xq,xk->...qk",
            values,
            table,
            precision=lax.Precision.HIGHEST,
            preferred_element_type=jnp.float32,
        )

    out_real = transform_rows(real_part, cosines) + transform_rows(imag_part, sines)
    out_imag = transform_rows(imag_part, cosines) - transform_rows(real_part, sines)
    stacked = jnp.stack([out_real, out_imag], axis=-3)
    return stacked.reshape(stacked.shape[:-2] + (stacked.shape[-2] * stacked.shape[-1],))


def on_device(prop_one, prop_two):
    fields = lax.map(
        lambda slice_pair: contract(slice_pair[0], slice_pair[1]), (prop_one, prop_two)
    )
    local_times, field_count, parts, slab = fields.shape
    planes = slab // (L * L)
    fields = plane_dft(fields.reshape(local_times, field_count, parts, planes, L * L))
    turned_fields = line_dft(lax.all_to_all(fields, "xyz", split_axis=4, concat_axis=3, tiled=True))
    result = lax.all_to_all(turned_fields, "ta", split_axis=1, concat_axis=0, tiled=True)
    return result

LANES = 128
GROUP_PERMS = (0, 2)


def spin_tables():
    chi = np.array(chiral_signs)
    alpha = np.array(spin_phases) * chi[None, :]
    beta = np.array([[spin_phases[n][c] * chi[spin_columns[n][c]] for c in range(4)] for n in range(4)])
    tables = []
    for phases in (alpha, beta):
        pairs = []
        for first in GROUP_PERMS:
            found = []
            for a in range(4):
                for members in found:
                    ratio = phases[first : first + 2, a] / phases[first : first + 2, members[0][0]]
                    if ratio[0] == ratio[1] and ratio[0] in (1, -1):
                        members.append((a, int(ratio[0].real)))
                        break
                else:
                    found.append([(a, 1)])
            assert len(found) == 2
            pairs.append(found)
        lead = np.array([[phases[m, pairs[m // 2][half][0][0]] for half in range(2)] for m in range(4)])
        signs = np.array([[int((lead[m, half] / lead[m, 0]).real) for half in range(2)] for m in range(4)])
        tables.append((pairs, lead[:, 0], signs))
    left, right = tables
    phase = np.outer(left[1], right[1]).reshape(16)
    return left[0], left[2], right[0], right[2], phase


def complex_block(table):
    return np.block([[table.real, table.imag], [-table.imag, table.real]])


def high_low(table):
    high = np.asarray(table).astype(jnp.bfloat16)
    low = (table - high.astype(np.float64)).astype(jnp.bfloat16)
    return jnp.asarray(np.stack([high, low]))


def plane_tables(length):
    quarter = LANES // length
    outer = length // quarter
    lane = np.arange(LANES)
    y, z = lane // length, lane % length
    twiddle = np.exp(-2j * np.pi * np.outer(np.arange(outer), y) / length)
    ky, slot = lane // length, lane % length
    kz = (slot % outer) * quarter + slot // outer
    table = np.exp(-2j * np.pi * (np.outer(y, ky) / quarter + np.outer(z, kz) / length)) / length
    return (
        jnp.asarray(np.stack([twiddle.real, twiddle.imag]), jnp.float32),
        high_low(complex_block(table)),
    )


def line_table(length, own, sources):
    x = np.arange(length)
    turn = np.exp(-2j * np.pi * np.outer(x, x) / length) / math.sqrt(length)
    parts = complex_block(turn).reshape(2, sources, length // sources, 2, length)
    full = np.einsum("asxbk,fg->sxafbgk", parts, np.eye(own))
    rows = length * 2 * own
    return high_low(full.reshape(rows, rows))


def split_dot(values, table):
    high = values.astype(jnp.bfloat16)
    low = (values - high.astype(jnp.float32)).astype(jnp.bfloat16)

    def dot(a, b):
        return jnp.dot(a, b, preferred_element_type=jnp.float32)

    return dot(high, table[0]) + (dot(low, table[0]) + dot(high, table[1]))


def small_fft(values):
    count = len(values)
    if count == 1:
        return values
    even, odd = small_fft(values[0::2]), small_fft(values[1::2])
    low, high = [], []
    for k in range(count // 2):
        re, im = odd[k]
        if k == 0:
            pass
        elif 4 * k == count:
            re, im = im, -re
        else:
            c, s = math.cos(2 * math.pi * k / count), math.sin(2 * math.pi * k / count)
            re, im = c * re + s * im, c * im - s * re
        low.append((even[k][0] + re, even[k][1] + im))
        high.append((even[k][0] - re, even[k][1] - im))
    return low + high


def swap_blocks(values):
    width = LANES // 4
    shape = values[0].shape
    block = lax.broadcasted_iota(jnp.int32, shape, len(shape) - 1) // width
    axis = len(shape) - 1
    values = list(values)
    for step in (2, 1):
        keep = (block // step) % 2 == 0
        result = [None] * 4
        for i in range(4):
            if (i // step) % 2 == 0:
                a, b = values[i], values[i + step]
                result[i] = jnp.where(keep, a, pltpu.roll(b, step * width, axis))
                result[i + step] = jnp.where(keep, pltpu.roll(a, LANES - step * width, axis), b)
        values = result
    return values


def add_signed(total, term, sign):
    if total is None:
        return term if sign > 0 else -term
    return total + term if sign > 0 else total - term


def widen(sources, targets, row):
    rows = targets[0].shape[2]

    @pl.loop(0, 12)
    def _(sink):
        for c in range(12):
            for source, target in zip(sources, targets):
                target[sink, c, :, :] = source[sink, c, pl.ds(row, rows), :].astype(jnp.float32)


def site_sums(tables, one, two, partial, mixed):
    left_groups, left_signs, right_groups, right_signs, phases = tables
    tiles = one.shape[2] // 2
    columns = [spin_columns[first] for first in GROUP_PERMS]
    left_of = [{a: (half, sign) for half in range(2) for a, sign in left_groups[pair][half]} for pair in range(2)]
    right_of = [{c: (side, sign) for side in range(2) for c, sign in right_groups[turn][side]} for turn in range(2)]

    def read(ref, at, kind, sign):
        first, second = (ref[at[0], at[1], pl.ds(part, tiles, stride=2), :] if kind in (part, 2) else None for part in range(2))
        if kind < 2:
            return second if kind else first
        return first + second if sign > 0 else first - second

    def blocks(kind):
        def step(i, sums):
            sums = list(sums)
            for j, q_first, c_first in itertools.product(range(3), (0, 2), (0, 2)):
                ones = {
                    (q, c): read(one, (q * 3 + i, c * 3 + j), kind, 1)
                    for q in (q_first, q_first + 1)
                    for c in (c_first, c_first + 1)
                }
                twos = {}
                for q, c in ones:
                    for pair in range(2):
                        for turn in range(2):
                            at = (columns[pair][q], columns[turn][c])
                            if at not in twos:
                                twos[at] = read(two, (at[0] * 3 + i, at[1] * 3 + j), kind, -1)
                for q, c in ones:
                    for pair in range(2):
                        half, left_sign = left_of[pair][columns[pair][q]]
                        for turn in range(2):
                            side, right_sign = right_of[turn][c]
                            k = ((pair * 2 + half) * 2 + turn) * 2 + side
                            term = ones[q, c] * twos[columns[pair][q], columns[turn][c]]
                            sums[k] = add_signed(sums[k], term, left_sign * right_sign)
            return tuple(sums)

        start = tuple(jnp.zeros((tiles, LANES), jnp.float32) for _ in range(16))
        return lax.fori_loop(0, 3, step, start)

    for kind in range(2):
        for k, total in enumerate(blocks(kind)):
            partial[kind, k, :, :] = total
    both = blocks(2)
    for pair in range(2):
        for turn in range(2):
            quads = ([], [])
            for half in range(2):
                for side in range(2):
                    k = ((pair * 2 + half) * 2 + turn) * 2 + side
                    straight, crossed = partial[0, k, :, :], partial[1, k, :, :]
                    quads[0].append(straight + crossed)
                    quads[1].append(both[k] - (straight - crossed))
            for nu in (2 * turn, 2 * turn + 1):
                joined = []
                for quad in quads:
                    for half in range(2):
                        total = add_signed(None, quad[2 * half], int(right_signs[nu][0]))
                        joined.append(add_signed(total, quad[2 * half + 1], int(right_signs[nu][1])))
                for mu in (2 * pair, 2 * pair + 1):
                    field = 4 * mu + nu
                    phase = phases[field]
                    for part in range(2):
                        sign = (phase.real + phase.imag) * (-1 if part and phase.imag else 1)
                        total = add_signed(None, joined[2 * part], int(left_signs[mu][0] * sign))
                        total = add_signed(total, joined[2 * part + 1], int(left_signs[mu][1] * sign))
                        where = 1 - part if phase.imag else part
                        mixed[where, field * tiles : (field + 1) * tiles, :] = total


def plane_blocks(twiddle_ref, plane_ref, mixed, tiles, store):
    blocks = [tuple(mixed[part, pl.ds(t, 16, stride=tiles), :] for part in range(2)) for t in range(tiles)]
    spectrum = small_fft(blocks)
    turned = []
    for k, (re, im) in enumerate(spectrum):
        c = twiddle_ref[0, k : k + 1, :]
        s = twiddle_ref[1, k : k + 1, :]
        turned.append(jnp.concatenate([re * c - im * s, re * s + im * c], axis=1) if k else jnp.concatenate([re, im], axis=1))
    out = split_dot(jnp.concatenate(turned, axis=0), plane_ref)
    upper = lax.broadcasted_iota(jnp.int32, (8, LANES), 0) < 4
    for half in range(tiles // 4):
        parts = []
        for part in range(2):
            rows = [
                out[(4 * half + p) * 16 : (4 * half + p + 1) * 16, part * LANES : (part + 1) * LANES]
                for p in range(4)
            ]
            parts.append(swap_blocks(rows))
        for k in range(4):
            owner = k * (tiles // 4) + half
            for pair in range(2):
                re = parts[0][k][pair * 8 : pair * 8 + 8]
                im = parts[1][k][pair * 8 : pair * 8 + 8]
                store(owner, 2 * pair, jnp.where(upper, re, pltpu.roll(im, 4, 0)))
                store(owner, 2 * pair + 1, jnp.where(upper, pltpu.roll(re, 4, 0), im))


def finish_time(rows, line_ref, out_ref, at, own):
    out = split_dot(rows.T, line_ref)
    for part in range(2):
        grid = out[:, part * LANES : (part + 1) * LANES].reshape(4, 4, 8, LANES)
        done = swap_blocks([grid[:, q].reshape(32, LANES) for q in range(4)])
        for f in range(own):
            out_ref[at, f, pl.ds(part, 32, stride=2), :] = done[f]


def peers_of(t, s):
    y, core, z, x = t // 2, t % 2, s // 2, s % 2
    beyond = z // 2
    edge = 3 * (1 - beyond)
    inner = edge + 2 * beyond - 1
    near = beyond * 2 + (z + 1) % 2
    here = y * 2 + x
    first, second = here % 2 * (1 - here // 2), (1 - here % 2) * (here // 2)
    others = ((3 - here) // 3 * 3, 1 + first, 2 + first + second)
    turn = [(here + k) % 4 for k in range(4)]
    head = [0] + [1 + (here + k) % 3 for k in range(3)]
    edges = [beyond * head[k] + (1 - beyond) * turn[k] for k in range(4)]
    inners = [beyond * head[k] + (1 - beyond) * turn[k] for k in range(4)]

    def chip(level, at):
        return [(at // 2 * 2 + (core + dc) % 2, level * 2 + at % 2) for dc in (1, 0)]

    across = [
        ((y + plane // 4) % 2 * 2 + (core + plane) % 2, level * 2 + (x + plane // 2) % 2)
        for plane in reversed(range(8))
        for level in (edge, inner)
    ]
    late = []
    late += [(False, peer) for peer in chip(near, head[0])]
    late += [(False, peer) for peer in chip(z, others[0])]
    late += [(True, peer) for peer in chip(edge, edges[0])]
    late += [(False, peer) for peer in chip(near, head[1])]
    late += [(True, peer) for peer in chip(edge, edges[1])]
    late += [(False, peer) for peer in chip(z, others[1])]
    late += [(True, peer) for peer in chip(inner, inners[0])]
    late += [(False, peer) for peer in chip(near, head[2])]
    late += [(True, peer) for peer in chip(edge, edges[2])]
    late += [(False, peer) for peer in chip(z, others[2])]
    late += [(True, peer) for peer in chip(inner, inners[1])]
    late += [(False, peer) for peer in chip(near, head[3])]
    late += [(True, peer) for peer in chip(edge, edges[3])]
    late += [(True, peer) for peer in chip(inner, inners[2])]
    late += [(True, peer) for peer in chip(inner, inners[3])]
    late.append((False, (y * 2 + 1 - core, s)))
    return across, late, (t, (3 - z) * 2 + x)


def exchange_kernel(
    tables, tiles, planes, times, sources, names,
    one_hbm, two_hbm, twiddle_hbm, plane_hbm, line_hbm, got, line_out,
    one_ref, two_ref, twiddle_ref, plane_ref, one_wide, two_wide, partial, mixed, send,
    in_sem, table_sem, send_sem, recv_sem, ready,
):
    t, s = lax.axis_index(names[0]), lax.axis_index(names[1])
    barrier = pltpu.get_barrier_semaphore()
    across, late_peers, mirror = peers_of(t, s)
    count = times * sources - 1
    early = planes // 2

    def move(source, target, peer):
        return pltpu.make_async_remote_copy(
            src_ref=source,
            dst_ref=target,
            send_sem=send_sem,
            recv_sem=recv_sem,
            device_id={names[0]: peer[0], names[1]: peer[1]},
            device_id_type=pl.DeviceIdType.MESH,
        )

    def send_to(peer, at):
        move(send.at[peer[0] * sources + peer[1], at], got.at[t * sources + s, at], peer).start()

    def signal(sem, peer):
        pl.semaphore_signal(
            sem, inc=1, device_id={names[0]: peer[0], names[1]: peer[1]}, device_id_type=pl.DeviceIdType.MESH
        )

    def load(p, which):
        source, target = ((one_hbm, one_ref), (two_hbm, two_ref))[which]
        rows = pl.ds(pl.multiple_of(p * 2 * tiles, 2 * tiles), 2 * tiles)
        return pltpu.make_async_copy(source.at[:, :, rows, :], target.at[:, :, rows, :], in_sem.at[which, p])

    table_copies = [
        pltpu.make_async_copy(source, target, table_sem.at[k])
        for k, (source, target) in enumerate(
            ((twiddle_hbm, twiddle_ref), (plane_hbm, plane_ref), (line_hbm, line_out))
        )
    ]
    for which in (1, 0):
        load(0, which).start()
    for peer in across:
        signal(barrier, peer)
    for copy in table_copies[:2]:
        copy.start()
    for p in range(1, planes):
        for which in (1, 0):
            load(p, which).start()
    table_copies[2].start()

    @pl.loop(0, planes)
    def _(p):
        load(p, 1).wait()
        load(p, 0).wait()
        row = pl.multiple_of(p * 2 * tiles, 2 * tiles)
        widen((two_ref, one_ref), (two_wide, one_wide), row)
        site_sums(tables, one_wide, two_wide, partial, mixed)

        @pl.when(p == 0)
        def _():
            for copy in table_copies[:2]:
                copy.wait()

        def store(owner, group, value):
            send[group * sources + owner, p, :, :] = value

        plane_blocks(twiddle_ref, plane_ref, mixed, tiles, store)

        @pl.when(p == 0)
        def _():
            pl.semaphore_wait(barrier, len(across))
            signal(ready, mirror)

        @pl.when(p < early)
        def _():
            for peer in across:
                send_to(peer, p)

        own = t * sources + s
        got[own, p, :, :] = send[own, p, :, :]

    pl.semaphore_wait(ready, 1)
    for crossing, peer in late_peers:
        send_to(peer, pl.ds(early, planes - early) if crossing else pl.ds(0, planes))
    table_copies[2].wait()
    everything = move(send.at[pl.ds(0, count)], got.at[pl.ds(0, count)], mirror)
    everything.wait_recv()
    everything.wait_send()


def finish_kernel(times, own, got, line_ref, out_hbm, out_ref, out_sem):
    copies = []
    for at in range(times):
        span = got.shape[0] // times
        rows = got[at * span : (at + 1) * span].reshape(-1, LANES)
        finish_time(rows, line_ref, out_ref, at, own)
        copy = pltpu.make_async_copy(out_ref.at[at], out_hbm.at[at], out_sem.at[at])
        copy.start()
        copies.append(copy)
    for copy in copies:
        copy.wait()


def fast_device(prop_one, prop_two, times, sources):
    slab = prop_one.shape[-1]
    plane = L * L
    planes, tiles = slab // plane, plane // LANES
    own = 16 // times
    tables = spin_tables()
    twiddle, plane_table = plane_tables(L)
    line = line_table(L, own, sources)

    def paired(prop):
        split = prop.reshape(2, 12, 12, slab // LANES, LANES).transpose(1, 2, 3, 0, 4)
        return split.reshape(12, 12, slab // LANES * 2, LANES)

    anywhere = pl.BlockSpec(memory_space=pltpu.HBM)
    vmem = pl.BlockSpec(memory_space=pltpu.VMEM)
    everyone = times * sources
    inputs = (paired(prop_one), paired(prop_two), twiddle, plane_table, line)
    got, line_near = pl.pallas_call(
        functools.partial(exchange_kernel, tables, tiles, planes, times, sources, ("ta", "xyz")),
        out_shape=(
            pltpu.VMEM((everyone, planes, 8, LANES), jnp.float32),
            pltpu.VMEM(line.shape, line.dtype),
        ),
        in_specs=[anywhere] * len(inputs),
        out_specs=(vmem, vmem),
        scratch_shapes=[
            pltpu.VMEM((12, 12, slab // LANES * 2, LANES), jnp.bfloat16),
            pltpu.VMEM((12, 12, slab // LANES * 2, LANES), jnp.bfloat16),
            pltpu.VMEM(twiddle.shape, twiddle.dtype),
            pltpu.VMEM(plane_table.shape, plane_table.dtype),
            pltpu.VMEM((12, 12, 2 * tiles, LANES), jnp.float32),
            pltpu.VMEM((12, 12, 2 * tiles, LANES), jnp.float32),
            pltpu.VMEM((2, 16, tiles, LANES), jnp.float32),
            pltpu.VMEM((2, 16 * tiles, LANES), jnp.float32),
            pltpu.VMEM((everyone, planes, 8, LANES), jnp.float32),
            pltpu.SemaphoreType.DMA((2, planes)),
            pltpu.SemaphoreType.DMA((3,)),
            pltpu.SemaphoreType.DMA,
            pltpu.SemaphoreType.DMA,
            pltpu.SemaphoreType.REGULAR,
        ],
        compiler_params=pltpu.CompilerParams(
            collective_id=0, has_side_effects=True, vmem_limit_bytes=40 * 2**20
        ),
    )(*[pltpu.with_memory_space_constraint(v, pltpu.HBM) for v in inputs])
    shape = (times, own, slab * 2 // LANES, LANES)
    out = pl.pallas_call(
        functools.partial(finish_kernel, times, own),
        out_shape=jax.ShapeDtypeStruct(shape, jnp.float32),
        in_specs=[vmem, vmem],
        out_specs=anywhere,
        scratch_shapes=[pltpu.VMEM(shape, jnp.float32), pltpu.SemaphoreType.DMA((times,))],
        compiler_params=pltpu.CompilerParams(vmem_limit_bytes=40 * 2**20),
    )(got, line_near)
    return out.reshape(times, own, slab // LANES, 2, LANES).transpose(0, 1, 3, 2, 4).reshape(times, own, 2, slab)


def solution(mesh):
    placed = (P("ta", None, None, None, "xyz"), P("ta", None, None, None, "xyz"))
    times, sources = mesh.shape["ta"], mesh.shape["xyz"]

    def device(prop_one, prop_two):
        planes = prop_one.shape[-1] // (L * L)
        fits = 4 * L == LANES and planes * sources == L and L // sources == 4 and times == 4
        if fits and prop_one.shape[0] == 1:
            return fast_device(prop_one, prop_two, times, sources)
        return on_device(prop_one, prop_two)

    return jax.shard_map(
        device, mesh=mesh, in_specs=placed, out_specs=P(None, "ta", None, "xyz"), check_vma=False
    )
```

```python
import functools
import itertools
import math

import jax
import jax.numpy as jnp
import numpy as np
from jax import lax
from jax.experimental import pallas as pl
from jax.experimental.pallas import tpu as pltpu
from jax.sharding import PartitionSpec as P

L = 32


spin_columns = [[3, 2, 1, 0], [3, 2, 1, 0], [2, 3, 0, 1], [2, 3, 0, 1]]
spin_phases = [[1j, 1j, -1j, -1j], [-1.0, 1.0, 1.0, -1.0], [1j, -1j, -1j, 1j], [1.0, 1.0, 1.0, 1.0]]
chiral_signs = [1.0, 1.0, -1.0, -1.0]


def vertex_parts():
    result = []
    for gamma_index in range(4):
        columns = spin_columns[gamma_index]
        phases = spin_phases[gamma_index]
        rows_list = [columns[a // 3] * 3 + a % 3 for a in range(12)]
        phase_list = [complex(phases[a // 3]) for a in range(12)]
        result.append((rows_list, phase_list))
    return (result, [chiral_signs[a // 3] for a in range(12)])


def contract(prop_a, prop_b):
    gammas, chirality = vertex_parts()
    left_real, left_imag, right_real, right_imag = ([], [], [], [])
    for rows_list, phase_list in gammas:
        pick_real = jnp.stack([prop_a[0, q] for q in rows_list])
        pick_imag = jnp.stack([prop_a[1, q] for q in rows_list])
        phase_real = jnp.asarray(np.array([p.real for p in phase_list]), jnp.bfloat16)[
            :, None, None
        ]
        phase_imag = jnp.asarray(np.array([p.imag for p in phase_list]), jnp.bfloat16)[
            :, None, None
        ]
        left_real.append(phase_real * pick_real - phase_imag * pick_imag)
        left_imag.append(phase_real * pick_imag + phase_imag * pick_real)
        col_real = jnp.stack([prop_b[0][:, q] for q in rows_list], axis=1)
        col_imag = jnp.stack([prop_b[1][:, q] for q in rows_list], axis=1)
        factor = np.array(
            [
                [phase_list[c] * chirality[rows_list[c]] * chirality[a] for c in range(12)]
                for a in range(12)
            ]
        )
        factor_real = jnp.asarray(factor.real, jnp.bfloat16)[:, :, None]
        factor_imag = jnp.asarray(factor.imag, jnp.bfloat16)[:, :, None]
        right_real.append(factor_real * col_real + factor_imag * col_imag)
        right_imag.append(factor_imag * col_real - factor_real * col_imag)
    left_rows = jnp.stack(left_real + left_imag).reshape(8, 144, -1)
    right_rows = jnp.stack(right_real + right_imag).reshape(8, 144, -1)
    products = jnp.einsum("mks,nks->mns", left_rows, right_rows, preferred_element_type=jnp.float32)
    real_sum = products[:4, :4] - products[4:, 4:]
    imag_sum = products[:4, 4:] + products[4:, :4]
    return jnp.stack([real_sum.reshape(16, -1), imag_sum.reshape(16, -1)], axis=1)


def dft_tables(length):
    positions = np.arange(length)
    turn_count = positions[:, None] * positions[None, :] % length
    angles = turn_count * (2.0 * math.pi / length)
    cosines = jnp.asarray(np.cos(angles) / math.sqrt(length), jnp.float32)
    sines = jnp.asarray(np.sin(angles) / math.sqrt(length), jnp.float32)
    return (cosines, sines)


def plane_dft(fields):
    cosines, sines = dft_tables(L)
    highest = lax.Precision.HIGHEST
    shape = fields.shape
    grid = fields.reshape(shape[:4] + (L, L))
    real_part = grid[:, :, 0]
    imag_part = grid[:, :, 1]

    def along_z(values, table):
        return jnp.einsum(
            "tfpyz,zk->tfpyk", values, table, precision=highest, preferred_element_type=jnp.float32
        )

    def along_y(values, table):
        return jnp.einsum(
            "tfpyz,yk->tfpkz", values, table, precision=highest, preferred_element_type=jnp.float32
        )

    mid_real = along_z(real_part, cosines) + along_z(imag_part, sines)
    mid_imag = along_z(imag_part, cosines) - along_z(real_part, sines)
    out_real = along_y(mid_real, cosines) + along_y(mid_imag, sines)
    out_imag = along_y(mid_imag, cosines) - along_y(mid_real, sines)
    return jnp.stack([out_real, out_imag], axis=2).reshape(shape)


def line_dft(data):
    length = data.shape[-2]
    cosines, sines = dft_tables(length)
    real_part = data[..., 0, :, :]
    imag_part = data[..., 1, :, :]

    def transform_rows(values, table):
        return jnp.einsum(
            "...xq,xk->...qk",
            values,
            table,
            precision=lax.Precision.HIGHEST,
            preferred_element_type=jnp.float32,
        )

    out_real = transform_rows(real_part, cosines) + transform_rows(imag_part, sines)
    out_imag = transform_rows(imag_part, cosines) - transform_rows(real_part, sines)
    stacked = jnp.stack([out_real, out_imag], axis=-3)
    return stacked.reshape(stacked.shape[:-2] + (stacked.shape[-2] * stacked.shape[-1],))


def on_device(prop_one, prop_two):
    fields = lax.map(
        lambda slice_pair: contract(slice_pair[0], slice_pair[1]), (prop_one, prop_two)
    )
    local_times, field_count, parts, slab = fields.shape
    planes = slab // (L * L)
    fields = plane_dft(fields.reshape(local_times, field_count, parts, planes, L * L))
    turned_fields = line_dft(lax.all_to_all(fields, "xyz", split_axis=4, concat_axis=3, tiled=True))
    result = lax.all_to_all(turned_fields, "ta", split_axis=1, concat_axis=0, tiled=True)
    return result

LANES = 128
GROUP_PERMS = (0, 2)
LATE, AROUND, BULK = range(3)


def spin_tables():
    chi = np.array(chiral_signs)
    alpha = np.array(spin_phases) * chi[None, :]
    beta = np.array([[spin_phases[n][c] * chi[spin_columns[n][c]] for c in range(4)] for n in range(4)])
    tables = []
    for phases in (alpha, beta):
        pairs = []
        for first in GROUP_PERMS:
            found = []
            for a in range(4):
                for members in found:
                    ratio = phases[first : first + 2, a] / phases[first : first + 2, members[0][0]]
                    if ratio[0] == ratio[1] and ratio[0] in (1, -1):
                        members.append((a, int(ratio[0].real)))
                        break
                else:
                    found.append([(a, 1)])
            assert len(found) == 2
            pairs.append(found)
        lead = np.array([[phases[m, pairs[m // 2][half][0][0]] for half in range(2)] for m in range(4)])
        signs = np.array([[int((lead[m, half] / lead[m, 0]).real) for half in range(2)] for m in range(4)])
        tables.append((pairs, lead[:, 0], signs))
    left, right = tables
    phase = np.outer(left[1], right[1]).reshape(16)
    return left[0], left[2], right[0], right[2], phase


def complex_block(table):
    return np.block([[table.real, table.imag], [-table.imag, table.real]])


def high_low(table):
    high = np.asarray(table).astype(jnp.bfloat16)
    low = (table - high.astype(np.float64)).astype(jnp.bfloat16)
    return jnp.asarray(np.stack([high, low]))


def plane_tables(length):
    quarter = LANES // length
    outer = length // quarter
    lane = np.arange(LANES)
    y, z = lane // length, lane % length
    twiddle = np.exp(-2j * np.pi * np.outer(np.arange(outer), y) / length)
    ky, slot = lane // length, lane % length
    kz = (slot % outer) * quarter + slot // outer
    table = np.exp(-2j * np.pi * (np.outer(y, ky) / quarter + np.outer(z, kz) / length)) / length
    return (
        jnp.asarray(np.stack([twiddle.real, twiddle.imag]), jnp.float32),
        high_low(complex_block(table)),
    )


def line_table(length, own, sources):
    x = np.arange(length)
    turn = np.exp(-2j * np.pi * np.outer(x, x) / length) / math.sqrt(length)
    parts = complex_block(turn).reshape(2, sources, length // sources, 2, length)
    full = np.einsum("asxbk,fg->sxafbgk", parts, np.eye(own))
    rows = length * 2 * own
    return high_low(full.reshape(rows, rows))


def split_dot(values, table):
    high = values.astype(jnp.bfloat16)
    low = (values - high.astype(jnp.float32)).astype(jnp.bfloat16)

    def dot(a, b):
        return jnp.dot(a, b, preferred_element_type=jnp.float32)

    return dot(high, table[0]) + (dot(low, table[0]) + dot(high, table[1]))


def small_fft(values):
    count = len(values)
    if count == 1:
        return values
    even, odd = small_fft(values[0::2]), small_fft(values[1::2])
    low, high = [], []
    for k in range(count // 2):
        re, im = odd[k]
        if k == 0:
            pass
        elif 4 * k == count:
            re, im = im, -re
        else:
            c, s = math.cos(2 * math.pi * k / count), math.sin(2 * math.pi * k / count)
            re, im = c * re + s * im, c * im - s * re
        low.append((even[k][0] + re, even[k][1] + im))
        high.append((even[k][0] - re, even[k][1] - im))
    return low + high


def swap_blocks(values):
    width = LANES // 4
    shape = values[0].shape
    axis = len(shape) - 1
    block = lax.broadcasted_iota(jnp.int32, shape, axis) // width
    low, even = block < 2, block % 2 == 0
    values = list(values)
    for i in range(2):
        first, second = values[i], values[i + 2]
        moved = pltpu.roll(jnp.where(low, second, first), 2 * width, axis)
        values[i], values[i + 2] = jnp.where(low, first, moved), jnp.where(low, moved, second)
    for i in (0, 2):
        first, second = values[i], values[i + 1]
        values[i] = jnp.where(even, first, pltpu.roll(second, width, axis))
        values[i + 1] = jnp.where(even, pltpu.roll(first, LANES - width, axis), second)
    return values


def add_signed(total, term, sign):
    if total is None:
        return term if sign > 0 else -term
    return total + term if sign > 0 else total - term


def widen(sources, targets, row):
    rows = targets[0].shape[2]

    @pl.loop(0, 12)
    def _(sink):
        for c in range(12):
            for source, target in zip(sources, targets):
                target[sink, c, :, :] = source[sink, c, pl.ds(row, rows), :].astype(jnp.float32)


def site_sums(tables, one, two, partial, mixed):
    left_groups, left_signs, right_groups, right_signs, phases = tables
    tiles = one.shape[2] // 2
    columns = [spin_columns[first] for first in GROUP_PERMS]
    left_of = [{a: (half, sign) for half in range(2) for a, sign in left_groups[pair][half]} for pair in range(2)]
    right_of = [{c: (side, sign) for side in range(2) for c, sign in right_groups[turn][side]} for turn in range(2)]

    def read(ref, at, kind, sign):
        first, second = (ref[at[0], at[1], pl.ds(part, tiles, stride=2), :] if kind in (part, 2) else None for part in range(2))
        if kind < 2:
            return second if kind else first
        return first + second if sign > 0 else first - second

    def blocks(kind):
        def step(i, sums):
            sums = list(sums)
            for j, q_first, c_first in itertools.product(range(3), (0, 2), (0, 2)):
                ones = {
                    (q, c): read(one, (q * 3 + i, c * 3 + j), kind, 1)
                    for q in (q_first, q_first + 1)
                    for c in (c_first, c_first + 1)
                }
                twos = {}
                for q, c in ones:
                    for pair in range(2):
                        for turn in range(2):
                            at = (columns[pair][q], columns[turn][c])
                            if at not in twos:
                                twos[at] = read(two, (at[0] * 3 + i, at[1] * 3 + j), kind, -1)
                for q, c in ones:
                    for pair in range(2):
                        half, left_sign = left_of[pair][columns[pair][q]]
                        for turn in range(2):
                            side, right_sign = right_of[turn][c]
                            k = ((pair * 2 + half) * 2 + turn) * 2 + side
                            term = ones[q, c] * twos[columns[pair][q], columns[turn][c]]
                            sums[k] = add_signed(sums[k], term, left_sign * right_sign)
            return tuple(sums)

        start = tuple(jnp.zeros((tiles, LANES), jnp.float32) for _ in range(16))
        return lax.fori_loop(0, 3, step, start)

    for kind in range(2):
        for k, total in enumerate(blocks(kind)):
            partial[kind, k, :, :] = total
    both = blocks(2)
    for pair in range(2):
        for turn in range(2):
            quads = ([], [])
            for half in range(2):
                for side in range(2):
                    k = ((pair * 2 + half) * 2 + turn) * 2 + side
                    straight, crossed = partial[0, k, :, :], partial[1, k, :, :]
                    quads[0].append(straight + crossed)
                    quads[1].append(both[k] - (straight - crossed))
            for nu in (2 * turn, 2 * turn + 1):
                joined = []
                for quad in quads:
                    for half in range(2):
                        total = add_signed(None, quad[2 * half], int(right_signs[nu][0]))
                        joined.append(add_signed(total, quad[2 * half + 1], int(right_signs[nu][1])))
                for mu in (2 * pair, 2 * pair + 1):
                    field = 4 * mu + nu
                    phase = phases[field]
                    for part in range(2):
                        sign = (phase.real + phase.imag) * (-1 if part and phase.imag else 1)
                        total = add_signed(None, joined[2 * part], int(left_signs[mu][0] * sign))
                        total = add_signed(total, joined[2 * part + 1], int(left_signs[mu][1] * sign))
                        where = 1 - part if phase.imag else part
                        mixed[where, field * tiles : (field + 1) * tiles, :] = total


def plane_blocks(twiddle_ref, plane_ref, mixed, tiles, store):
    blocks = [tuple(mixed[part, pl.ds(t, 16, stride=tiles), :] for part in range(2)) for t in range(tiles)]
    spectrum = small_fft(blocks)
    turned = []
    for k, (re, im) in enumerate(spectrum):
        c = twiddle_ref[0, k : k + 1, :]
        s = twiddle_ref[1, k : k + 1, :]
        turned.append(jnp.concatenate([re * c - im * s, re * s + im * c], axis=1) if k else jnp.concatenate([re, im], axis=1))
    out = split_dot(jnp.concatenate(turned, axis=0), plane_ref)
    upper = lax.broadcasted_iota(jnp.int32, (8, LANES), 0) < 4
    for half in range(tiles // 4):
        parts = []
        for part in range(2):
            rows = [
                out[(4 * half + p) * 16 : (4 * half + p + 1) * 16, part * LANES : (part + 1) * LANES]
                for p in range(4)
            ]
            parts.append(swap_blocks(rows))
        for k in range(4):
            owner = k * (tiles // 4) + half
            for pair in range(2):
                re = parts[0][k][pair * 8 : pair * 8 + 8]
                im = parts[1][k][pair * 8 : pair * 8 + 8]
                store(owner, 2 * pair, jnp.where(upper, re, pltpu.roll(im, 4, 0)))
                store(owner, 2 * pair + 1, jnp.where(upper, pltpu.roll(re, 4, 0), im))


def finish_time(rows, line_ref, out_ref, at, own):
    out = split_dot(rows.T, line_ref)
    for part in range(2):
        grid = out[:, part * LANES : (part + 1) * LANES].reshape(4, 4, 8, LANES)
        done = swap_blocks([grid[:, q].reshape(32, LANES) for q in range(4)])
        for f in range(own):
            out_ref[at, f, pl.ds(part, 32, stride=2), :] = done[f]


def peers_of(t, s):
    y, core, z, x = t // 2, t % 2, s // 2, s % 2
    beyond = z // 2
    edge = 3 * (1 - beyond)
    inner = edge + 2 * beyond - 1
    near = beyond * 2 + (z + 1) % 2
    here = y * 2 + x
    first, second = here % 2 * (1 - here // 2), (1 - here % 2) * (here // 2)
    others = ((3 - here) // 3 * 3, 1 + first, 2 + first + second)
    turn = [(here + k) % 4 for k in range(4)]
    head = [0] + [1 + (here + k) % 3 for k in range(3)]
    edges = [beyond * head[k] + (1 - beyond) * turn[k] for k in range(4)]
    inners = [beyond * head[k] + (1 - beyond) * turn[k] for k in range(4)]

    def chip(level, at):
        return [(at // 2 * 2 + (core + dc) % 2, level * 2 + at % 2) for dc in (1, 0)]

    beside = chip(z, others[0]) + chip(z, others[1]) + chip(z, others[2]) + [(y * 2 + 1 - core, s)]
    late = []
    late += [peer for peer in chip(z, others[0])]
    late += [peer for peer in chip(near, head[0])]
    late += [peer for peer in chip(edge, edges[0])]
    late += [peer for peer in chip(near, head[1])]
    late += [peer for peer in chip(z, others[1])]
    late += [peer for peer in chip(near, head[2])]
    late += [peer for peer in chip(z, others[2])]
    late += [peer for peer in chip(near, head[3])]
    late.append((y * 2 + 1 - core, s))
    late += [peer for peer in chip(edge, edges[1])]
    late += [peer for peer in chip(inner, inners[0])]
    late += [peer for peer in chip(edge, edges[2])]
    late += [peer for peer in chip(inner, inners[1])]
    late += [peer for peer in chip(edge, edges[3])]
    late += [peer for peer in chip(inner, inners[2])]
    late += [peer for peer in chip(inner, inners[3])]
    return (edge, inner, near), beside, late


def exchange_kernel(
    tables, tiles, planes, times, sources, names,
    one_hbm, two_hbm, twiddle_hbm, plane_hbm, line_hbm, got, line_out,
    one_ref, two_ref, twiddle_ref, plane_ref, one_wide, two_wide, partial, mixed, send, relay,
    in_sem, table_sem, send_sem, recv_sem, relay_sem, ready,
):
    t, s = lax.axis_index(names[0]), lax.axis_index(names[1])
    barrier = pltpu.get_barrier_semaphore()
    z, x = s // 2, s % 2
    levels, beside, late_peers = peers_of(t, s)
    (edge, inner, near), count, early = levels, times * sources - 1, planes // 2
    column = [(t, level * 2 + x) for level in levels]
    plane_size, late = times * 2, pl.ds(early, planes - early)

    def slot(peer):
        return peer[1] // 2 * plane_size + peer[0] * 2 + peer[1] % 2

    def move(source, target, peer, kind, landed=None):
        return pltpu.make_async_remote_copy(
            src_ref=source,
            dst_ref=target,
            send_sem=send_sem.at[kind],
            recv_sem=recv_sem.at[kind] if landed is None else landed,
            device_id={names[0]: peer[0], names[1]: peer[1]},
            device_id_type=pl.DeviceIdType.MESH,
        )

    def signal(sem, peer):
        pl.semaphore_signal(
            sem, inc=1, device_id={names[0]: peer[0], names[1]: peer[1]}, device_id_type=pl.DeviceIdType.MESH
        )

    def load(p, which):
        source, target = ((one_hbm, one_ref), (two_hbm, two_ref))[which]
        rows = pl.ds(pl.multiple_of(p * 2 * tiles, 2 * tiles), 2 * tiles)
        return pltpu.make_async_copy(source.at[:, :, rows, :], target.at[:, :, rows, :], in_sem.at[which, p])

    table_copies = [
        pltpu.make_async_copy(source, target, table_sem.at[k])
        for k, (source, target) in enumerate(
            ((twiddle_hbm, twiddle_ref), (plane_hbm, plane_ref), (line_hbm, line_out))
        )
    ]
    for which in (1, 0):
        load(0, which).start()
    for peer in column + beside:
        signal(barrier, peer)
    for copy in table_copies[:2]:
        copy.start()
    for which in (1, 0):
        load(1, which).start()

    @pl.loop(0, planes)
    def _(p):
        load(p, 1).wait()
        load(p, 0).wait()

        @pl.when(p == 0)
        def _():
            for later in range(2, planes):
                for which in (1, 0):
                    load(later, which).start()
            table_copies[2].start()

        row = pl.multiple_of(p * 2 * tiles, 2 * tiles)
        widen((two_ref, one_ref), (two_wide, one_wide), row)
        site_sums(tables, one_wide, two_wide, partial, mixed)

        @pl.when(p == 0)
        def _():
            for copy in table_copies[:2]:
                copy.wait()

        def store(owner, group, value):
            send[slot((group, owner)), p, :, :] = value

        plane_blocks(twiddle_ref, plane_ref, mixed, tiles, store)

        @pl.when(p == 0)
        def _():
            pl.semaphore_wait(barrier, len(column + beside))
            for peer in column:
                signal(ready, peer)

        @pl.when(p < early)
        def _():
            for level, peer in zip(levels, column):
                group = pl.ds(level * plane_size, plane_size)
                move(send.at[group, p], relay.at[z, :, p], peer, BULK, relay_sem.at[z]).start()

        got[t * sources + s, p, :, :] = send[slot((t, s)), p, :, :]

    pl.semaphore_wait(ready, len(column))
    for peer in late_peers:
        move(send.at[slot(peer), late], got.at[t * sources + s, late], peer, LATE).start()
    first = pl.ds(0, early)
    for peer in beside:
        move(send.at[slot(peer), first], got.at[t * sources + s, first], peer, AROUND).start()
    for level in (near, edge, inner):
        move(relay.at[level], relay.at[level], column[0], BULK, relay_sem.at[level]).wait_recv()
        here = t * sources + level * 2 + x
        for peer in beside:
            move(relay.at[level, peer[0] * 2 + peer[1] % 2], got.at[here, first], peer, AROUND).start()
        got[here, first, :, :] = relay[level, t * 2 + x, :, :, :]
    table_copies[2].wait()
    for kind, number in ((LATE, count), (AROUND, (len(column) + 1) * len(beside)), (BULK, len(column) * plane_size)):
        span = pl.ds(0, number)
        total = move(send.at[span, first], got.at[span, first], column[0], kind)
        if kind != BULK:
            total.wait_recv()
        total.wait_send()


def finish_kernel(times, own, got, line_ref, out_hbm, out_ref, out_sem):
    copies = []
    for at in range(times):
        span = got.shape[0] // times
        rows = got[at * span : (at + 1) * span].reshape(-1, LANES)
        finish_time(rows, line_ref, out_ref, at, own)
        copy = pltpu.make_async_copy(out_ref.at[at], out_hbm.at[at], out_sem.at[at])
        copy.start()
        copies.append(copy)
    for copy in copies:
        copy.wait()


def fast_device(prop_one, prop_two, times, sources):
    slab = prop_one.shape[-1]
    plane = L * L
    planes, tiles = slab // plane, plane // LANES
    own = 16 // times
    tables = spin_tables()
    twiddle, plane_table = plane_tables(L)
    line = line_table(L, own, sources)

    def paired(prop):
        split = prop.reshape(2, 12, 12, slab // LANES, LANES).transpose(1, 2, 3, 0, 4)
        return split.reshape(12, 12, slab // LANES * 2, LANES)

    anywhere = pl.BlockSpec(memory_space=pltpu.HBM)
    vmem = pl.BlockSpec(memory_space=pltpu.VMEM)
    everyone = times * sources
    inputs = (paired(prop_one), paired(prop_two), twiddle, plane_table, line)
    got, line_near = pl.pallas_call(
        functools.partial(exchange_kernel, tables, tiles, planes, times, sources, ("ta", "xyz")),
        out_shape=(
            pltpu.VMEM((everyone, planes, 8, LANES), jnp.float32),
            pltpu.VMEM(line.shape, line.dtype),
        ),
        in_specs=[anywhere] * len(inputs),
        out_specs=(vmem, vmem),
        scratch_shapes=[
            pltpu.VMEM((12, 12, slab // LANES * 2, LANES), jnp.bfloat16),
            pltpu.VMEM((12, 12, slab // LANES * 2, LANES), jnp.bfloat16),
            pltpu.VMEM(twiddle.shape, twiddle.dtype),
            pltpu.VMEM(plane_table.shape, plane_table.dtype),
            pltpu.VMEM((12, 12, 2 * tiles, LANES), jnp.float32),
            pltpu.VMEM((12, 12, 2 * tiles, LANES), jnp.float32),
            pltpu.VMEM((2, 16, tiles, LANES), jnp.float32),
            pltpu.VMEM((2, 16 * tiles, LANES), jnp.float32),
            pltpu.VMEM((everyone, planes, 8, LANES), jnp.float32),
            pltpu.VMEM((sources // 2, times * 2, planes // 2, 8, LANES), jnp.float32),
            pltpu.SemaphoreType.DMA((2, planes)),
            pltpu.SemaphoreType.DMA((3,)),
            pltpu.SemaphoreType.DMA((3,)),
            pltpu.SemaphoreType.DMA((2,)),
            pltpu.SemaphoreType.DMA((sources // 2,)),
            pltpu.SemaphoreType.REGULAR,
        ],
        compiler_params=pltpu.CompilerParams(
            collective_id=0, has_side_effects=True, vmem_limit_bytes=40 * 2**20
        ),
    )(*[pltpu.with_memory_space_constraint(v, pltpu.HBM) for v in inputs])
    shape = (times, own, slab * 2 // LANES, LANES)
    out = pl.pallas_call(
        functools.partial(finish_kernel, times, own),
        out_shape=jax.ShapeDtypeStruct(shape, jnp.float32),
        in_specs=[vmem, vmem],
        out_specs=anywhere,
        scratch_shapes=[pltpu.VMEM(shape, jnp.float32), pltpu.SemaphoreType.DMA((times,))],
        compiler_params=pltpu.CompilerParams(vmem_limit_bytes=40 * 2**20),
    )(got, line_near)
    return out.reshape(times, own, slab // LANES, 2, LANES).transpose(0, 1, 3, 2, 4).reshape(times, own, 2, slab)


def solution(mesh):
    placed = (P("ta", None, None, None, "xyz"), P("ta", None, None, None, "xyz"))
    times, sources = mesh.shape["ta"], mesh.shape["xyz"]

    def device(prop_one, prop_two):
        planes = prop_one.shape[-1] // (L * L)
        fits = 4 * L == LANES and planes * sources == L and L // sources == 4 and times == 4
        if fits and prop_one.shape[0] == 1:
            return fast_device(prop_one, prop_two, times, sources)
        return on_device(prop_one, prop_two)

    return jax.shard_map(
        device, mesh=mesh, in_specs=placed, out_specs=P(None, "ta", None, "xyz"), check_vma=False
    )
```

```python
import functools
import itertools
import math

import jax
import jax.numpy as jnp
import numpy as np
from jax import lax
from jax.experimental import pallas as pl
from jax.experimental.pallas import tpu as pltpu
from jax.sharding import PartitionSpec as P

L = 32


spin_columns = [[3, 2, 1, 0], [3, 2, 1, 0], [2, 3, 0, 1], [2, 3, 0, 1]]
spin_phases = [[1j, 1j, -1j, -1j], [-1.0, 1.0, 1.0, -1.0], [1j, -1j, -1j, 1j], [1.0, 1.0, 1.0, 1.0]]
chiral_signs = [1.0, 1.0, -1.0, -1.0]


def vertex_parts():
    result = []
    for gamma_index in range(4):
        columns = spin_columns[gamma_index]
        phases = spin_phases[gamma_index]
        rows_list = [columns[a // 3] * 3 + a % 3 for a in range(12)]
        phase_list = [complex(phases[a // 3]) for a in range(12)]
        result.append((rows_list, phase_list))
    return (result, [chiral_signs[a // 3] for a in range(12)])


def contract(prop_a, prop_b):
    gammas, chirality = vertex_parts()
    left_real, left_imag, right_real, right_imag = ([], [], [], [])
    for rows_list, phase_list in gammas:
        pick_real = jnp.stack([prop_a[0, q] for q in rows_list])
        pick_imag = jnp.stack([prop_a[1, q] for q in rows_list])
        phase_real = jnp.asarray(np.array([p.real for p in phase_list]), jnp.bfloat16)[
            :, None, None
        ]
        phase_imag = jnp.asarray(np.array([p.imag for p in phase_list]), jnp.bfloat16)[
            :, None, None
        ]
        left_real.append(phase_real * pick_real - phase_imag * pick_imag)
        left_imag.append(phase_real * pick_imag + phase_imag * pick_real)
        col_real = jnp.stack([prop_b[0][:, q] for q in rows_list], axis=1)
        col_imag = jnp.stack([prop_b[1][:, q] for q in rows_list], axis=1)
        factor = np.array(
            [
                [phase_list[c] * chirality[rows_list[c]] * chirality[a] for c in range(12)]
                for a in range(12)
            ]
        )
        factor_real = jnp.asarray(factor.real, jnp.bfloat16)[:, :, None]
        factor_imag = jnp.asarray(factor.imag, jnp.bfloat16)[:, :, None]
        right_real.append(factor_real * col_real + factor_imag * col_imag)
        right_imag.append(factor_imag * col_real - factor_real * col_imag)
    left_rows = jnp.stack(left_real + left_imag).reshape(8, 144, -1)
    right_rows = jnp.stack(right_real + right_imag).reshape(8, 144, -1)
    products = jnp.einsum("mks,nks->mns", left_rows, right_rows, preferred_element_type=jnp.float32)
    real_sum = products[:4, :4] - products[4:, 4:]
    imag_sum = products[:4, 4:] + products[4:, :4]
    return jnp.stack([real_sum.reshape(16, -1), imag_sum.reshape(16, -1)], axis=1)


def dft_tables(length):
    positions = np.arange(length)
    turn_count = positions[:, None] * positions[None, :] % length
    angles = turn_count * (2.0 * math.pi / length)
    cosines = jnp.asarray(np.cos(angles) / math.sqrt(length), jnp.float32)
    sines = jnp.asarray(np.sin(angles) / math.sqrt(length), jnp.float32)
    return (cosines, sines)


def plane_dft(fields):
    cosines, sines = dft_tables(L)
    highest = lax.Precision.HIGHEST
    shape = fields.shape
    grid = fields.reshape(shape[:4] + (L, L))
    real_part = grid[:, :, 0]
    imag_part = grid[:, :, 1]

    def along_z(values, table):
        return jnp.einsum(
            "tfpyz,zk->tfpyk", values, table, precision=highest, preferred_element_type=jnp.float32
        )

    def along_y(values, table):
        return jnp.einsum(
            "tfpyz,yk->tfpkz", values, table, precision=highest, preferred_element_type=jnp.float32
        )

    mid_real = along_z(real_part, cosines) + along_z(imag_part, sines)
    mid_imag = along_z(imag_part, cosines) - along_z(real_part, sines)
    out_real = along_y(mid_real, cosines) + along_y(mid_imag, sines)
    out_imag = along_y(mid_imag, cosines) - along_y(mid_real, sines)
    return jnp.stack([out_real, out_imag], axis=2).reshape(shape)


def line_dft(data):
    length = data.shape[-2]
    cosines, sines = dft_tables(length)
    real_part = data[..., 0, :, :]
    imag_part = data[..., 1, :, :]

    def transform_rows(values, table):
        return jnp.einsum(
            "...xq,xk->...qk",
            values,
            table,
            precision=lax.Precision.HIGHEST,
            preferred_element_type=jnp.float32,
        )

    out_real = transform_rows(real_part, cosines) + transform_rows(imag_part, sines)
    out_imag = transform_rows(imag_part, cosines) - transform_rows(real_part, sines)
    stacked = jnp.stack([out_real, out_imag], axis=-3)
    return stacked.reshape(stacked.shape[:-2] + (stacked.shape[-2] * stacked.shape[-1],))


def on_device(prop_one, prop_two):
    fields = lax.map(
        lambda slice_pair: contract(slice_pair[0], slice_pair[1]), (prop_one, prop_two)
    )
    local_times, field_count, parts, slab = fields.shape
    planes = slab // (L * L)
    fields = plane_dft(fields.reshape(local_times, field_count, parts, planes, L * L))
    turned_fields = line_dft(lax.all_to_all(fields, "xyz", split_axis=4, concat_axis=3, tiled=True))
    result = lax.all_to_all(turned_fields, "ta", split_axis=1, concat_axis=0, tiled=True)
    return result

LANES = 128
GROUP_PERMS = (0, 2)
LATE, AROUND, BULK = range(3)


def spin_tables():
    chi = np.array(chiral_signs)
    alpha = np.array(spin_phases) * chi[None, :]
    beta = np.array([[spin_phases[n][c] * chi[spin_columns[n][c]] for c in range(4)] for n in range(4)])
    tables = []
    for phases in (alpha, beta):
        pairs = []
        for first in GROUP_PERMS:
            found = []
            for a in range(4):
                for members in found:
                    ratio = phases[first : first + 2, a] / phases[first : first + 2, members[0][0]]
                    if ratio[0] == ratio[1] and ratio[0] in (1, -1):
                        members.append((a, int(ratio[0].real)))
                        break
                else:
                    found.append([(a, 1)])
            assert len(found) == 2
            pairs.append(found)
        lead = np.array([[phases[m, pairs[m // 2][half][0][0]] for half in range(2)] for m in range(4)])
        signs = np.array([[int((lead[m, half] / lead[m, 0]).real) for half in range(2)] for m in range(4)])
        tables.append((pairs, lead[:, 0], signs))
    left, right = tables
    phase = np.outer(left[1], right[1]).reshape(16)
    return left[0], left[2], right[0], right[2], phase


def complex_block(table):
    return np.block([[table.real, table.imag], [-table.imag, table.real]])


def high_low(table):
    high = np.asarray(table).astype(jnp.bfloat16)
    low = (table - high.astype(np.float64)).astype(jnp.bfloat16)
    return jnp.asarray(np.stack([high, low]))


def plane_tables(length):
    quarter = LANES // length
    outer = length // quarter
    lane = np.arange(LANES)
    y, z = lane // length, lane % length
    twiddle = np.exp(-2j * np.pi * np.outer(np.arange(outer), y) / length)
    ky, slot = lane // length, lane % length
    kz = (slot % outer) * quarter + slot // outer
    table = np.exp(-2j * np.pi * (np.outer(y, ky) / quarter + np.outer(z, kz) / length)) / length
    return (
        jnp.asarray(np.stack([twiddle.real, twiddle.imag]), jnp.float32),
        high_low(complex_block(table)),
    )


def line_table(length, own, sources):
    x = np.arange(length)
    turn = np.exp(-2j * np.pi * np.outer(x, x) / length) / math.sqrt(length)
    parts = complex_block(turn).reshape(2, sources, length // sources, 2, length)
    full = np.einsum("asxbk,fg->sxafbgk", parts, np.eye(own))
    rows = length * 2 * own
    return high_low(full.reshape(rows, rows))


def split_dot(values, table):
    high = values.astype(jnp.bfloat16)
    low = (values - high.astype(jnp.float32)).astype(jnp.bfloat16)

    def dot(a, b):
        return jnp.dot(a, b, preferred_element_type=jnp.float32)

    return dot(high, table[0]) + (dot(low, table[0]) + dot(high, table[1]))


def small_fft(values):
    count = len(values)
    if count == 1:
        return values
    even, odd = small_fft(values[0::2]), small_fft(values[1::2])
    low, high = [], []
    for k in range(count // 2):
        re, im = odd[k]
        if k == 0:
            pass
        elif 4 * k == count:
            re, im = im, -re
        else:
            c, s = math.cos(2 * math.pi * k / count), math.sin(2 * math.pi * k / count)
            re, im = c * re + s * im, c * im - s * re
        low.append((even[k][0] + re, even[k][1] + im))
        high.append((even[k][0] - re, even[k][1] - im))
    return low + high


def swap_blocks(values):
    width = LANES // 4
    shape = values[0].shape
    axis = len(shape) - 1
    block = lax.broadcasted_iota(jnp.int32, shape, axis) // width
    low, even = block < 2, block % 2 == 0
    values = list(values)
    for i in range(2):
        first, second = values[i], values[i + 2]
        moved = pltpu.roll(jnp.where(low, second, first), 2 * width, axis)
        values[i], values[i + 2] = jnp.where(low, first, moved), jnp.where(low, moved, second)
    for i in (0, 2):
        first, second = values[i], values[i + 1]
        values[i] = jnp.where(even, first, pltpu.roll(second, width, axis))
        values[i + 1] = jnp.where(even, pltpu.roll(first, LANES - width, axis), second)
    return values


def add_signed(total, term, sign):
    if total is None:
        return term if sign > 0 else -term
    return total + term if sign > 0 else total - term


def widen(sources, targets, row):
    rows = targets[0].shape[2]

    @pl.loop(0, 12)
    def _(sink):
        for c in range(12):
            for source, target in zip(sources, targets):
                target[sink, c, :, :] = source[sink, c, pl.ds(row, rows), :].astype(jnp.float32)


def site_sums(tables, one, two, partial, mixed):
    left_groups, left_signs, right_groups, right_signs, phases = tables
    tiles = one.shape[2] // 2
    columns = [spin_columns[first] for first in GROUP_PERMS]
    left_of = [{a: (half, sign) for half in range(2) for a, sign in left_groups[pair][half]} for pair in range(2)]
    right_of = [{c: (side, sign) for side in range(2) for c, sign in right_groups[turn][side]} for turn in range(2)]

    def read(ref, at, kind, sign):
        first, second = (ref[at[0], at[1], pl.ds(part, tiles, stride=2), :] if kind in (part, 2) else None for part in range(2))
        if kind < 2:
            return second if kind else first
        return first + second if sign > 0 else first - second

    def blocks(kind):
        def step(i, sums):
            sums = list(sums)
            for j, q_first, c_first in itertools.product(range(3), (0, 2), (0, 2)):
                ones = {
                    (q, c): read(one, (q * 3 + i, c * 3 + j), kind, 1)
                    for q in (q_first, q_first + 1)
                    for c in (c_first, c_first + 1)
                }
                twos = {}
                for q, c in ones:
                    for pair in range(2):
                        for turn in range(2):
                            at = (columns[pair][q], columns[turn][c])
                            if at not in twos:
                                twos[at] = read(two, (at[0] * 3 + i, at[1] * 3 + j), kind, -1)
                for q, c in ones:
                    for pair in range(2):
                        half, left_sign = left_of[pair][columns[pair][q]]
                        for turn in range(2):
                            side, right_sign = right_of[turn][c]
                            k = ((pair * 2 + half) * 2 + turn) * 2 + side
                            term = ones[q, c] * twos[columns[pair][q], columns[turn][c]]
                            sums[k] = add_signed(sums[k], term, left_sign * right_sign)
            return tuple(sums)

        start = tuple(jnp.zeros((tiles, LANES), jnp.float32) for _ in range(16))
        return lax.fori_loop(0, 3, step, start)

    for kind in range(2):
        for k, total in enumerate(blocks(kind)):
            partial[kind, k, :, :] = total
    both = blocks(2)
    for pair in range(2):
        for turn in range(2):
            quads = ([], [])
            for half in range(2):
                for side in range(2):
                    k = ((pair * 2 + half) * 2 + turn) * 2 + side
                    straight, crossed = partial[0, k, :, :], partial[1, k, :, :]
                    quads[0].append(straight + crossed)
                    quads[1].append(both[k] - (straight - crossed))
            for nu in (2 * turn, 2 * turn + 1):
                joined = []
                for quad in quads:
                    for half in range(2):
                        total = add_signed(None, quad[2 * half], int(right_signs[nu][0]))
                        joined.append(add_signed(total, quad[2 * half + 1], int(right_signs[nu][1])))
                for mu in (2 * pair, 2 * pair + 1):
                    field = 4 * mu + nu
                    phase = phases[field]
                    for part in range(2):
                        sign = (phase.real + phase.imag) * (-1 if part and phase.imag else 1)
                        total = add_signed(None, joined[2 * part], int(left_signs[mu][0] * sign))
                        total = add_signed(total, joined[2 * part + 1], int(left_signs[mu][1] * sign))
                        where = 1 - part if phase.imag else part
                        mixed[where, field * tiles : (field + 1) * tiles, :] = total


def plane_blocks(twiddle_ref, plane_ref, mixed, tiles, store):
    blocks = [tuple(mixed[part, pl.ds(t, 16, stride=tiles), :] for part in range(2)) for t in range(tiles)]
    spectrum = small_fft(blocks)
    turned = []
    for k, (re, im) in enumerate(spectrum):
        c = twiddle_ref[0, k : k + 1, :]
        s = twiddle_ref[1, k : k + 1, :]
        turned.append(jnp.concatenate([re * c - im * s, re * s + im * c], axis=1) if k else jnp.concatenate([re, im], axis=1))
    out = split_dot(jnp.concatenate(turned, axis=0), plane_ref)
    upper = lax.broadcasted_iota(jnp.int32, (8, LANES), 0) < 4
    for half in range(tiles // 4):
        parts = []
        for part in range(2):
            rows = [
                out[(4 * half + p) * 16 : (4 * half + p + 1) * 16, part * LANES : (part + 1) * LANES]
                for p in range(4)
            ]
            parts.append(swap_blocks(rows))
        for k in range(4):
            owner = k * (tiles // 4) + half
            for pair in range(2):
                re = parts[0][k][pair * 8 : pair * 8 + 8]
                im = parts[1][k][pair * 8 : pair * 8 + 8]
                store(owner, 2 * pair, jnp.where(upper, re, pltpu.roll(im, 4, 0)))
                store(owner, 2 * pair + 1, jnp.where(upper, pltpu.roll(re, 4, 0), im))


def finish_time(rows, line_ref, out_ref, at, own):
    out = split_dot(rows.T, line_ref)
    for part in range(2):
        grid = out[:, part * LANES : (part + 1) * LANES].reshape(4, 4, 8, LANES)
        done = swap_blocks([grid[:, q].reshape(32, LANES) for q in range(4)])
        for f in range(own):
            out_ref[at, f, pl.ds(part, 32, stride=2), :] = done[f]


def peers_of(t, s):
    y, core, z, x = t // 2, t % 2, s // 2, s % 2
    beyond = z // 2
    edge = 3 * (1 - beyond)
    inner = edge + 2 * beyond - 1
    near = beyond * 2 + (z + 1) % 2
    here = y * 2 + x
    first, second = here % 2 * (1 - here // 2), (1 - here % 2) * (here // 2)
    others = ((3 - here) // 3 * 3, 1 + first, 2 + first + second)
    turn = [(here + k) % 4 for k in range(4)]
    head = [0] + [1 + (here + k) % 3 for k in range(3)]
    edges = [beyond * head[k] + (1 - beyond) * turn[k] for k in range(4)]
    inners = [beyond * head[k] + (1 - beyond) * turn[k] for k in range(4)]

    def chip(level, at):
        return [(at // 2 * 2 + (core + dc) % 2, level * 2 + at % 2) for dc in (1, 0)]

    beside = chip(z, others[0]) + chip(z, others[1]) + chip(z, others[2]) + [(y * 2 + 1 - core, s)]
    late = []
    late += [peer for peer in chip(z, others[0])]
    late += [peer for peer in chip(near, head[0])]
    late += [peer for peer in chip(edge, edges[0])]
    late += [peer for peer in chip(near, head[1])]
    late += [peer for peer in chip(z, others[1])]
    late += [peer for peer in chip(near, head[2])]
    late += [peer for peer in chip(z, others[2])]
    late += [peer for peer in chip(near, head[3])]
    late.append((y * 2 + 1 - core, s))
    late += [peer for peer in chip(edge, edges[1])]
    late += [peer for peer in chip(inner, inners[0])]
    late += [peer for peer in chip(edge, edges[2])]
    late += [peer for peer in chip(inner, inners[1])]
    late += [peer for peer in chip(edge, edges[3])]
    late += [peer for peer in chip(inner, inners[2])]
    late += [peer for peer in chip(inner, inners[3])]
    return (edge, inner, near), beside, late


def exchange_kernel(
    tables, tiles, planes, times, sources, names,
    one_hbm, two_hbm, twiddle_hbm, plane_hbm, line_hbm, got, line_out,
    one_ref, two_ref, twiddle_ref, plane_ref, one_wide, two_wide, partial, mixed, send, relay,
    in_sem, table_sem, send_sem, recv_sem, relay_sem, ready,
):
    t, s = lax.axis_index(names[0]), lax.axis_index(names[1])
    barrier = pltpu.get_barrier_semaphore()
    z, x = s // 2, s % 2
    levels, beside, late_peers = peers_of(t, s)
    (edge, inner, near), count, early = levels, times * sources - 1, planes // 2
    levels = (near, edge, inner)
    column = [(t, level * 2 + x) for level in levels]
    plane_size, late = times * 2, pl.ds(early, planes - early)

    def slot(peer):
        return peer[1] // 2 * plane_size + peer[0] * 2 + peer[1] % 2

    def move(source, target, peer, kind, landed=None):
        return pltpu.make_async_remote_copy(
            src_ref=source,
            dst_ref=target,
            send_sem=send_sem.at[kind],
            recv_sem=recv_sem.at[kind] if landed is None else landed,
            device_id={names[0]: peer[0], names[1]: peer[1]},
            device_id_type=pl.DeviceIdType.MESH,
        )

    def signal(sem, peer):
        pl.semaphore_signal(
            sem, inc=1, device_id={names[0]: peer[0], names[1]: peer[1]}, device_id_type=pl.DeviceIdType.MESH
        )

    def load(p, which):
        source, target = ((one_hbm, one_ref), (two_hbm, two_ref))[which]
        rows = pl.ds(pl.multiple_of(p * 2 * tiles, 2 * tiles), 2 * tiles)
        return pltpu.make_async_copy(source.at[:, :, rows, :], target.at[:, :, rows, :], in_sem.at[which, p])

    table_copies = [
        pltpu.make_async_copy(source, target, table_sem.at[k])
        for k, (source, target) in enumerate(
            ((twiddle_hbm, twiddle_ref), (plane_hbm, plane_ref), (line_hbm, line_out))
        )
    ]
    for which in (1, 0):
        load(0, which).start()
    for peer in column + beside:
        signal(barrier, peer)
    for copy in table_copies[:2]:
        copy.start()
    for which in (1, 0):
        load(1, which).start()

    @pl.loop(0, planes)
    def _(p):
        load(p, 1).wait()
        load(p, 0).wait()

        @pl.when(p == 0)
        def _():
            for later in range(2, planes):
                for which in (1, 0):
                    load(later, which).start()
            table_copies[2].start()

        row = pl.multiple_of(p * 2 * tiles, 2 * tiles)
        widen((two_ref, one_ref), (two_wide, one_wide), row)
        site_sums(tables, one_wide, two_wide, partial, mixed)

        @pl.when(p == 0)
        def _():
            for copy in table_copies[:2]:
                copy.wait()

        def store(owner, group, value):
            send[slot((group, owner)), p, :, :] = value

        plane_blocks(twiddle_ref, plane_ref, mixed, tiles, store)

        @pl.when(p == 0)
        def _():
            pl.semaphore_wait(barrier, len(column + beside))
            for peer in column:
                signal(ready, peer)

        @pl.when(p < early)
        def _():
            for level, peer in zip(levels, column):
                group = pl.ds(level * plane_size, plane_size)
                move(send.at[group, p], relay.at[z, :, p], peer, BULK, relay_sem.at[z]).start()

        got[t * sources + s, p, :, :] = send[slot((t, s)), p, :, :]

    pl.semaphore_wait(ready, len(column))
    for peer in late_peers:
        move(send.at[slot(peer), late], got.at[t * sources + s, late], peer, LATE).start()
    first = pl.ds(0, early)
    for peer in beside:
        move(send.at[slot(peer), first], got.at[t * sources + s, first], peer, AROUND).start()
    for level in (near, edge, inner):
        move(relay.at[level], relay.at[level], column[0], BULK, relay_sem.at[level]).wait_recv()
        here = t * sources + level * 2 + x
        for peer in beside:
            move(relay.at[level, peer[0] * 2 + peer[1] % 2], got.at[here, first], peer, AROUND).start()
        got[here, first, :, :] = relay[level, t * 2 + x, :, :, :]
    table_copies[2].wait()
    for kind, number in ((LATE, count), (AROUND, (len(column) + 1) * len(beside)), (BULK, len(column) * plane_size)):
        span = pl.ds(0, number)
        total = move(send.at[span, first], got.at[span, first], column[0], kind)
        if kind != BULK:
            total.wait_recv()
        total.wait_send()


def finish_kernel(times, own, got, line_ref, out_hbm, out_ref, out_sem):
    copies = []
    for at in range(times):
        span = got.shape[0] // times
        rows = got[at * span : (at + 1) * span].reshape(-1, LANES)
        finish_time(rows, line_ref, out_ref, at, own)
        copy = pltpu.make_async_copy(out_ref.at[at], out_hbm.at[at], out_sem.at[at])
        copy.start()
        copies.append(copy)
    for copy in copies:
        copy.wait()


def fast_device(prop_one, prop_two, times, sources):
    slab = prop_one.shape[-1]
    plane = L * L
    planes, tiles = slab // plane, plane // LANES
    own = 16 // times
    tables = spin_tables()
    twiddle, plane_table = plane_tables(L)
    line = line_table(L, own, sources)

    def paired(prop):
        split = prop.reshape(2, 12, 12, slab // LANES, LANES).transpose(1, 2, 3, 0, 4)
        return split.reshape(12, 12, slab // LANES * 2, LANES)

    anywhere = pl.BlockSpec(memory_space=pltpu.HBM)
    vmem = pl.BlockSpec(memory_space=pltpu.VMEM)
    everyone = times * sources
    inputs = (paired(prop_one), paired(prop_two), twiddle, plane_table, line)
    got, line_near = pl.pallas_call(
        functools.partial(exchange_kernel, tables, tiles, planes, times, sources, ("ta", "xyz")),
        out_shape=(
            pltpu.VMEM((everyone, planes, 8, LANES), jnp.float32),
            pltpu.VMEM(line.shape, line.dtype),
        ),
        in_specs=[anywhere] * len(inputs),
        out_specs=(vmem, vmem),
        scratch_shapes=[
            pltpu.VMEM((12, 12, slab // LANES * 2, LANES), jnp.bfloat16),
            pltpu.VMEM((12, 12, slab // LANES * 2, LANES), jnp.bfloat16),
            pltpu.VMEM(twiddle.shape, twiddle.dtype),
            pltpu.VMEM(plane_table.shape, plane_table.dtype),
            pltpu.VMEM((12, 12, 2 * tiles, LANES), jnp.float32),
            pltpu.VMEM((12, 12, 2 * tiles, LANES), jnp.float32),
            pltpu.VMEM((2, 16, tiles, LANES), jnp.float32),
            pltpu.VMEM((2, 16 * tiles, LANES), jnp.float32),
            pltpu.VMEM((everyone, planes, 8, LANES), jnp.float32),
            pltpu.VMEM((sources // 2, times * 2, planes // 2, 8, LANES), jnp.float32),
            pltpu.SemaphoreType.DMA((2, planes)),
            pltpu.SemaphoreType.DMA((3,)),
            pltpu.SemaphoreType.DMA((3,)),
            pltpu.SemaphoreType.DMA((2,)),
            pltpu.SemaphoreType.DMA((sources // 2,)),
            pltpu.SemaphoreType.REGULAR,
        ],
        compiler_params=pltpu.CompilerParams(
            collective_id=0, has_side_effects=True, vmem_limit_bytes=40 * 2**20
        ),
    )(*[pltpu.with_memory_space_constraint(v, pltpu.HBM) for v in inputs])
    shape = (times, own, slab * 2 // LANES, LANES)
    out = pl.pallas_call(
        functools.partial(finish_kernel, times, own),
        out_shape=jax.ShapeDtypeStruct(shape, jnp.float32),
        in_specs=[vmem, vmem],
        out_specs=anywhere,
        scratch_shapes=[pltpu.VMEM(shape, jnp.float32), pltpu.SemaphoreType.DMA((times,))],
        compiler_params=pltpu.CompilerParams(vmem_limit_bytes=40 * 2**20),
    )(got, line_near)
    return out.reshape(times, own, slab // LANES, 2, LANES).transpose(0, 1, 3, 2, 4).reshape(times, own, 2, slab)


def solution(mesh):
    placed = (P("ta", None, None, None, "xyz"), P("ta", None, None, None, "xyz"))
    times, sources = mesh.shape["ta"], mesh.shape["xyz"]

    def device(prop_one, prop_two):
        planes = prop_one.shape[-1] // (L * L)
        fits = 4 * L == LANES and planes * sources == L and L // sources == 4 and times == 4
        if fits and prop_one.shape[0] == 1:
            return fast_device(prop_one, prop_two, times, sources)
        return on_device(prop_one, prop_two)

    return jax.shard_map(
        device, mesh=mesh, in_specs=placed, out_specs=P(None, "ta", None, "xyz"), check_vma=False
    )
```

```python
import functools
import itertools
import math

import jax
import jax.numpy as jnp
import numpy as np
from jax import lax
from jax.experimental import pallas as pl
from jax.experimental.pallas import tpu as pltpu
from jax.sharding import PartitionSpec as P

L = 32


spin_columns = [[3, 2, 1, 0], [3, 2, 1, 0], [2, 3, 0, 1], [2, 3, 0, 1]]
spin_phases = [[1j, 1j, -1j, -1j], [-1.0, 1.0, 1.0, -1.0], [1j, -1j, -1j, 1j], [1.0, 1.0, 1.0, 1.0]]
chiral_signs = [1.0, 1.0, -1.0, -1.0]


def vertex_parts():
    result = []
    for gamma_index in range(4):
        columns = spin_columns[gamma_index]
        phases = spin_phases[gamma_index]
        rows_list = [columns[a // 3] * 3 + a % 3 for a in range(12)]
        phase_list = [complex(phases[a // 3]) for a in range(12)]
        result.append((rows_list, phase_list))
    return (result, [chiral_signs[a // 3] for a in range(12)])


def contract(prop_a, prop_b):
    gammas, chirality = vertex_parts()
    left_real, left_imag, right_real, right_imag = ([], [], [], [])
    for rows_list, phase_list in gammas:
        pick_real = jnp.stack([prop_a[0, q] for q in rows_list])
        pick_imag = jnp.stack([prop_a[1, q] for q in rows_list])
        phase_real = jnp.asarray(np.array([p.real for p in phase_list]), jnp.bfloat16)[
            :, None, None
        ]
        phase_imag = jnp.asarray(np.array([p.imag for p in phase_list]), jnp.bfloat16)[
            :, None, None
        ]
        left_real.append(phase_real * pick_real - phase_imag * pick_imag)
        left_imag.append(phase_real * pick_imag + phase_imag * pick_real)
        col_real = jnp.stack([prop_b[0][:, q] for q in rows_list], axis=1)
        col_imag = jnp.stack([prop_b[1][:, q] for q in rows_list], axis=1)
        factor = np.array(
            [
                [phase_list[c] * chirality[rows_list[c]] * chirality[a] for c in range(12)]
                for a in range(12)
            ]
        )
        factor_real = jnp.asarray(factor.real, jnp.bfloat16)[:, :, None]
        factor_imag = jnp.asarray(factor.imag, jnp.bfloat16)[:, :, None]
        right_real.append(factor_real * col_real + factor_imag * col_imag)
        right_imag.append(factor_imag * col_real - factor_real * col_imag)
    left_rows = jnp.stack(left_real + left_imag).reshape(8, 144, -1)
    right_rows = jnp.stack(right_real + right_imag).reshape(8, 144, -1)
    products = jnp.einsum("mks,nks->mns", left_rows, right_rows, preferred_element_type=jnp.float32)
    real_sum = products[:4, :4] - products[4:, 4:]
    imag_sum = products[:4, 4:] + products[4:, :4]
    return jnp.stack([real_sum.reshape(16, -1), imag_sum.reshape(16, -1)], axis=1)


def dft_tables(length):
    positions = np.arange(length)
    turn_count = positions[:, None] * positions[None, :] % length
    angles = turn_count * (2.0 * math.pi / length)
    cosines = jnp.asarray(np.cos(angles) / math.sqrt(length), jnp.float32)
    sines = jnp.asarray(np.sin(angles) / math.sqrt(length), jnp.float32)
    return (cosines, sines)


def plane_dft(fields):
    cosines, sines = dft_tables(L)
    highest = lax.Precision.HIGHEST
    shape = fields.shape
    grid = fields.reshape(shape[:4] + (L, L))
    real_part = grid[:, :, 0]
    imag_part = grid[:, :, 1]

    def along_z(values, table):
        return jnp.einsum(
            "tfpyz,zk->tfpyk", values, table, precision=highest, preferred_element_type=jnp.float32
        )

    def along_y(values, table):
        return jnp.einsum(
            "tfpyz,yk->tfpkz", values, table, precision=highest, preferred_element_type=jnp.float32
        )

    mid_real = along_z(real_part, cosines) + along_z(imag_part, sines)
    mid_imag = along_z(imag_part, cosines) - along_z(real_part, sines)
    out_real = along_y(mid_real, cosines) + along_y(mid_imag, sines)
    out_imag = along_y(mid_imag, cosines) - along_y(mid_real, sines)
    return jnp.stack([out_real, out_imag], axis=2).reshape(shape)


def line_dft(data):
    length = data.shape[-2]
    cosines, sines = dft_tables(length)
    real_part = data[..., 0, :, :]
    imag_part = data[..., 1, :, :]

    def transform_rows(values, table):
        return jnp.einsum(
            "...xq,xk->...qk",
            values,
            table,
            precision=lax.Precision.HIGHEST,
            preferred_element_type=jnp.float32,
        )

    out_real = transform_rows(real_part, cosines) + transform_rows(imag_part, sines)
    out_imag = transform_rows(imag_part, cosines) - transform_rows(real_part, sines)
    stacked = jnp.stack([out_real, out_imag], axis=-3)
    return stacked.reshape(stacked.shape[:-2] + (stacked.shape[-2] * stacked.shape[-1],))


def on_device(prop_one, prop_two):
    fields = lax.map(
        lambda slice_pair: contract(slice_pair[0], slice_pair[1]), (prop_one, prop_two)
    )
    local_times, field_count, parts, slab = fields.shape
    planes = slab // (L * L)
    fields = plane_dft(fields.reshape(local_times, field_count, parts, planes, L * L))
    turned_fields = line_dft(lax.all_to_all(fields, "xyz", split_axis=4, concat_axis=3, tiled=True))
    result = lax.all_to_all(turned_fields, "ta", split_axis=1, concat_axis=0, tiled=True)
    return result

LANES = 128
GROUP_PERMS = (0, 2)
LATE, AROUND, BULK = range(3)
TOGETHER = 2


def spin_tables():
    chi = np.array(chiral_signs)
    alpha = np.array(spin_phases) * chi[None, :]
    beta = np.array([[spin_phases[n][c] * chi[spin_columns[n][c]] for c in range(4)] for n in range(4)])
    tables = []
    for phases in (alpha, beta):
        pairs = []
        for first in GROUP_PERMS:
            found = []
            for a in range(4):
                for members in found:
                    ratio = phases[first : first + 2, a] / phases[first : first + 2, members[0][0]]
                    if ratio[0] == ratio[1] and ratio[0] in (1, -1):
                        members.append((a, int(ratio[0].real)))
                        break
                else:
                    found.append([(a, 1)])
            assert len(found) == 2
            pairs.append(found)
        lead = np.array([[phases[m, pairs[m // 2][half][0][0]] for half in range(2)] for m in range(4)])
        signs = np.array([[int((lead[m, half] / lead[m, 0]).real) for half in range(2)] for m in range(4)])
        tables.append((pairs, lead[:, 0], signs))
    left, right = tables
    phase = np.outer(left[1], right[1]).reshape(16)
    return left[0], left[2], right[0], right[2], phase


def complex_block(table):
    return np.block([[table.real, table.imag], [-table.imag, table.real]])


def high_low(table):
    high = np.asarray(table).astype(jnp.bfloat16)
    low = (table - high.astype(np.float64)).astype(jnp.bfloat16)
    return jnp.asarray(np.stack([high, low]))


def plane_tables(length):
    quarter = LANES // length
    outer = length // quarter
    lane = np.arange(LANES)
    y, z = lane // length, lane % length
    twiddle = np.exp(-2j * np.pi * np.outer(np.arange(outer), y) / length)
    ky, slot = lane // length, lane % length
    kz = (slot % outer) * quarter + slot // outer
    table = np.exp(-2j * np.pi * (np.outer(y, ky) / quarter + np.outer(z, kz) / length)) / length
    return (
        jnp.asarray(np.stack([twiddle.real, twiddle.imag]), jnp.float32),
        high_low(complex_block(table)),
    )


def line_table(length, own, sources):
    x = np.arange(length)
    turn = np.exp(-2j * np.pi * np.outer(x, x) / length) / math.sqrt(length)
    parts = complex_block(turn).reshape(2, sources, length // sources, 2, length)
    full = np.einsum("asxbk,fg->sxafbgk", parts, np.eye(own))
    rows = length * 2 * own
    full = full.reshape(rows, 2, rows // 2)
    moved = np.roll(full, length, axis=2)
    return jnp.concatenate([high_low(full.reshape(rows, rows)), high_low(moved.reshape(rows, rows))])


def split_dot(values, table):
    high = values.astype(jnp.bfloat16)
    low = (values - high.astype(jnp.float32)).astype(jnp.bfloat16)

    def dot(a, b):
        return jnp.dot(a, b, preferred_element_type=jnp.float32)

    return dot(high, table[0]) + (dot(low, table[0]) + dot(high, table[1]))


def small_fft(values):
    count = len(values)
    if count == 1:
        return values
    even, odd = small_fft(values[0::2]), small_fft(values[1::2])
    low, high = [], []
    for k in range(count // 2):
        re, im = odd[k]
        if k == 0:
            pass
        elif 4 * k == count:
            re, im = im, -re
        else:
            c, s = math.cos(2 * math.pi * k / count), math.sin(2 * math.pi * k / count)
            re, im = c * re + s * im, c * im - s * re
        low.append((even[k][0] + re, even[k][1] + im))
        high.append((even[k][0] - re, even[k][1] - im))
    return low + high


def swap_blocks(values):
    width = LANES // 4
    shape = values[0].shape
    axis = len(shape) - 1
    block = lax.broadcasted_iota(jnp.int32, shape, axis) // width
    low, even = block < 2, block % 2 == 0
    values = list(values)
    for i in range(2):
        first, second = values[i], values[i + 2]
        moved = pltpu.roll(jnp.where(low, second, first), 2 * width, axis)
        values[i], values[i + 2] = jnp.where(low, first, moved), jnp.where(low, moved, second)
    for i in (0, 2):
        first, second = values[i], values[i + 1]
        values[i] = jnp.where(even, first, pltpu.roll(second, width, axis))
        values[i + 1] = jnp.where(even, pltpu.roll(first, LANES - width, axis), second)
    return values


def add_signed(total, term, sign):
    if total is None:
        return term if sign > 0 else -term
    return total + term if sign > 0 else total - term


def widen(sources, targets, row):
    rows = targets[0].shape[2]

    @pl.loop(0, 12)
    def _(sink):
        for c in range(12):
            for source, target in zip(sources, targets):
                target[sink, c, :, :] = source[sink, c, pl.ds(row, rows), :].astype(jnp.float32)


def site_sums(tables, one, two, partial, mixed):
    left_groups, left_signs, right_groups, right_signs, phases = tables
    tiles = one.shape[2] // 2
    columns = [spin_columns[first] for first in GROUP_PERMS]
    left_of = [{a: (half, sign) for half in range(2) for a, sign in left_groups[pair][half]} for pair in range(2)]
    right_of = [{c: (side, sign) for side in range(2) for c, sign in right_groups[turn][side]} for turn in range(2)]

    def read(ref, at, kind, sign):
        first, second = (ref[at[0], at[1], pl.ds(part, tiles, stride=2), :] if kind in (part, 2) else None for part in range(2))
        if kind < 2:
            return second if kind else first
        return first + second if sign > 0 else first - second

    def blocks(kind):
        def step(i, sums):
            sums = list(sums)
            for j, q_first, c_first in itertools.product(range(3), (0, 2), (0, 2)):
                ones = {
                    (q, c): read(one, (q * 3 + i, c * 3 + j), kind, 1)
                    for q in (q_first, q_first + 1)
                    for c in (c_first, c_first + 1)
                }
                twos = {}
                for q, c in ones:
                    for pair in range(2):
                        for turn in range(2):
                            at = (columns[pair][q], columns[turn][c])
                            if at not in twos:
                                twos[at] = read(two, (at[0] * 3 + i, at[1] * 3 + j), kind, -1)
                for q, c in ones:
                    for pair in range(2):
                        half, left_sign = left_of[pair][columns[pair][q]]
                        for turn in range(2):
                            side, right_sign = right_of[turn][c]
                            k = ((pair * 2 + half) * 2 + turn) * 2 + side
                            term = ones[q, c] * twos[columns[pair][q], columns[turn][c]]
                            sums[k] = add_signed(sums[k], term, left_sign * right_sign)
            return tuple(sums)

        start = tuple(jnp.zeros((tiles, LANES), jnp.float32) for _ in range(16))
        return lax.fori_loop(0, 3, step, start)

    for kind in range(2):
        for k, total in enumerate(blocks(kind)):
            partial[kind, k, :, :] = total
    both = blocks(2)
    for pair in range(2):
        for turn in range(2):
            quads = ([], [])
            for half in range(2):
                for side in range(2):
                    k = ((pair * 2 + half) * 2 + turn) * 2 + side
                    straight, crossed = partial[0, k, :, :], partial[1, k, :, :]
                    quads[0].append(straight + crossed)
                    quads[1].append(both[k] - (straight - crossed))
            for nu in (2 * turn, 2 * turn + 1):
                joined = []
                for quad in quads:
                    for half in range(2):
                        total = add_signed(None, quad[2 * half], int(right_signs[nu][0]))
                        joined.append(add_signed(total, quad[2 * half + 1], int(right_signs[nu][1])))
                for mu in (2 * pair, 2 * pair + 1):
                    field = 4 * mu + nu
                    phase = phases[field]
                    for part in range(2):
                        sign = (phase.real + phase.imag) * (-1 if part and phase.imag else 1)
                        total = add_signed(None, joined[2 * part], int(left_signs[mu][0] * sign))
                        total = add_signed(total, joined[2 * part + 1], int(left_signs[mu][1] * sign))
                        where = 1 - part if phase.imag else part
                        mixed[where, field * tiles : (field + 1) * tiles, :] = total


def plane_blocks(twiddle_ref, plane_ref, mixed, tiles, store):
    blocks = [tuple(mixed[part, pl.ds(t, 16, stride=tiles), :] for part in range(2)) for t in range(tiles)]
    spectrum = small_fft(blocks)
    turned = []
    for k, (re, im) in enumerate(spectrum):
        c = twiddle_ref[0, k : k + 1, :]
        s = twiddle_ref[1, k : k + 1, :]
        turned.append(jnp.concatenate([re * c - im * s, re * s + im * c], axis=1) if k else jnp.concatenate([re, im], axis=1))
    out = split_dot(jnp.concatenate(turned, axis=0), plane_ref)
    upper = lax.broadcasted_iota(jnp.int32, (8, LANES), 0) < 4
    for half in range(tiles // 4):
        parts = []
        for part in range(2):
            rows = [
                out[(4 * half + p) * 16 : (4 * half + p + 1) * 16, part * LANES : (part + 1) * LANES]
                for p in range(4)
            ]
            parts.append(swap_blocks(rows))
        for k in range(4):
            owner = k * (tiles // 4) + half
            for pair in range(2):
                re = parts[0][k][pair * 8 : pair * 8 + 8]
                im = parts[1][k][pair * 8 : pair * 8 + 8]
                store(owner, 2 * pair, jnp.where(upper, re, pltpu.roll(im, 4, 0)))
                store(owner, 2 * pair + 1, jnp.where(upper, pltpu.roll(re, 4, 0), im))


def finish_times(blocks, line_ref, out_ref, first, own):
    operands = ([], [])
    for rows in blocks:
        grid = rows.T.reshape(4, 4, 8, -1)
        for q in range(4):
            operands[q % 2].append(grid[:, q].reshape(32, -1))
    out = [split_dot(jnp.concatenate(operands[k], axis=0), (line_ref[2 * k], line_ref[2 * k + 1])) for k in range(2)]
    block = lax.broadcasted_iota(jnp.int32, (32, LANES), 1) // L
    low, even = block < 2, block % 2 == 0
    for at in range(len(blocks)):
        for part in range(2):
            lanes = slice(part * LANES, (part + 1) * LANES)
            pairs = []
            for half in range(2):
                start = (2 * at + half) * 32
                plain, moved = (out[k][start : start + 32, lanes] for k in range(2))
                crossed = pltpu.roll(jnp.where(even, moved, plain), LANES - L, 1)
                pairs.append((jnp.where(even, plain, moved), crossed))
            for f in range(2):
                left, right = pairs[0][f], pairs[1][f]
                swapped = pltpu.roll(jnp.where(low, right, left), LANES // 2, 1)
                out_ref[first + at, f, pl.ds(part, 32, stride=2), :] = jnp.where(low, left, swapped)
                out_ref[first + at, f + 2, pl.ds(part, 32, stride=2), :] = jnp.where(low, swapped, right)


def levels_of(s):
    z = s // 2
    beyond = z // 2
    edge = 3 * (1 - beyond)
    return edge, edge + 2 * beyond - 1, beyond * 2 + (z + 1) % 2


def chip(core, level, at):
    return [(at // 2 * 2 + (core + dc) % 2, level * 2 + at % 2) for dc in (1, 0)]


def others_of(t, s):
    here = t // 2 * 2 + s % 2
    first, second = here % 2 * (1 - here // 2), (1 - here % 2) * (here // 2)
    return (3 - here) // 3 * 3, 1 + first, 2 + first + second


def beside_of(t, s):
    return [peer for at in others_of(t, s) for peer in chip(t % 2, s // 2, at)] + [(t // 2 * 2 + 1 - t % 2, s)]


def late_of(t, s):
    y, core, z, x = t // 2, t % 2, s // 2, s % 2
    beyond = z // 2
    edge, inner, near = levels_of(s)
    here = y * 2 + x
    others = others_of(t, s)
    turn = [(here + k) % 4 for k in range(4)]
    head = [0] + [1 + (here + k) % 3 for k in range(3)]
    edges = inners = [beyond * head[k] + (1 - beyond) * turn[k] for k in range(4)]
    late = []
    late += [peer for peer in chip(core, z, others[0])]
    late += [peer for peer in chip(core, near, head[0])]
    late += [peer for peer in chip(core, edge, edges[0])]
    late += [peer for peer in chip(core, near, head[1])]
    late += [peer for peer in chip(core, z, others[1])]
    late += [peer for peer in chip(core, near, head[2])]
    late += [peer for peer in chip(core, z, others[2])]
    late += [peer for peer in chip(core, near, head[3])]
    late.append((y * 2 + 1 - core, s))
    late += [peer for peer in chip(core, edge, edges[1])]
    late += [peer for peer in chip(core, inner, inners[0])]
    late += [peer for peer in chip(core, edge, edges[2])]
    late += [peer for peer in chip(core, inner, inners[1])]
    late += [peer for peer in chip(core, edge, edges[3])]
    late += [peer for peer in chip(core, inner, inners[2])]
    late += [peer for peer in chip(core, inner, inners[3])]
    return late


def exchange_kernel(
    tables, tiles, planes, times, sources, names,
    one_hbm, two_hbm, twiddle_hbm, plane_hbm, line_hbm, got, line_out,
    one_ref, two_ref, twiddle_ref, plane_ref, one_wide, two_wide, partial, mixed, send, relay,
    in_sem, table_sem, send_sem, recv_sem, relay_sem, ready,
):
    def load(p, which):
        source, target = ((one_hbm, one_ref), (two_hbm, two_ref))[which]
        rows = pl.ds(pl.multiple_of(p * 2 * tiles, 2 * tiles), 2 * tiles)
        return pltpu.make_async_copy(source.at[:, :, rows, :], target.at[:, :, rows, :], in_sem.at[which, p])

    @pl.loop(0, 2)
    def _(p):
        for which in (1, 0):
            load(p, which).start()

    t, s = lax.axis_index(names[0]), lax.axis_index(names[1])
    barrier = pltpu.get_barrier_semaphore()
    z, x = s // 2, s % 2
    edge, inner, near = levels_of(s)
    levels, count, early = (near, edge, inner), times * sources - 1, planes // 2
    column = [(t, level * 2 + x) for level in levels]
    beside = beside_of(t, s)
    plane_size, late = times * 2, pl.ds(early, planes - early)

    def slot(peer):
        return peer[1] // 2 * plane_size + peer[0] * 2 + peer[1] % 2

    def move(source, target, peer, kind, landed=None):
        return pltpu.make_async_remote_copy(
            src_ref=source,
            dst_ref=target,
            send_sem=send_sem.at[kind],
            recv_sem=recv_sem.at[kind] if landed is None else landed,
            device_id={names[0]: peer[0], names[1]: peer[1]},
            device_id_type=pl.DeviceIdType.MESH,
        )

    def signal(sem, peer):
        pl.semaphore_signal(
            sem, inc=1, device_id={names[0]: peer[0], names[1]: peer[1]}, device_id_type=pl.DeviceIdType.MESH
        )

    table_copies = [
        pltpu.make_async_copy(source, target, table_sem.at[k])
        for k, (source, target) in enumerate(
            ((twiddle_hbm, twiddle_ref), (plane_hbm, plane_ref), (line_hbm, line_out))
        )
    ]
    for peer in column + beside:
        signal(barrier, peer)
    for copy in table_copies[:2]:
        copy.start()
    late_peers = [(peer, slot(peer)) for peer in late_of(t, s)]
    beside_slots = [(peer, slot(peer)) for peer in beside]
    mine = t * sources + s

    @pl.loop(0, planes)
    def _(p):
        load(p, 1).wait()
        load(p, 0).wait()

        @pl.when(p == 0)
        def _():
            for later in range(2, planes):
                for which in (1, 0):
                    load(later, which).start()
            table_copies[2].start()

        row = pl.multiple_of(p * 2 * tiles, 2 * tiles)
        widen((two_ref, one_ref), (two_wide, one_wide), row)
        site_sums(tables, one_wide, two_wide, partial, mixed)

        @pl.when(p == 0)
        def _():
            for copy in table_copies[:2]:
                copy.wait()

        def store(owner, group, value):
            send[slot((group, owner)), p, :, :] = value

        plane_blocks(twiddle_ref, plane_ref, mixed, tiles, store)

        @pl.when(p == 0)
        def _():
            pl.semaphore_wait(barrier, len(column + beside))
            for peer in column:
                signal(ready, peer)

        @pl.when(p < early)
        def _():
            for level, peer in zip(levels, column):
                group = pl.ds(level * plane_size, plane_size)
                move(send.at[group, p], relay.at[z, :, p], peer, BULK, relay_sem.at[z]).start()

        got[t * sources + s, p, :, :] = send[slot((t, s)), p, :, :]

    pl.semaphore_wait(ready, len(column))
    for peer, at in late_peers:
        move(send.at[at, late], got.at[mine, late], peer, LATE).start()
    first = pl.ds(0, early)
    for peer, at in beside_slots:
        move(send.at[at, first], got.at[mine, first], peer, AROUND).start()
    for level in (near, edge, inner):
        move(relay.at[level], relay.at[level], column[0], BULK, relay_sem.at[level]).wait_recv()
        here = t * sources + level * 2 + x
        for peer in beside:
            move(relay.at[level, peer[0] * 2 + peer[1] % 2], got.at[here, first], peer, AROUND).start()
        got[here, first, :, :] = relay[level, t * 2 + x, :, :, :]
    table_copies[2].wait()
    for kind, number in ((LATE, count), (AROUND, (len(column) + 1) * len(beside)), (BULK, len(column) * plane_size)):
        span = pl.ds(0, number)
        total = move(send.at[span, first], got.at[span, first], column[0], kind)
        if kind != BULK:
            total.wait_recv()
        total.wait_send()


def finish_kernel(times, own, got, line_ref, out_hbm, out_ref, out_sem):
    copies = []
    span = got.shape[0] // times
    for first in range(0, times, TOGETHER):
        blocks = [got[at * span : (at + 1) * span].reshape(-1, LANES) for at in range(first, first + TOGETHER)]
        finish_times(blocks, line_ref, out_ref, first, own)
        for at in range(first, first + TOGETHER):
            copy = pltpu.make_async_copy(out_ref.at[at], out_hbm.at[at], out_sem.at[at])
            copy.start()
            copies.append(copy)
    for copy in copies:
        copy.wait()


def fast_device(prop_one, prop_two, times, sources):
    slab = prop_one.shape[-1]
    plane = L * L
    planes, tiles = slab // plane, plane // LANES
    own = 16 // times
    tables = spin_tables()
    twiddle, plane_table = plane_tables(L)
    line = line_table(L, own, sources)

    def paired(prop):
        split = prop.reshape(2, 12, 12, slab // LANES, LANES).transpose(1, 2, 3, 0, 4)
        return split.reshape(12, 12, slab // LANES * 2, LANES)

    anywhere = pl.BlockSpec(memory_space=pltpu.HBM)
    vmem = pl.BlockSpec(memory_space=pltpu.VMEM)
    everyone = times * sources
    inputs = (paired(prop_one), paired(prop_two), twiddle, plane_table, line)
    got, line_near = pl.pallas_call(
        functools.partial(exchange_kernel, tables, tiles, planes, times, sources, ("ta", "xyz")),
        out_shape=(
            pltpu.VMEM((everyone, planes, 8, LANES), jnp.float32),
            pltpu.VMEM(line.shape, line.dtype),
        ),
        in_specs=[anywhere] * len(inputs),
        out_specs=(vmem, vmem),
        scratch_shapes=[
            pltpu.VMEM((12, 12, slab // LANES * 2, LANES), jnp.bfloat16),
            pltpu.VMEM((12, 12, slab // LANES * 2, LANES), jnp.bfloat16),
            pltpu.VMEM(twiddle.shape, twiddle.dtype),
            pltpu.VMEM(plane_table.shape, plane_table.dtype),
            pltpu.VMEM((12, 12, 2 * tiles, LANES), jnp.float32),
            pltpu.VMEM((12, 12, 2 * tiles, LANES), jnp.float32),
            pltpu.VMEM((2, 16, tiles, LANES), jnp.float32),
            pltpu.VMEM((2, 16 * tiles, LANES), jnp.float32),
            pltpu.VMEM((everyone, planes, 8, LANES), jnp.float32),
            pltpu.VMEM((sources // 2, times * 2, planes // 2, 8, LANES), jnp.float32),
            pltpu.SemaphoreType.DMA((2, planes)),
            pltpu.SemaphoreType.DMA((3,)),
            pltpu.SemaphoreType.DMA((3,)),
            pltpu.SemaphoreType.DMA((2,)),
            pltpu.SemaphoreType.DMA((sources // 2,)),
            pltpu.SemaphoreType.REGULAR,
        ],
        compiler_params=pltpu.CompilerParams(
            collective_id=0, has_side_effects=True, vmem_limit_bytes=40 * 2**20
        ),
    )(*[pltpu.with_memory_space_constraint(v, pltpu.HBM) for v in inputs])
    shape = (times, own, slab * 2 // LANES, LANES)
    out = pl.pallas_call(
        functools.partial(finish_kernel, times, own),
        out_shape=jax.ShapeDtypeStruct(shape, jnp.float32),
        in_specs=[vmem, vmem],
        out_specs=anywhere,
        scratch_shapes=[pltpu.VMEM(shape, jnp.float32), pltpu.SemaphoreType.DMA((times,))],
        compiler_params=pltpu.CompilerParams(vmem_limit_bytes=40 * 2**20),
    )(got, line_near)
    return out.reshape(times, own, slab // LANES, 2, LANES).transpose(0, 1, 3, 2, 4).reshape(times, own, 2, slab)


def solution(mesh):
    placed = (P("ta", None, None, None, "xyz"), P("ta", None, None, None, "xyz"))
    times, sources = mesh.shape["ta"], mesh.shape["xyz"]

    def device(prop_one, prop_two):
        planes = prop_one.shape[-1] // (L * L)
        fits = 4 * L == LANES and planes * sources == L and L // sources == 4 and times == 4
        if fits and prop_one.shape[0] == 1:
            return fast_device(prop_one, prop_two, times, sources)
        return on_device(prop_one, prop_two)

    return jax.shard_map(
        device, mesh=mesh, in_specs=placed, out_specs=P(None, "ta", None, "xyz"), check_vma=False
    )
```

```python
import functools
import itertools
import math

import jax
import jax.numpy as jnp
import numpy as np
from jax import lax
from jax.experimental import pallas as pl
from jax.experimental.pallas import tpu as pltpu
from jax.sharding import PartitionSpec as P

L = 32


spin_columns = [[3, 2, 1, 0], [3, 2, 1, 0], [2, 3, 0, 1], [2, 3, 0, 1]]
spin_phases = [[1j, 1j, -1j, -1j], [-1.0, 1.0, 1.0, -1.0], [1j, -1j, -1j, 1j], [1.0, 1.0, 1.0, 1.0]]
chiral_signs = [1.0, 1.0, -1.0, -1.0]


def vertex_parts():
    result = []
    for gamma_index in range(4):
        columns = spin_columns[gamma_index]
        phases = spin_phases[gamma_index]
        rows_list = [columns[a // 3] * 3 + a % 3 for a in range(12)]
        phase_list = [complex(phases[a // 3]) for a in range(12)]
        result.append((rows_list, phase_list))
    return (result, [chiral_signs[a // 3] for a in range(12)])


def contract(prop_a, prop_b):
    gammas, chirality = vertex_parts()
    left_real, left_imag, right_real, right_imag = ([], [], [], [])
    for rows_list, phase_list in gammas:
        pick_real = jnp.stack([prop_a[0, q] for q in rows_list])
        pick_imag = jnp.stack([prop_a[1, q] for q in rows_list])
        phase_real = jnp.asarray(np.array([p.real for p in phase_list]), jnp.bfloat16)[
            :, None, None
        ]
        phase_imag = jnp.asarray(np.array([p.imag for p in phase_list]), jnp.bfloat16)[
            :, None, None
        ]
        left_real.append(phase_real * pick_real - phase_imag * pick_imag)
        left_imag.append(phase_real * pick_imag + phase_imag * pick_real)
        col_real = jnp.stack([prop_b[0][:, q] for q in rows_list], axis=1)
        col_imag = jnp.stack([prop_b[1][:, q] for q in rows_list], axis=1)
        factor = np.array(
            [
                [phase_list[c] * chirality[rows_list[c]] * chirality[a] for c in range(12)]
                for a in range(12)
            ]
        )
        factor_real = jnp.asarray(factor.real, jnp.bfloat16)[:, :, None]
        factor_imag = jnp.asarray(factor.imag, jnp.bfloat16)[:, :, None]
        right_real.append(factor_real * col_real + factor_imag * col_imag)
        right_imag.append(factor_imag * col_real - factor_real * col_imag)
    left_rows = jnp.stack(left_real + left_imag).reshape(8, 144, -1)
    right_rows = jnp.stack(right_real + right_imag).reshape(8, 144, -1)
    products = jnp.einsum("mks,nks->mns", left_rows, right_rows, preferred_element_type=jnp.float32)
    real_sum = products[:4, :4] - products[4:, 4:]
    imag_sum = products[:4, 4:] + products[4:, :4]
    return jnp.stack([real_sum.reshape(16, -1), imag_sum.reshape(16, -1)], axis=1)


def dft_tables(length):
    positions = np.arange(length)
    turn_count = positions[:, None] * positions[None, :] % length
    angles = turn_count * (2.0 * math.pi / length)
    cosines = jnp.asarray(np.cos(angles) / math.sqrt(length), jnp.float32)
    sines = jnp.asarray(np.sin(angles) / math.sqrt(length), jnp.float32)
    return (cosines, sines)


def plane_dft(fields):
    cosines, sines = dft_tables(L)
    highest = lax.Precision.HIGHEST
    shape = fields.shape
    grid = fields.reshape(shape[:4] + (L, L))
    real_part = grid[:, :, 0]
    imag_part = grid[:, :, 1]

    def along_z(values, table):
        return jnp.einsum(
            "tfpyz,zk->tfpyk", values, table, precision=highest, preferred_element_type=jnp.float32
        )

    def along_y(values, table):
        return jnp.einsum(
            "tfpyz,yk->tfpkz", values, table, precision=highest, preferred_element_type=jnp.float32
        )

    mid_real = along_z(real_part, cosines) + along_z(imag_part, sines)
    mid_imag = along_z(imag_part, cosines) - along_z(real_part, sines)
    out_real = along_y(mid_real, cosines) + along_y(mid_imag, sines)
    out_imag = along_y(mid_imag, cosines) - along_y(mid_real, sines)
    return jnp.stack([out_real, out_imag], axis=2).reshape(shape)


def line_dft(data):
    length = data.shape[-2]
    cosines, sines = dft_tables(length)
    real_part = data[..., 0, :, :]
    imag_part = data[..., 1, :, :]

    def transform_rows(values, table):
        return jnp.einsum(
            "...xq,xk->...qk",
            values,
            table,
            precision=lax.Precision.HIGHEST,
            preferred_element_type=jnp.float32,
        )

    out_real = transform_rows(real_part, cosines) + transform_rows(imag_part, sines)
    out_imag = transform_rows(imag_part, cosines) - transform_rows(real_part, sines)
    stacked = jnp.stack([out_real, out_imag], axis=-3)
    return stacked.reshape(stacked.shape[:-2] + (stacked.shape[-2] * stacked.shape[-1],))


def on_device(prop_one, prop_two):
    fields = lax.map(
        lambda slice_pair: contract(slice_pair[0], slice_pair[1]), (prop_one, prop_two)
    )
    local_times, field_count, parts, slab = fields.shape
    planes = slab // (L * L)
    fields = plane_dft(fields.reshape(local_times, field_count, parts, planes, L * L))
    turned_fields = line_dft(lax.all_to_all(fields, "xyz", split_axis=4, concat_axis=3, tiled=True))
    result = lax.all_to_all(turned_fields, "ta", split_axis=1, concat_axis=0, tiled=True)
    return result

LANES = 128
GROUP_PERMS = (0, 2)
LATE, AROUND, BULK = range(3)
TOGETHER = 2


def spin_tables():
    chi = np.array(chiral_signs)
    alpha = np.array(spin_phases) * chi[None, :]
    beta = np.array([[spin_phases[n][c] * chi[spin_columns[n][c]] for c in range(4)] for n in range(4)])
    tables = []
    for phases in (alpha, beta):
        pairs = []
        for first in GROUP_PERMS:
            found = []
            for a in range(4):
                for members in found:
                    ratio = phases[first : first + 2, a] / phases[first : first + 2, members[0][0]]
                    if ratio[0] == ratio[1] and ratio[0] in (1, -1):
                        members.append((a, int(ratio[0].real)))
                        break
                else:
                    found.append([(a, 1)])
            assert len(found) == 2
            pairs.append(found)
        lead = np.array([[phases[m, pairs[m // 2][half][0][0]] for half in range(2)] for m in range(4)])
        signs = np.array([[int((lead[m, half] / lead[m, 0]).real) for half in range(2)] for m in range(4)])
        tables.append((pairs, lead[:, 0], signs))
    left, right = tables
    phase = np.outer(left[1], right[1]).reshape(16)
    return left[0], left[2], right[0], right[2], phase


def complex_block(table):
    return np.block([[table.real, table.imag], [-table.imag, table.real]])


def high_low(table):
    high = np.asarray(table).astype(jnp.bfloat16)
    low = (table - high.astype(np.float64)).astype(jnp.bfloat16)
    return jnp.asarray(np.stack([high, low]))


def plane_tables(length):
    quarter = LANES // length
    outer = length // quarter
    lane = np.arange(LANES)
    y, z = lane // length, lane % length
    twiddle = np.exp(-2j * np.pi * np.outer(np.arange(outer), y) / length)
    ky, slot = lane // length, lane % length
    kz = (slot % outer) * quarter + slot // outer
    table = np.exp(-2j * np.pi * (np.outer(y, ky) / quarter + np.outer(z, kz) / length)) / length
    return (
        jnp.asarray(np.stack([twiddle.real, twiddle.imag]), jnp.float32),
        high_low(complex_block(table)),
    )


def line_table(length, own, sources):
    x = np.arange(length)
    turn = np.exp(-2j * np.pi * np.outer(x, x) / length) / math.sqrt(length)
    parts = complex_block(turn).reshape(2, sources, length // sources, 2, length)
    full = np.einsum("asxbk,fg->sxafbgk", parts, np.eye(own))
    rows = length * 2 * own
    full = full.reshape(rows, 2, rows // 2)
    moved = np.roll(full, length, axis=2)
    return jnp.concatenate([high_low(full.reshape(rows, rows)), high_low(moved.reshape(rows, rows))])


def split_dot(values, table):
    high = values.astype(jnp.bfloat16)
    low = (values - high.astype(jnp.float32)).astype(jnp.bfloat16)

    def dot(a, b):
        return jnp.dot(a, b, preferred_element_type=jnp.float32)

    return dot(high, table[0]) + (dot(low, table[0]) + dot(high, table[1]))


def small_fft(values):
    count = len(values)
    if count == 1:
        return values
    even, odd = small_fft(values[0::2]), small_fft(values[1::2])
    low, high = [], []
    for k in range(count // 2):
        re, im = odd[k]
        if k == 0:
            pass
        elif 4 * k == count:
            re, im = im, -re
        else:
            c, s = math.cos(2 * math.pi * k / count), math.sin(2 * math.pi * k / count)
            re, im = c * re + s * im, c * im - s * re
        low.append((even[k][0] + re, even[k][1] + im))
        high.append((even[k][0] - re, even[k][1] - im))
    return low + high


def swap_blocks(values):
    width = LANES // 4
    shape = values[0].shape
    axis = len(shape) - 1
    block = lax.broadcasted_iota(jnp.int32, shape, axis) // width
    low, even = block < 2, block % 2 == 0
    values = list(values)
    for i in range(2):
        first, second = values[i], values[i + 2]
        moved = pltpu.roll(jnp.where(low, second, first), 2 * width, axis)
        values[i], values[i + 2] = jnp.where(low, first, moved), jnp.where(low, moved, second)
    for i in (0, 2):
        first, second = values[i], values[i + 1]
        values[i] = jnp.where(even, first, pltpu.roll(second, width, axis))
        values[i + 1] = jnp.where(even, pltpu.roll(first, LANES - width, axis), second)
    return values


def add_signed(total, term, sign):
    if total is None:
        return term if sign > 0 else -term
    return total + term if sign > 0 else total - term


def widen(sources, targets, row):
    rows = targets[0].shape[2]

    @pl.loop(0, 12)
    def _(sink):
        for c in range(12):
            for source, target in zip(sources, targets):
                target[sink, c, :, :] = source[sink, c, pl.ds(row, rows), :].astype(jnp.float32)


def site_sums(tables, one, two, partial, mixed):
    left_groups, left_signs, right_groups, right_signs, phases = tables
    tiles = one.shape[2] // 2
    columns = [spin_columns[first] for first in GROUP_PERMS]
    left_of = [{a: (half, sign) for half in range(2) for a, sign in left_groups[pair][half]} for pair in range(2)]
    right_of = [{c: (side, sign) for side in range(2) for c, sign in right_groups[turn][side]} for turn in range(2)]

    def read(ref, at, kind, sign):
        first, second = (ref[at[0], at[1], pl.ds(part, tiles, stride=2), :] if kind in (part, 2) else None for part in range(2))
        if kind < 2:
            return second if kind else first
        return first + second if sign > 0 else first - second

    def blocks(kind):
        def step(i, sums):
            sums = list(sums)
            for j, q_first, c_first in itertools.product(range(3), (0, 2), (0, 2)):
                ones = {
                    (q, c): read(one, (q * 3 + i, c * 3 + j), kind, 1)
                    for q in (q_first, q_first + 1)
                    for c in (c_first, c_first + 1)
                }
                twos = {}
                for q, c in ones:
                    for pair in range(2):
                        for turn in range(2):
                            at = (columns[pair][q], columns[turn][c])
                            if at not in twos:
                                twos[at] = read(two, (at[0] * 3 + i, at[1] * 3 + j), kind, -1)
                for q, c in ones:
                    for pair in range(2):
                        half, left_sign = left_of[pair][columns[pair][q]]
                        for turn in range(2):
                            side, right_sign = right_of[turn][c]
                            k = ((pair * 2 + half) * 2 + turn) * 2 + side
                            term = ones[q, c] * twos[columns[pair][q], columns[turn][c]]
                            sums[k] = add_signed(sums[k], term, left_sign * right_sign)
            return tuple(sums)

        start = tuple(jnp.zeros((tiles, LANES), jnp.float32) for _ in range(16))
        return lax.fori_loop(0, 3, step, start)

    for kind in range(2):
        for k, total in enumerate(blocks(kind)):
            partial[kind, k, :, :] = total
    both = blocks(2)
    for pair in range(2):
        for turn in range(2):
            quads = ([], [])
            for half in range(2):
                for side in range(2):
                    k = ((pair * 2 + half) * 2 + turn) * 2 + side
                    straight, crossed = partial[0, k, :, :], partial[1, k, :, :]
                    quads[0].append(straight + crossed)
                    quads[1].append(both[k] - (straight - crossed))
            for nu in (2 * turn, 2 * turn + 1):
                joined = []
                for quad in quads:
                    for half in range(2):
                        total = add_signed(None, quad[2 * half], int(right_signs[nu][0]))
                        joined.append(add_signed(total, quad[2 * half + 1], int(right_signs[nu][1])))
                for mu in (2 * pair, 2 * pair + 1):
                    field = 4 * mu + nu
                    phase = phases[field]
                    for part in range(2):
                        sign = (phase.real + phase.imag) * (-1 if part and phase.imag else 1)
                        total = add_signed(None, joined[2 * part], int(left_signs[mu][0] * sign))
                        total = add_signed(total, joined[2 * part + 1], int(left_signs[mu][1] * sign))
                        where = 1 - part if phase.imag else part
                        mixed[where, field * tiles : (field + 1) * tiles, :] = total


def plane_blocks(twiddle_ref, plane_ref, mixed, tiles, store):
    blocks = [tuple(mixed[part, pl.ds(t, 16, stride=tiles), :] for part in range(2)) for t in range(tiles)]
    spectrum = small_fft(blocks)
    turned = []
    for k, (re, im) in enumerate(spectrum):
        c = twiddle_ref[0, k : k + 1, :]
        s = twiddle_ref[1, k : k + 1, :]
        turned.append(jnp.concatenate([re * c - im * s, re * s + im * c], axis=1) if k else jnp.concatenate([re, im], axis=1))
    out = split_dot(jnp.concatenate(turned, axis=0), plane_ref)
    upper = lax.broadcasted_iota(jnp.int32, (8, LANES), 0) < 4
    for half in range(tiles // 4):
        parts = []
        for part in range(2):
            rows = [
                out[(4 * half + p) * 16 : (4 * half + p + 1) * 16, part * LANES : (part + 1) * LANES]
                for p in range(4)
            ]
            parts.append(swap_blocks(rows))
        for k in range(4):
            owner = k * (tiles // 4) + half
            for pair in range(2):
                re = parts[0][k][pair * 8 : pair * 8 + 8]
                im = parts[1][k][pair * 8 : pair * 8 + 8]
                store(owner, 2 * pair, jnp.where(upper, re, pltpu.roll(im, 4, 0)))
                store(owner, 2 * pair + 1, jnp.where(upper, pltpu.roll(re, 4, 0), im))


def finish_times(blocks, line_ref, out_ref, first, own):
    operands = ([], [])
    for rows in blocks:
        grid = rows.T.reshape(4, 4, 8, -1)
        for q in range(4):
            operands[q % 2].append(grid[:, q].reshape(32, -1))
    out = [split_dot(jnp.concatenate(operands[k], axis=0), (line_ref[2 * k], line_ref[2 * k + 1])) for k in range(2)]
    block = lax.broadcasted_iota(jnp.int32, (32, LANES), 1) // L
    low, even = block < 2, block % 2 == 0
    for at in range(len(blocks)):
        for part in range(2):
            lanes = slice(part * LANES, (part + 1) * LANES)
            pairs = []
            for half in range(2):
                start = (2 * at + half) * 32
                plain, moved = (out[k][start : start + 32, lanes] for k in range(2))
                crossed = pltpu.roll(jnp.where(even, moved, plain), LANES - L, 1)
                pairs.append((jnp.where(even, plain, moved), crossed))
            for f in range(2):
                left, right = pairs[0][f], pairs[1][f]
                swapped = pltpu.roll(jnp.where(low, right, left), LANES // 2, 1)
                out_ref[first + at, f, pl.ds(part, 32, stride=2), :] = jnp.where(low, left, swapped)
                out_ref[first + at, f + 2, pl.ds(part, 32, stride=2), :] = jnp.where(low, swapped, right)


def levels_of(s):
    z = s // 2
    beyond = z // 2
    edge = 3 * (1 - beyond)
    return edge, edge + 2 * beyond - 1, beyond * 2 + (z + 1) % 2


def chip(core, level, at):
    return [(at // 2 * 2 + (core + dc) % 2, level * 2 + at % 2) for dc in (1, 0)]


def others_of(t, s):
    here = t // 2 * 2 + s % 2
    first, second = here % 2 * (1 - here // 2), (1 - here % 2) * (here // 2)
    return (3 - here) // 3 * 3, 1 + first, 2 + first + second


def beside_of(t, s):
    return [peer for at in others_of(t, s) for peer in chip(t % 2, s // 2, at)] + [(t // 2 * 2 + 1 - t % 2, s)]


def late_of(t, s):
    y, core, z, x = t // 2, t % 2, s // 2, s % 2
    beyond = z // 2
    edge, inner, near = levels_of(s)
    here = y * 2 + x
    others = others_of(t, s)
    turn = [(here + k) % 4 for k in range(4)]
    head = [0] + [1 + (here + k) % 3 for k in range(3)]
    edges = inners = [beyond * head[k] + (1 - beyond) * turn[k] for k in range(4)]
    late = []
    late += [peer for peer in chip(core, z, others[0])]
    late += [peer for peer in chip(core, near, head[0])]
    late += [peer for peer in chip(core, edge, edges[0])]
    late += [peer for peer in chip(core, near, head[1])]
    late += [peer for peer in chip(core, z, others[1])]
    late += [peer for peer in chip(core, near, head[2])]
    late += [peer for peer in chip(core, z, others[2])]
    late += [peer for peer in chip(core, near, head[3])]
    late.append((y * 2 + 1 - core, s))
    late += [peer for peer in chip(core, edge, edges[1])]
    late += [peer for peer in chip(core, inner, inners[0])]
    late += [peer for peer in chip(core, edge, edges[2])]
    late += [peer for peer in chip(core, inner, inners[1])]
    late += [peer for peer in chip(core, edge, edges[3])]
    late += [peer for peer in chip(core, inner, inners[2])]
    late += [peer for peer in chip(core, inner, inners[3])]
    return late


def exchange_kernel(
    tables, tiles, planes, times, sources, names,
    one_hbm, two_hbm, twiddle_hbm, plane_hbm, line_hbm, got, line_out,
    one_ref, two_ref, twiddle_ref, plane_ref, one_wide, two_wide, partial, mixed, send, relay,
    in_sem, table_sem, send_sem, recv_sem, relay_sem, ready,
):
    def load(p, which):
        source, target = ((one_hbm, one_ref), (two_hbm, two_ref))[which]
        rows = pl.ds(pl.multiple_of(p * 2 * tiles, 2 * tiles), 2 * tiles)
        return pltpu.make_async_copy(source.at[:, :, rows, :], target.at[:, :, rows, :], in_sem.at[which, p])

    @pl.loop(0, 2)
    def _(p):
        for which in (1, 0):
            load(p, which).start()

    t, s = lax.axis_index(names[0]), lax.axis_index(names[1])
    barrier = pltpu.get_barrier_semaphore()
    z, x = s // 2, s % 2
    edge, inner, near = levels_of(s)
    levels, count, early = (near, edge, inner), times * sources - 1, planes // 2
    column = [(t, level * 2 + x) for level in levels]
    beside = beside_of(t, s)
    plane_size, late = times * 2, pl.ds(early, planes - early)

    def slot(peer):
        return peer[1] // 2 * plane_size + peer[0] * 2 + peer[1] % 2

    def move(source, target, peer, kind, landed=None):
        return pltpu.make_async_remote_copy(
            src_ref=source,
            dst_ref=target,
            send_sem=send_sem.at[kind],
            recv_sem=recv_sem.at[kind] if landed is None else landed,
            device_id={names[0]: peer[0], names[1]: peer[1]},
            device_id_type=pl.DeviceIdType.MESH,
        )

    def signal(sem, peer):
        pl.semaphore_signal(
            sem, inc=1, device_id={names[0]: peer[0], names[1]: peer[1]}, device_id_type=pl.DeviceIdType.MESH
        )

    table_copies = [
        pltpu.make_async_copy(source, target, table_sem.at[k])
        for k, (source, target) in enumerate(
            ((twiddle_hbm, twiddle_ref), (plane_hbm, plane_ref), (line_hbm, line_out))
        )
    ]
    for peer in column + beside:
        signal(barrier, peer)
    for copy in table_copies[:2]:
        copy.start()
    late_peers = [(peer, slot(peer)) for peer in late_of(t, s)]
    beside_slots = [(peer, slot(peer)) for peer in beside]
    mine = t * sources + s

    @pl.loop(0, planes)
    def _(p):
        load(p, 1).wait()
        load(p, 0).wait()

        @pl.when(p == 0)
        def _():
            for later in range(2, planes):
                for which in (1, 0):
                    load(later, which).start()
            table_copies[2].start()

        row = pl.multiple_of(p * 2 * tiles, 2 * tiles)
        widen((two_ref, one_ref), (two_wide, one_wide), row)
        site_sums(tables, one_wide, two_wide, partial, mixed)

        @pl.when(p == 0)
        def _():
            for copy in table_copies[:2]:
                copy.wait()

        def store(owner, group, value):
            send[slot((group, owner)), p, :, :] = value

        plane_blocks(twiddle_ref, plane_ref, mixed, tiles, store)

        @pl.when(p == 0)
        def _():
            pl.semaphore_wait(barrier, len(column + beside))
            for peer in column:
                signal(ready, peer)

        @pl.when(p < early)
        def _():
            for level, peer in zip(levels, column):
                group = pl.ds(level * plane_size, plane_size)
                move(send.at[group, p], relay.at[z, :, p], peer, BULK, relay_sem.at[z]).start()

        got[t * sources + s, p, :, :] = send[slot((t, s)), p, :, :]

    pl.semaphore_wait(ready, len(column))
    first = pl.ds(0, early)
    for peer, at in beside_slots:
        move(send.at[at, first], got.at[mine, first], peer, AROUND).start()
    for peer, at in late_peers:
        move(send.at[at, late], got.at[mine, late], peer, LATE).start()
    for level in (near, edge, inner):
        move(relay.at[level], relay.at[level], column[0], BULK, relay_sem.at[level]).wait_recv()
        here = t * sources + level * 2 + x
        for peer in beside:
            move(relay.at[level, peer[0] * 2 + peer[1] % 2], got.at[here, first], peer, AROUND).start()
        got[here, first, :, :] = relay[level, t * 2 + x, :, :, :]
    table_copies[2].wait()
    for kind, number in ((LATE, count), (AROUND, (len(column) + 1) * len(beside)), (BULK, len(column) * plane_size)):
        span = pl.ds(0, number)
        total = move(send.at[span, first], got.at[span, first], column[0], kind)
        if kind != BULK:
            total.wait_recv()
        total.wait_send()


def finish_kernel(times, own, got, line_ref, out_hbm, out_ref, out_sem):
    copies = []
    span = got.shape[0] // times
    for first in range(0, times, TOGETHER):
        blocks = [got[at * span : (at + 1) * span].reshape(-1, LANES) for at in range(first, first + TOGETHER)]
        finish_times(blocks, line_ref, out_ref, first, own)
        for at in range(first, first + TOGETHER):
            copy = pltpu.make_async_copy(out_ref.at[at], out_hbm.at[at], out_sem.at[at])
            copy.start()
            copies.append(copy)
    for copy in copies:
        copy.wait()


def fast_device(prop_one, prop_two, times, sources):
    slab = prop_one.shape[-1]
    plane = L * L
    planes, tiles = slab // plane, plane // LANES
    own = 16 // times
    tables = spin_tables()
    twiddle, plane_table = plane_tables(L)
    line = line_table(L, own, sources)

    def paired(prop):
        split = prop.reshape(2, 12, 12, slab // LANES, LANES).transpose(1, 2, 3, 0, 4)
        return split.reshape(12, 12, slab // LANES * 2, LANES)

    anywhere = pl.BlockSpec(memory_space=pltpu.HBM)
    vmem = pl.BlockSpec(memory_space=pltpu.VMEM)
    everyone = times * sources
    inputs = (paired(prop_one), paired(prop_two), twiddle, plane_table, line)
    got, line_near = pl.pallas_call(
        functools.partial(exchange_kernel, tables, tiles, planes, times, sources, ("ta", "xyz")),
        out_shape=(
            pltpu.VMEM((everyone, planes, 8, LANES), jnp.float32),
            pltpu.VMEM(line.shape, line.dtype),
        ),
        in_specs=[anywhere] * len(inputs),
        out_specs=(vmem, vmem),
        scratch_shapes=[
            pltpu.VMEM((12, 12, slab // LANES * 2, LANES), jnp.bfloat16),
            pltpu.VMEM((12, 12, slab // LANES * 2, LANES), jnp.bfloat16),
            pltpu.VMEM(twiddle.shape, twiddle.dtype),
            pltpu.VMEM(plane_table.shape, plane_table.dtype),
            pltpu.VMEM((12, 12, 2 * tiles, LANES), jnp.float32),
            pltpu.VMEM((12, 12, 2 * tiles, LANES), jnp.float32),
            pltpu.VMEM((2, 16, tiles, LANES), jnp.float32),
            pltpu.VMEM((2, 16 * tiles, LANES), jnp.float32),
            pltpu.VMEM((everyone, planes, 8, LANES), jnp.float32),
            pltpu.VMEM((sources // 2, times * 2, planes // 2, 8, LANES), jnp.float32),
            pltpu.SemaphoreType.DMA((2, planes)),
            pltpu.SemaphoreType.DMA((3,)),
            pltpu.SemaphoreType.DMA((3,)),
            pltpu.SemaphoreType.DMA((2,)),
            pltpu.SemaphoreType.DMA((sources // 2,)),
            pltpu.SemaphoreType.REGULAR,
        ],
        compiler_params=pltpu.CompilerParams(
            collective_id=0, has_side_effects=True, vmem_limit_bytes=40 * 2**20
        ),
    )(*[pltpu.with_memory_space_constraint(v, pltpu.HBM) for v in inputs])
    shape = (times, own, slab * 2 // LANES, LANES)
    out = pl.pallas_call(
        functools.partial(finish_kernel, times, own),
        out_shape=jax.ShapeDtypeStruct(shape, jnp.float32),
        in_specs=[vmem, vmem],
        out_specs=anywhere,
        scratch_shapes=[pltpu.VMEM(shape, jnp.float32), pltpu.SemaphoreType.DMA((times,))],
        compiler_params=pltpu.CompilerParams(vmem_limit_bytes=40 * 2**20),
    )(got, line_near)
    return out.reshape(times, own, slab // LANES, 2, LANES).transpose(0, 1, 3, 2, 4).reshape(times, own, 2, slab)


def solution(mesh):
    placed = (P("ta", None, None, None, "xyz"), P("ta", None, None, None, "xyz"))
    times, sources = mesh.shape["ta"], mesh.shape["xyz"]

    def device(prop_one, prop_two):
        planes = prop_one.shape[-1] // (L * L)
        fits = 4 * L == LANES and planes * sources == L and L // sources == 4 and times == 4
        if fits and prop_one.shape[0] == 1:
            return fast_device(prop_one, prop_two, times, sources)
        return on_device(prop_one, prop_two)

    return jax.shard_map(
        device, mesh=mesh, in_specs=placed, out_specs=P(None, "ta", None, "xyz"), check_vma=False
    )
```

```python
import functools
import itertools
import math

import jax
import jax.numpy as jnp
import numpy as np
from jax import lax
from jax.experimental import pallas as pl
from jax.experimental.pallas import tpu as pltpu
from jax.sharding import PartitionSpec as P

L = 32


spin_columns = [[3, 2, 1, 0], [3, 2, 1, 0], [2, 3, 0, 1], [2, 3, 0, 1]]
spin_phases = [[1j, 1j, -1j, -1j], [-1.0, 1.0, 1.0, -1.0], [1j, -1j, -1j, 1j], [1.0, 1.0, 1.0, 1.0]]
chiral_signs = [1.0, 1.0, -1.0, -1.0]


def vertex_parts():
    result = []
    for gamma_index in range(4):
        columns = spin_columns[gamma_index]
        phases = spin_phases[gamma_index]
        rows_list = [columns[a // 3] * 3 + a % 3 for a in range(12)]
        phase_list = [complex(phases[a // 3]) for a in range(12)]
        result.append((rows_list, phase_list))
    return (result, [chiral_signs[a // 3] for a in range(12)])


def contract(prop_a, prop_b):
    gammas, chirality = vertex_parts()
    left_real, left_imag, right_real, right_imag = ([], [], [], [])
    for rows_list, phase_list in gammas:
        pick_real = jnp.stack([prop_a[0, q] for q in rows_list])
        pick_imag = jnp.stack([prop_a[1, q] for q in rows_list])
        phase_real = jnp.asarray(np.array([p.real for p in phase_list]), jnp.bfloat16)[
            :, None, None
        ]
        phase_imag = jnp.asarray(np.array([p.imag for p in phase_list]), jnp.bfloat16)[
            :, None, None
        ]
        left_real.append(phase_real * pick_real - phase_imag * pick_imag)
        left_imag.append(phase_real * pick_imag + phase_imag * pick_real)
        col_real = jnp.stack([prop_b[0][:, q] for q in rows_list], axis=1)
        col_imag = jnp.stack([prop_b[1][:, q] for q in rows_list], axis=1)
        factor = np.array(
            [
                [phase_list[c] * chirality[rows_list[c]] * chirality[a] for c in range(12)]
                for a in range(12)
            ]
        )
        factor_real = jnp.asarray(factor.real, jnp.bfloat16)[:, :, None]
        factor_imag = jnp.asarray(factor.imag, jnp.bfloat16)[:, :, None]
        right_real.append(factor_real * col_real + factor_imag * col_imag)
        right_imag.append(factor_imag * col_real - factor_real * col_imag)
    left_rows = jnp.stack(left_real + left_imag).reshape(8, 144, -1)
    right_rows = jnp.stack(right_real + right_imag).reshape(8, 144, -1)
    products = jnp.einsum("mks,nks->mns", left_rows, right_rows, preferred_element_type=jnp.float32)
    real_sum = products[:4, :4] - products[4:, 4:]
    imag_sum = products[:4, 4:] + products[4:, :4]
    return jnp.stack([real_sum.reshape(16, -1), imag_sum.reshape(16, -1)], axis=1)


def dft_tables(length):
    positions = np.arange(length)
    turn_count = positions[:, None] * positions[None, :] % length
    angles = turn_count * (2.0 * math.pi / length)
    cosines = jnp.asarray(np.cos(angles) / math.sqrt(length), jnp.float32)
    sines = jnp.asarray(np.sin(angles) / math.sqrt(length), jnp.float32)
    return (cosines, sines)


def plane_dft(fields):
    cosines, sines = dft_tables(L)
    highest = lax.Precision.HIGHEST
    shape = fields.shape
    grid = fields.reshape(shape[:4] + (L, L))
    real_part = grid[:, :, 0]
    imag_part = grid[:, :, 1]

    def along_z(values, table):
        return jnp.einsum(
            "tfpyz,zk->tfpyk", values, table, precision=highest, preferred_element_type=jnp.float32
        )

    def along_y(values, table):
        return jnp.einsum(
            "tfpyz,yk->tfpkz", values, table, precision=highest, preferred_element_type=jnp.float32
        )

    mid_real = along_z(real_part, cosines) + along_z(imag_part, sines)
    mid_imag = along_z(imag_part, cosines) - along_z(real_part, sines)
    out_real = along_y(mid_real, cosines) + along_y(mid_imag, sines)
    out_imag = along_y(mid_imag, cosines) - along_y(mid_real, sines)
    return jnp.stack([out_real, out_imag], axis=2).reshape(shape)


def line_dft(data):
    length = data.shape[-2]
    cosines, sines = dft_tables(length)
    real_part = data[..., 0, :, :]
    imag_part = data[..., 1, :, :]

    def transform_rows(values, table):
        return jnp.einsum(
            "...xq,xk->...qk",
            values,
            table,
            precision=lax.Precision.HIGHEST,
            preferred_element_type=jnp.float32,
        )

    out_real = transform_rows(real_part, cosines) + transform_rows(imag_part, sines)
    out_imag = transform_rows(imag_part, cosines) - transform_rows(real_part, sines)
    stacked = jnp.stack([out_real, out_imag], axis=-3)
    return stacked.reshape(stacked.shape[:-2] + (stacked.shape[-2] * stacked.shape[-1],))


def on_device(prop_one, prop_two):
    fields = lax.map(
        lambda slice_pair: contract(slice_pair[0], slice_pair[1]), (prop_one, prop_two)
    )
    local_times, field_count, parts, slab = fields.shape
    planes = slab // (L * L)
    fields = plane_dft(fields.reshape(local_times, field_count, parts, planes, L * L))
    turned_fields = line_dft(lax.all_to_all(fields, "xyz", split_axis=4, concat_axis=3, tiled=True))
    result = lax.all_to_all(turned_fields, "ta", split_axis=1, concat_axis=0, tiled=True)
    return result

LANES = 128
GROUP_PERMS = (0, 2)
LATE, AROUND, BULK = range(3)
TOGETHER = 2


def spin_tables():
    chi = np.array(chiral_signs)
    alpha = np.array(spin_phases) * chi[None, :]
    beta = np.array([[spin_phases[n][c] * chi[spin_columns[n][c]] for c in range(4)] for n in range(4)])
    tables = []
    for phases in (alpha, beta):
        pairs = []
        for first in GROUP_PERMS:
            found = []
            for a in range(4):
                for members in found:
                    ratio = phases[first : first + 2, a] / phases[first : first + 2, members[0][0]]
                    if ratio[0] == ratio[1] and ratio[0] in (1, -1):
                        members.append((a, int(ratio[0].real)))
                        break
                else:
                    found.append([(a, 1)])
            assert len(found) == 2
            pairs.append(found)
        lead = np.array([[phases[m, pairs[m // 2][half][0][0]] for half in range(2)] for m in range(4)])
        signs = np.array([[int((lead[m, half] / lead[m, 0]).real) for half in range(2)] for m in range(4)])
        tables.append((pairs, lead[:, 0], signs))
    left, right = tables
    phase = np.outer(left[1], right[1]).reshape(16)
    return left[0], left[2], right[0], right[2], phase


def complex_block(table):
    return np.block([[table.real, table.imag], [-table.imag, table.real]])


def high_low(table):
    high = np.asarray(table).astype(jnp.bfloat16)
    low = (table - high.astype(np.float64)).astype(jnp.bfloat16)
    return jnp.asarray(np.stack([high, low]))


def plane_tables(length):
    quarter = LANES // length
    outer = length // quarter
    lane = np.arange(LANES)
    y, z = lane // length, lane % length
    twiddle = np.exp(-2j * np.pi * np.outer(np.arange(outer), y) / length)
    ky, slot = lane // length, lane % length
    kz = (slot % outer) * quarter + slot // outer
    table = np.exp(-2j * np.pi * (np.outer(y, ky) / quarter + np.outer(z, kz) / length)) / length
    return (
        jnp.asarray(np.stack([twiddle.real, twiddle.imag]), jnp.float32),
        high_low(complex_block(table)),
    )


def line_table(length, own, sources):
    x = np.arange(length)
    turn = np.exp(-2j * np.pi * np.outer(x, x) / length) / math.sqrt(length)
    parts = complex_block(turn).reshape(2, sources, length // sources, 2, length)
    full = np.einsum("asxbk,fg->sxafbgk", parts, np.eye(own))
    rows = length * 2 * own
    full = full.reshape(rows, 2, rows // 2)
    moved = np.roll(full, length, axis=2)
    return jnp.concatenate([high_low(full.reshape(rows, rows)), high_low(moved.reshape(rows, rows))])


def split_dot(values, table):
    high = values.astype(jnp.bfloat16)
    low = (values - high.astype(jnp.float32)).astype(jnp.bfloat16)

    def dot(a, b):
        return jnp.dot(a, b, preferred_element_type=jnp.float32)

    return dot(high, table[0]) + (dot(low, table[0]) + dot(high, table[1]))


def small_fft(values):
    count = len(values)
    if count == 1:
        return values
    even, odd = small_fft(values[0::2]), small_fft(values[1::2])
    low, high = [], []
    for k in range(count // 2):
        re, im = odd[k]
        if k == 0:
            pass
        elif 4 * k == count:
            re, im = im, -re
        else:
            c, s = math.cos(2 * math.pi * k / count), math.sin(2 * math.pi * k / count)
            re, im = c * re + s * im, c * im - s * re
        low.append((even[k][0] + re, even[k][1] + im))
        high.append((even[k][0] - re, even[k][1] - im))
    return low + high


def swap_blocks(values):
    width = LANES // 4
    shape = values[0].shape
    axis = len(shape) - 1
    block = lax.broadcasted_iota(jnp.int32, shape, axis) // width
    low, even = block < 2, block % 2 == 0
    values = list(values)
    for i in range(2):
        first, second = values[i], values[i + 2]
        moved = pltpu.roll(jnp.where(low, second, first), 2 * width, axis)
        values[i], values[i + 2] = jnp.where(low, first, moved), jnp.where(low, moved, second)
    for i in (0, 2):
        first, second = values[i], values[i + 1]
        values[i] = jnp.where(even, first, pltpu.roll(second, width, axis))
        values[i + 1] = jnp.where(even, pltpu.roll(first, LANES - width, axis), second)
    return values


def add_signed(total, term, sign):
    if total is None:
        return term if sign > 0 else -term
    return total + term if sign > 0 else total - term


def widen(sources, targets, row):
    rows = targets[0].shape[2]

    @pl.loop(0, 12)
    def _(sink):
        for c in range(12):
            for source, target in zip(sources, targets):
                target[sink, c, :, :] = source[sink, c, pl.ds(row, rows), :].astype(jnp.float32)


def site_sums(tables, one, two, partial, mixed):
    left_groups, left_signs, right_groups, right_signs, phases = tables
    tiles = one.shape[2] // 2
    columns = [spin_columns[first] for first in GROUP_PERMS]
    left_of = [{a: (half, sign) for half in range(2) for a, sign in left_groups[pair][half]} for pair in range(2)]
    right_of = [{c: (side, sign) for side in range(2) for c, sign in right_groups[turn][side]} for turn in range(2)]

    def read(ref, at, kind, sign):
        first, second = (ref[at[0], at[1], pl.ds(part, tiles, stride=2), :] if kind in (part, 2) else None for part in range(2))
        if kind < 2:
            return second if kind else first
        return first + second if sign > 0 else first - second

    def blocks(kind):
        def step(i, sums):
            sums = list(sums)
            for j, q_first, c_first in itertools.product(range(3), (0, 2), (0, 2)):
                ones = {
                    (q, c): read(one, (q * 3 + i, c * 3 + j), kind, 1)
                    for q in (q_first, q_first + 1)
                    for c in (c_first, c_first + 1)
                }
                twos = {}
                for q, c in ones:
                    for pair in range(2):
                        for turn in range(2):
                            at = (columns[pair][q], columns[turn][c])
                            if at not in twos:
                                twos[at] = read(two, (at[0] * 3 + i, at[1] * 3 + j), kind, -1)
                for q, c in ones:
                    for pair in range(2):
                        half, left_sign = left_of[pair][columns[pair][q]]
                        for turn in range(2):
                            side, right_sign = right_of[turn][c]
                            k = ((pair * 2 + half) * 2 + turn) * 2 + side
                            term = ones[q, c] * twos[columns[pair][q], columns[turn][c]]
                            sums[k] = add_signed(sums[k], term, left_sign * right_sign)
            return tuple(sums)

        start = tuple(jnp.zeros((tiles, LANES), jnp.float32) for _ in range(16))
        return lax.fori_loop(0, 3, step, start)

    for kind in range(2):
        for k, total in enumerate(blocks(kind)):
            partial[kind, k, :, :] = total
    both = blocks(2)
    for pair in range(2):
        for turn in range(2):
            quads = ([], [])
            for half in range(2):
                for side in range(2):
                    k = ((pair * 2 + half) * 2 + turn) * 2 + side
                    straight, crossed = partial[0, k, :, :], partial[1, k, :, :]
                    quads[0].append(straight + crossed)
                    quads[1].append(both[k] - (straight - crossed))
            for nu in (2 * turn, 2 * turn + 1):
                joined = []
                for quad in quads:
                    for half in range(2):
                        total = add_signed(None, quad[2 * half], int(right_signs[nu][0]))
                        joined.append(add_signed(total, quad[2 * half + 1], int(right_signs[nu][1])))
                for mu in (2 * pair, 2 * pair + 1):
                    field = 4 * mu + nu
                    phase = phases[field]
                    for part in range(2):
                        sign = (phase.real + phase.imag) * (-1 if part and phase.imag else 1)
                        total = add_signed(None, joined[2 * part], int(left_signs[mu][0] * sign))
                        total = add_signed(total, joined[2 * part + 1], int(left_signs[mu][1] * sign))
                        where = 1 - part if phase.imag else part
                        mixed[where, field * tiles : (field + 1) * tiles, :] = total


def plane_blocks(twiddle_ref, plane_ref, mixed, tiles, store):
    blocks = [tuple(mixed[part, pl.ds(t, 16, stride=tiles), :] for part in range(2)) for t in range(tiles)]
    spectrum = small_fft(blocks)
    turned = []
    for k, (re, im) in enumerate(spectrum):
        c = twiddle_ref[0, k : k + 1, :]
        s = twiddle_ref[1, k : k + 1, :]
        turned.append(jnp.concatenate([re * c - im * s, re * s + im * c], axis=1) if k else jnp.concatenate([re, im], axis=1))
    out = split_dot(jnp.concatenate(turned, axis=0), plane_ref)
    upper = lax.broadcasted_iota(jnp.int32, (8, LANES), 0) < 4
    for half in range(tiles // 4):
        parts = []
        for part in range(2):
            rows = [
                out[(4 * half + p) * 16 : (4 * half + p + 1) * 16, part * LANES : (part + 1) * LANES]
                for p in range(4)
            ]
            parts.append(swap_blocks(rows))
        for k in range(4):
            owner = k * (tiles // 4) + half
            for pair in range(2):
                re = parts[0][k][pair * 8 : pair * 8 + 8]
                im = parts[1][k][pair * 8 : pair * 8 + 8]
                store(owner, 2 * pair, jnp.where(upper, re, pltpu.roll(im, 4, 0)))
                store(owner, 2 * pair + 1, jnp.where(upper, pltpu.roll(re, 4, 0), im))


def finish_times(blocks, line_ref, out_ref, first, own):
    operands = ([], [])
    for rows in blocks:
        grid = rows.T.reshape(4, 4, 8, -1)
        for q in range(4):
            operands[q % 2].append(grid[:, q].reshape(32, -1))
    out = [split_dot(jnp.concatenate(operands[k], axis=0), (line_ref[2 * k], line_ref[2 * k + 1])) for k in range(2)]
    block = lax.broadcasted_iota(jnp.int32, (32, LANES), 1) // L
    low, even = block < 2, block % 2 == 0
    for at in range(len(blocks)):
        for part in range(2):
            lanes = slice(part * LANES, (part + 1) * LANES)
            pairs = []
            for half in range(2):
                start = (2 * at + half) * 32
                plain, moved = (out[k][start : start + 32, lanes] for k in range(2))
                crossed = pltpu.roll(jnp.where(even, moved, plain), LANES - L, 1)
                pairs.append((jnp.where(even, plain, moved), crossed))
            for f in range(2):
                left, right = pairs[0][f], pairs[1][f]
                swapped = pltpu.roll(jnp.where(low, right, left), LANES // 2, 1)
                out_ref[first + at, f, pl.ds(part, 32, stride=2), :] = jnp.where(low, left, swapped)
                out_ref[first + at, f + 2, pl.ds(part, 32, stride=2), :] = jnp.where(low, swapped, right)


def levels_of(s):
    z = s // 2
    beyond = z // 2
    edge = 3 * (1 - beyond)
    return edge, edge + 2 * beyond - 1, beyond * 2 + (z + 1) % 2


def chip(core, level, at):
    return [(at // 2 * 2 + (core + dc) % 2, level * 2 + at % 2) for dc in (1, 0)]


def others_of(t, s):
    here = t // 2 * 2 + s % 2
    first, second = here % 2 * (1 - here // 2), (1 - here % 2) * (here // 2)
    return (3 - here) // 3 * 3, 1 + first, 2 + first + second


def beside_of(t, s):
    return [peer for at in others_of(t, s) for peer in chip(t % 2, s // 2, at)] + [(t // 2 * 2 + 1 - t % 2, s)]


def late_of(t, s):
    y, core, z, x = t // 2, t % 2, s // 2, s % 2
    beyond = z // 2
    edge, inner, near = levels_of(s)
    here = y * 2 + x
    others = others_of(t, s)
    turn = [(here + k) % 4 for k in range(4)]
    head = [0] + [1 + (here + k) % 3 for k in range(3)]
    edges = inners = [beyond * head[k] + (1 - beyond) * turn[k] for k in range(4)]
    late = []
    late += [peer for peer in chip(core, z, others[0])]
    late += [peer for peer in chip(core, near, head[0])]
    late += [peer for peer in chip(core, edge, edges[0])]
    late += [peer for peer in chip(core, near, head[1])]
    late += [peer for peer in chip(core, z, others[1])]
    late += [peer for peer in chip(core, near, head[2])]
    late += [peer for peer in chip(core, z, others[2])]
    late += [peer for peer in chip(core, near, head[3])]
    late.append((y * 2 + 1 - core, s))
    late += [peer for peer in chip(core, edge, edges[1])]
    late += [peer for peer in chip(core, inner, inners[0])]
    late += [peer for peer in chip(core, edge, edges[2])]
    late += [peer for peer in chip(core, inner, inners[1])]
    late += [peer for peer in chip(core, edge, edges[3])]
    late += [peer for peer in chip(core, inner, inners[2])]
    late += [peer for peer in chip(core, inner, inners[3])]
    return late


def exchange_kernel(
    tables, tiles, planes, times, sources, names,
    one_hbm, two_hbm, twiddle_hbm, plane_hbm, line_hbm, got, line_out,
    one_ref, two_ref, twiddle_ref, plane_ref, one_wide, two_wide, partial, mixed, send, relay,
    in_sem, table_sem, send_sem, recv_sem, relay_sem, ready,
):
    def load(p, which):
        source, target = ((one_hbm, one_ref), (two_hbm, two_ref))[which]
        rows = pl.ds(pl.multiple_of(p * 2 * tiles, 2 * tiles), 2 * tiles)
        return pltpu.make_async_copy(source.at[:, :, rows, :], target.at[:, :, rows, :], in_sem.at[which, p])

    @pl.loop(0, 2)
    def _(p):
        for which in (1, 0):
            load(p, which).start()

    t, s = lax.axis_index(names[0]), lax.axis_index(names[1])
    barrier = pltpu.get_barrier_semaphore()
    z, x = s // 2, s % 2
    edge, inner, near = levels_of(s)
    beyond = z // 2
    second = beyond * edge + (1 - beyond) * inner
    third = beyond * inner + (1 - beyond) * edge
    levels, count, early = (near, second, third), times * sources - 1, planes // 2
    column = [(t, level * 2 + x) for level in levels]
    beside = beside_of(t, s)
    plane_size, late = times * 2, pl.ds(early, planes - early)

    def slot(peer):
        return peer[1] // 2 * plane_size + peer[0] * 2 + peer[1] % 2

    def move(source, target, peer, kind, landed=None):
        return pltpu.make_async_remote_copy(
            src_ref=source,
            dst_ref=target,
            send_sem=send_sem.at[kind],
            recv_sem=recv_sem.at[kind] if landed is None else landed,
            device_id={names[0]: peer[0], names[1]: peer[1]},
            device_id_type=pl.DeviceIdType.MESH,
        )

    def signal(sem, peer):
        pl.semaphore_signal(
            sem, inc=1, device_id={names[0]: peer[0], names[1]: peer[1]}, device_id_type=pl.DeviceIdType.MESH
        )

    table_copies = [
        pltpu.make_async_copy(source, target, table_sem.at[k])
        for k, (source, target) in enumerate(
            ((twiddle_hbm, twiddle_ref), (plane_hbm, plane_ref), (line_hbm, line_out))
        )
    ]
    for peer in column + beside:
        signal(barrier, peer)
    for copy in table_copies[:2]:
        copy.start()
    late_peers = [(peer, slot(peer)) for peer in late_of(t, s)]
    beside_slots = [(peer, slot(peer)) for peer in beside]
    mine = t * sources + s

    @pl.loop(0, planes)
    def _(p):
        load(p, 1).wait()
        load(p, 0).wait()

        @pl.when(p == 0)
        def _():
            for later in range(2, planes):
                for which in (1, 0):
                    load(later, which).start()
            table_copies[2].start()

        row = pl.multiple_of(p * 2 * tiles, 2 * tiles)
        widen((two_ref, one_ref), (two_wide, one_wide), row)
        site_sums(tables, one_wide, two_wide, partial, mixed)

        @pl.when(p == 0)
        def _():
            for copy in table_copies[:2]:
                copy.wait()

        def store(owner, group, value):
            send[slot((group, owner)), p, :, :] = value

        plane_blocks(twiddle_ref, plane_ref, mixed, tiles, store)

        @pl.when(p == 0)
        def _():
            pl.semaphore_wait(barrier, len(column + beside))
            for peer in column:
                signal(ready, peer)

        @pl.when(p < early)
        def _():
            for level, peer in zip(levels, column):
                group = pl.ds(level * plane_size, plane_size)
                move(send.at[group, p], relay.at[z, :, p], peer, BULK, relay_sem.at[z]).start()

        got[t * sources + s, p, :, :] = send[slot((t, s)), p, :, :]

    pl.semaphore_wait(ready, len(column))
    first = pl.ds(0, early)
    for peer, at in beside_slots:
        move(send.at[at, first], got.at[mine, first], peer, AROUND).start()
    for peer, at in late_peers:
        move(send.at[at, late], got.at[mine, late], peer, LATE).start()
    for level in (near, edge, inner):
        move(relay.at[level], relay.at[level], column[0], BULK, relay_sem.at[level]).wait_recv()
        here = t * sources + level * 2 + x
        for peer in beside:
            move(relay.at[level, peer[0] * 2 + peer[1] % 2], got.at[here, first], peer, AROUND).start()
        got[here, first, :, :] = relay[level, t * 2 + x, :, :, :]
    table_copies[2].wait()
    for kind, number in ((LATE, count), (AROUND, (len(column) + 1) * len(beside)), (BULK, len(column) * plane_size)):
        span = pl.ds(0, number)
        total = move(send.at[span, first], got.at[span, first], column[0], kind)
        if kind != BULK:
            total.wait_recv()
        total.wait_send()


def finish_kernel(times, own, got, line_ref, out_hbm, out_ref, out_sem):
    copies = []
    span = got.shape[0] // times
    for first in range(0, times, TOGETHER):
        blocks = [got[at * span : (at + 1) * span].reshape(-1, LANES) for at in range(first, first + TOGETHER)]
        finish_times(blocks, line_ref, out_ref, first, own)
        for at in range(first, first + TOGETHER):
            copy = pltpu.make_async_copy(out_ref.at[at], out_hbm.at[at], out_sem.at[at])
            copy.start()
            copies.append(copy)
    for copy in copies:
        copy.wait()


def fast_device(prop_one, prop_two, times, sources):
    slab = prop_one.shape[-1]
    plane = L * L
    planes, tiles = slab // plane, plane // LANES
    own = 16 // times
    tables = spin_tables()
    twiddle, plane_table = plane_tables(L)
    line = line_table(L, own, sources)

    def paired(prop):
        split = prop.reshape(2, 12, 12, slab // LANES, LANES).transpose(1, 2, 3, 0, 4)
        return split.reshape(12, 12, slab // LANES * 2, LANES)

    anywhere = pl.BlockSpec(memory_space=pltpu.HBM)
    vmem = pl.BlockSpec(memory_space=pltpu.VMEM)
    everyone = times * sources
    inputs = (paired(prop_one), paired(prop_two), twiddle, plane_table, line)
    got, line_near = pl.pallas_call(
        functools.partial(exchange_kernel, tables, tiles, planes, times, sources, ("ta", "xyz")),
        out_shape=(
            pltpu.VMEM((everyone, planes, 8, LANES), jnp.float32),
            pltpu.VMEM(line.shape, line.dtype),
        ),
        in_specs=[anywhere] * len(inputs),
        out_specs=(vmem, vmem),
        scratch_shapes=[
            pltpu.VMEM((12, 12, slab // LANES * 2, LANES), jnp.bfloat16),
            pltpu.VMEM((12, 12, slab // LANES * 2, LANES), jnp.bfloat16),
            pltpu.VMEM(twiddle.shape, twiddle.dtype),
            pltpu.VMEM(plane_table.shape, plane_table.dtype),
            pltpu.VMEM((12, 12, 2 * tiles, LANES), jnp.float32),
            pltpu.VMEM((12, 12, 2 * tiles, LANES), jnp.float32),
            pltpu.VMEM((2, 16, tiles, LANES), jnp.float32),
            pltpu.VMEM((2, 16 * tiles, LANES), jnp.float32),
            pltpu.VMEM((everyone, planes, 8, LANES), jnp.float32),
            pltpu.VMEM((sources // 2, times * 2, planes // 2, 8, LANES), jnp.float32),
            pltpu.SemaphoreType.DMA((2, planes)),
            pltpu.SemaphoreType.DMA((3,)),
            pltpu.SemaphoreType.DMA((3,)),
            pltpu.SemaphoreType.DMA((2,)),
            pltpu.SemaphoreType.DMA((sources // 2,)),
            pltpu.SemaphoreType.REGULAR,
        ],
        compiler_params=pltpu.CompilerParams(
            collective_id=0, has_side_effects=True, vmem_limit_bytes=40 * 2**20
        ),
    )(*[pltpu.with_memory_space_constraint(v, pltpu.HBM) for v in inputs])
    shape = (times, own, slab * 2 // LANES, LANES)
    out = pl.pallas_call(
        functools.partial(finish_kernel, times, own),
        out_shape=jax.ShapeDtypeStruct(shape, jnp.float32),
        in_specs=[vmem, vmem],
        out_specs=anywhere,
        scratch_shapes=[pltpu.VMEM(shape, jnp.float32), pltpu.SemaphoreType.DMA((times,))],
        compiler_params=pltpu.CompilerParams(vmem_limit_bytes=40 * 2**20),
    )(got, line_near)
    return out.reshape(times, own, slab // LANES, 2, LANES).transpose(0, 1, 3, 2, 4).reshape(times, own, 2, slab)


def solution(mesh):
    placed = (P("ta", None, None, None, "xyz"), P("ta", None, None, None, "xyz"))
    times, sources = mesh.shape["ta"], mesh.shape["xyz"]

    def device(prop_one, prop_two):
        planes = prop_one.shape[-1] // (L * L)
        fits = 4 * L == LANES and planes * sources == L and L // sources == 4 and times == 4
        if fits and prop_one.shape[0] == 1:
            return fast_device(prop_one, prop_two, times, sources)
        return on_device(prop_one, prop_two)

    return jax.shard_map(
        device, mesh=mesh, in_specs=placed, out_specs=P(None, "ta", None, "xyz"), check_vma=False
    )
```
